128 devices in a mesh: row: 8 (over y, z_lo), col: 16 (over x, z_hi, core).
Axes of the slice: x: 4, y: 4, z: 4 (z_hi: 2, z_lo: 2; z = z_hi * 2 + z_lo), core: 2. Of those that a mesh axis runs over, the one named last changes fastest.
Arguments:
- object_field: float32 [2, 2048, 4096], P(None, 'row', 'col'), may hold values from -40 to 40
- probe: float32 [2, 4, 256, 256], replicated, may hold values from -3 to 3
- pos_rows: int32 [8, 16, 2, 3], P('row', 'col'), may hold values from 0 to 255
- pos_cols: int32 [8, 16, 2, 3], P('row', 'col'), may hold values from 0 to 255
- counts: int32 [8, 16, 2], P('row', 'col'), may hold values from 1 to 3, as said below
- magnitudes: float32 [8, 16, 2, 3, 256, 256], P('row', 'col'), may hold values from 0 to 4
Outputs:
- object_out: float32 [2, 2048, 4096], P(None, 'row', 'col')
- probe_out: float32 [2, 4, 256, 256], replicated
- errors: float32 [4], replicated
The draws below stay inside these ranges and needn't reach their ends.
Inputs may be any that keep to these rules, and one draw needn't show every extreme that they name: `counts`: every tile holds at least one live position in each batch, and in every batch some tile holds 3.
All inputs are finite; a program needn't handle non-finite values.
Results may differ from the reference program's by a relative error of at most 0.0015.
Values sent between devices are 32-bit elements; how exact they have to be, the bound alone decides.
A program may use at most 128 MiB of HBM per device.

```python
import math
import jax
import jax.numpy as jnp
from jax import lax

PROBE = 256
MODES = 4
TILE = 256
SLOTS = 3
BATCHES = 2
ITERS = 2
HALO = 128
GRID_ROWS = 8
GRID_COLS = 16
NX = 2048
NY = 4096


def draw_object_field(key, part):
    keys = jax.random.split(key, 1)
    base = jnp.clip(jax.random.normal(keys[0], (2, NX, NY), jnp.float32), -6.0, 6.0)
    col_scale = jnp.exp(jnp.linspace(math.log(0.6), math.log(1.8), NY)).astype(jnp.float32)
    return base * col_scale[None, None, :]


def draw_counts(key, part):
    keys = jax.random.split(key, 2)
    level = jax.random.randint(keys[0], (GRID_ROWS * GRID_COLS, BATCHES), 0, 10)
    middle = (SLOTS + 1) // 2
    filled = jnp.where(level >= 8, SLOTS, jnp.where(level >= 5, middle, 1)).astype(jnp.int32)
    chosen = jax.random.randint(keys[1], (BATCHES,), 0, GRID_ROWS * GRID_COLS)
    filled = filled.at[chosen, jnp.arange(BATCHES)].set(SLOTS)
    return filled.reshape(GRID_ROWS, GRID_COLS, BATCHES).astype(jnp.int32)


def with_ends(result, own_key, smallest, top_value):
    longest = result.shape.index(max(result.shape))
    spots = []
    for shift in (0, 1):
        where = [jax.random.randint(jax.random.fold_in(own_key, axis), (), 0, length) for axis, length in enumerate(result.shape)]
        where[longest] = (where[longest] + shift) % result.shape[longest]
        spots.append(tuple(where))
    return result.at[spots[0]].set(smallest).at[spots[1]].set(top_value)


def steps_of(rng, shape, pieces, smallest, top_value):
    def one(position, blocks):
        steps = jax.random.uniform(jax.random.fold_in(jax.random.fold_in(rng, 6), position), (blocks,), jnp.float32, smallest / len(pieces), top_value / len(pieces))
        return jnp.repeat(jnp.exp(steps), shape[position] // blocks).reshape((-1,) + (1,) * (len(shape) - position - 1))

    level = one(*pieces[0])
    for cut in pieces[1:]:
        level = level * one(*cut)
    return level


def bell_draw(own_key, dims, spread, bound, held_as=jnp.bfloat16):
    values = jax.random.normal(own_key, dims, jnp.float32) * spread
    return jnp.minimum(jnp.maximum(values, -bound), bound).astype(held_as)


def setup_inputs(seed: int = 0) -> dict:
    streams_of = jax.random.split(jax.random.key(seed), 7)
    object_field = draw_object_field(jax.random.fold_in(streams_of[6], 71), 0)
    probe = bell_draw(streams_of[1], (2, MODES, PROBE, PROBE), 0.5, 3.0, jnp.float32)
    pos_rows = with_ends(jax.random.randint(streams_of[2], (GRID_ROWS, GRID_COLS, BATCHES, SLOTS), 0, TILE), jax.random.fold_in(streams_of[2], 1), 0, TILE - 1).astype(jnp.int32)
    pos_cols = with_ends(jax.random.randint(streams_of[3], (GRID_ROWS, GRID_COLS, BATCHES, SLOTS), 0, TILE), jax.random.fold_in(streams_of[3], 1), 0, TILE - 1).astype(jnp.int32)
    counts = draw_counts(jax.random.fold_in(streams_of[6], 71), 0)
    magnitudes = jnp.clip(4.0 * jax.random.uniform(streams_of[5], (GRID_ROWS, GRID_COLS, BATCHES, SLOTS, PROBE, PROBE), jnp.float32) ** steps_of(streams_of[5], (GRID_ROWS, GRID_COLS, BATCHES, SLOTS, PROBE, PROBE), ((0, 8), (1, 16)), -0.2, 0.2), 0.0, 4.0)
    return {"object_field": object_field, "probe": probe, "pos_rows": pos_rows, "pos_cols": pos_cols, "counts": counts, "magnitudes": magnitudes}


object_rate = 0.9
probe_rate = 0.5
floor_value = 0.5
tiny_value = 1e-06

def dft_tables(probe_side):
    indices = jnp.arange(probe_side, dtype=jnp.int32)
    phase_index = indices[:, None] * indices[None, :] % probe_side
    angles = phase_index.astype(jnp.float32) * (2.0 * math.pi / probe_side)
    norm_scale = 1.0 / math.sqrt(probe_side)
    cosine = jnp.cos(angles) * norm_scale
    sine_part = -jnp.sin(angles) * norm_scale
    forward = jnp.stack([jnp.stack([cosine, -sine_part]), jnp.stack([sine_part, cosine])]).astype(jnp.bfloat16)
    inverse = jnp.stack([jnp.stack([cosine, sine_part]), jnp.stack([-sine_part, cosine])]).astype(jnp.bfloat16)
    return (forward, inverse)

def transform(field, table):
    table_wide = table.astype(jnp.float32)
    left_half = jnp.einsum('oixa,imab->omxb', table_wide, field.astype(jnp.float32)).astype(jnp.bfloat16)
    return jnp.einsum('imxb,oiby->omxy', left_half.astype(jnp.float32), table_wide)

def position_terms(window, probe, amplitude, forward, inverse):
    probe_re = probe[0]
    probe_im = probe[1]
    window_re = window[0][None]
    window_im = window[1][None]
    exit_wave = jnp.stack([probe_re * window_re - probe_im * window_im, probe_re * window_im + probe_im * window_re]).astype(jnp.bfloat16)
    far_field = transform(exit_wave, forward)
    modulus = jnp.sqrt(lax.optimization_barrier(jnp.sum(far_field * far_field, axis=(0, 1))))
    factor = amplitude / jnp.maximum(modulus, floor_value) - 1.0
    correction = (far_field * factor[None, None]).astype(jnp.bfloat16)
    update_wave = transform(correction, inverse)
    wave_re = update_wave[0]
    wave_im = update_wave[1]
    object_term = jnp.stack([lax.optimization_barrier(jnp.sum(probe_re * wave_re + probe_im * wave_im, axis=0)), lax.optimization_barrier(jnp.sum(probe_re * wave_im - probe_im * wave_re, axis=0))])
    probe_term = jnp.stack([window_re * wave_re + window_im * wave_im, window_re * wave_im - window_im * wave_re])
    power_term = jnp.sum(window * window)
    misfit = jnp.sum(jnp.square(modulus - amplitude))
    return (object_term, probe_term, power_term, misfit)

def reference(object_field, probe, pos_rows, pos_cols, counts, magnitudes):
    forward, inverse = dft_tables(PROBE)
    errors = []
    entries = jnp.arange(GRID_ROWS * GRID_COLS * SLOTS, dtype=jnp.int32)
    for sweep in range(ITERS):
        for batch in range(BATCHES):
            padded = jnp.pad(object_field, ((0, 0), (HALO, HALO), (HALO, HALO)))

            def step(carry, entry):
                object_grad, probe_grad, power_sum, misfit_sum = carry
                tile_row = entry // (GRID_COLS * SLOTS)
                tile_col = entry // SLOTS % GRID_COLS
                slot_index = entry % SLOTS
                live_mask = (slot_index < counts[tile_row, tile_col, batch]).astype(jnp.float32)
                corner_row = (tile_row * TILE + pos_rows[tile_row, tile_col, batch, slot_index]).astype(jnp.int32)
                corner_col = (tile_col * TILE + pos_cols[tile_row, tile_col, batch, slot_index]).astype(jnp.int32)
                anchor = (jnp.int32(0), corner_row, corner_col)
                window = lax.dynamic_slice(padded, anchor, (2, PROBE, PROBE))
                amplitude = magnitudes[tile_row, tile_col, batch, slot_index]
                object_term, probe_term, power_term, misfit = position_terms(window, probe, amplitude, forward, inverse)
                region = lax.dynamic_slice(object_grad, anchor, (2, PROBE, PROBE))
                object_grad = lax.dynamic_update_slice(object_grad, region + live_mask * object_term, anchor)
                return ((object_grad, probe_grad + live_mask * probe_term, power_sum + live_mask * power_term, misfit_sum + live_mask * misfit), None)
            start = (jnp.zeros(padded.shape, jnp.float32), jnp.zeros(probe.shape, jnp.float32), jnp.float32(0.0), jnp.float32(0.0))
            (object_grad, probe_grad, power_sum, misfit_sum), unused = lax.scan(step, start, entries)
            probe_peak = jnp.max(lax.optimization_barrier(jnp.sum(probe * probe, axis=(0, 1)))) + tiny_value
            object_field = object_field + object_rate / probe_peak * object_grad[:, HALO:HALO + NX, HALO:HALO + NY]
            probe = probe + probe_rate * PROBE * PROBE * probe_grad / power_sum
            errors.append(misfit_sum)
    return (object_field, probe, jnp.stack(errors))
```

```python
import functools
import math

import jax
import jax.numpy as jnp
import numpy as np
from jax import lax
from jax.experimental import pallas as pl
from jax.experimental.pallas import tpu as pltpu
from jax.sharding import Mesh
from jax.sharding import PartitionSpec as P

BATCHES = 2
ITERS = 2
SLOTS = 3
MODES = 4
SIDE = 256
HALF = 128
EXT = 512
AXES = ("row_0", "row_1", "col_0", "col_1", "col_2")
ROW = ("row_0", "row_1")
COL = ("col_0", "col_1", "col_2")
F32 = jnp.float32
BF16 = jnp.bfloat16

object_rate = 0.9
probe_rate = 0.5
floor_value = 0.5
tiny_value = 1e-06


def transform_tables():
    index = np.arange(SIDE)
    angles = (index[:, None] * index[None, :] % SIDE) * (2.0 * math.pi / SIDE)
    scale = 1.0 / math.sqrt(SIDE)
    c = np.cos(angles) * scale
    s = -np.sin(angles) * scale
    left = np.block([[c, -s], [s, c]])
    return left.astype(jnp.bfloat16), left.T.astype(jnp.bfloat16)


def compute_body(
    batch, rows_ref, cols_ref, counts_ref, obj, probe, mags, left_tab, right_tab,
    grad, pgrad, stats, win, wave, half, field,
):
    CH = 16
    steps = SIDE // CH
    lane = lax.broadcasted_iota(jnp.int32, (CH, 128), 1)

    grad[...] = jnp.zeros_like(grad)
    pgrad[...] = jnp.zeros_like(pgrad)
    stats[...] = jnp.zeros_like(stats)

    def fold(x):
        total = x[0:8, :]
        for i in range(1, x.shape[0] // 8):
            total = total + x[8 * i:8 * i + 8, :]
        return total

    def visit(slot, carry):
        row0 = rows_ref[batch * SLOTS + slot]
        col0 = cols_ref[batch * SLOTS + slot]
        block = lax.shift_right_logical(col0, 7)
        shift = col0 & 127
        back = (128 - shift) & 127

        def make_exit(i, c):
            at = pl.multiple_of(i * CH, CH)
            w = []
            for p in range(2):
                rolled = [
                    pltpu.roll(obj[p, block + j, pl.ds(row0 + at, CH), :], back, 1) for j in range(3)
                ]
                keep = lane < 128 - shift
                w.append([jnp.where(keep, rolled[j], rolled[j + 1]) for j in range(2)])
            power = jnp.zeros((8, 128), F32)
            for j in range(2):
                wr, wi = w[0][j], w[1][j]
                win[0, j, pl.ds(at, CH), :] = wr
                win[1, j, pl.ds(at, CH), :] = wi
                power = power + fold(wr * wr + wi * wi)
                for k in range(MODES):
                    pr = probe[0, k, pl.ds(j * SIDE + at, CH), :]
                    pi = probe[1, k, pl.ds(j * SIDE + at, CH), :]
                    wave[k, pl.ds(at, CH), j * 128:(j + 1) * 128] = (pr * wr - pi * wi).astype(BF16)
                    wave[k, pl.ds(SIDE + at, CH), j * 128:(j + 1) * 128] = (pr * wi + pi * wr).astype(BF16)
            stats[0] = stats[0] + power
            return c

        lax.fori_loop(0, steps, make_exit, 0)

        def transform(first, second):
            def left(k, c):
                res = jnp.dot(first[...], wave[k], preferred_element_type=F32).astype(BF16)
                at = pl.multiple_of(k * SIDE, SIDE)
                half[pl.ds(at, SIDE), 0:SIDE] = res[0:SIDE]
                half[pl.ds(at, SIDE), SIDE:EXT] = res[SIDE:EXT]
                return c

            lax.fori_loop(0, MODES, left, 0)

            def right(k, c):
                at = pl.multiple_of(k * 512, 512)
                field[pl.ds(at, 512), :] = jnp.dot(
                    half[pl.ds(at, 512), :], second[...], preferred_element_type=F32
                )
                return c

            lax.fori_loop(0, 2, right, 0)

        transform(left_tab, right_tab)

        def correct(i, c):
            at = pl.multiple_of(i * CH, CH)
            parts = [
                (field[pl.ds(k * SIDE + at, CH), 0:SIDE], field[pl.ds(k * SIDE + at, CH), SIDE:EXT])
                for k in range(MODES)
            ]
            total = sum(re * re + im * im for re, im in parts)
            modulus = jnp.sqrt(total)
            amplitude = mags[0, 0, 0, slot, pl.ds(at, CH), :]
            factor = amplitude / jnp.maximum(modulus, floor_value) - 1.0
            gap = modulus - amplitude
            gap = gap * gap
            stats[1] = stats[1] + fold(gap[:, 0:128]) + fold(gap[:, 128:256])
            for k in range(MODES):
                wave[k, pl.ds(at, CH), :] = (parts[k][0] * factor).astype(BF16)
                wave[k, pl.ds(SIDE + at, CH), :] = (parts[k][1] * factor).astype(BF16)
            return c

        lax.fori_loop(0, steps, correct, 0)
        transform(right_tab, left_tab)

        def spread(i, c):
            at = pl.multiple_of(i * CH, CH)
            term = [[None, None], [None, None]]
            for j in range(2):
                wr = win[0, j, pl.ds(at, CH), :]
                wi = win[1, j, pl.ds(at, CH), :]
                tr = ti = None
                for k in range(MODES):
                    ur = field[pl.ds(k * SIDE + at, CH), j * 128:(j + 1) * 128]
                    ui = field[pl.ds(k * SIDE + at, CH), SIDE + j * 128:SIDE + (j + 1) * 128]
                    spot = pl.ds(j * SIDE + at, CH)
                    pr = probe[0, k, spot, :]
                    pi = probe[1, k, spot, :]
                    ar = pr * ur + pi * ui
                    ai = pr * ui - pi * ur
                    tr = ar if tr is None else tr + ar
                    ti = ai if ti is None else ti + ai
                    pgrad[0, k, spot, :] = pgrad[0, k, spot, :] + (wr * ur + wi * ui)
                    pgrad[1, k, spot, :] = pgrad[1, k, spot, :] + (wr * ui - wi * ur)
                term[0][j], term[1][j] = tr, ti
            low = lane < shift
            zero = jnp.zeros((CH, 128), F32)
            for p in range(2):
                a = pltpu.roll(term[p][0], shift, 1)
                b = pltpu.roll(term[p][1], shift, 1)
                adds = (jnp.where(low, zero, a), jnp.where(low, a, b), jnp.where(low, b, zero))
                for j in range(3):
                    spot = pl.ds(row0 + at, CH)
                    grad[p, block + j, spot, :] = grad[p, block + j, spot, :] + adds[j]
            return c

        lax.fori_loop(0, steps, spread, 0)
        return carry

    lax.fori_loop(0, counts_ref[batch], visit, 0)


def position_work(batch, pos_rows, pos_cols, counts, obj, probe, magnitudes, tables):
    whole = pl.BlockSpec(memory_space=pltpu.VMEM)
    smem = pl.BlockSpec(memory_space=pltpu.SMEM)
    mags = pl.BlockSpec((1, 1, 1, SLOTS, SIDE, SIDE), lambda i: (0, 0, batch, 0, 0, 0))
    flops = SLOTS * 2 * 2 * MODES * 4 * 2 * SIDE ** 3
    return pl.pallas_call(
        functools.partial(compute_body, batch),
        grid=(1,),
        out_shape=(
            jax.ShapeDtypeStruct((2, 4, EXT, 128), F32),
            jax.ShapeDtypeStruct((2, MODES, EXT, 128), F32),
            jax.ShapeDtypeStruct((2, 8, 128), F32),
        ),
        in_specs=[smem, smem, smem, whole, whole, mags, whole, whole],
        out_specs=(whole, whole, whole),
        scratch_shapes=[
            pltpu.VMEM((2, 2, SIDE, 128), F32),
            pltpu.VMEM((MODES, EXT, SIDE), BF16),
            pltpu.VMEM((MODES * SIDE, EXT), BF16),
            pltpu.VMEM((MODES * SIDE, EXT), F32),
        ],
        cost_estimate=pl.CostEstimate(flops=flops, bytes_accessed=12 << 20, transcendentals=0),
        compiler_params=pltpu.CompilerParams(vmem_limit_bytes=56 << 20),
        name="position_work",
    )(pos_rows, pos_cols, counts, obj, probe, magnitudes, *tables)


def where_am_i():
    y, lo, x, hi, core = (lax.axis_index(name) for name in AXES)
    row, col = y * 2 + lo, x * 4 + hi * 2 + core
    z = hi * 2 + lo

    def tile(r, c):
        return (r // 2, r % 2, c // 4, (c // 2) % 2, c % 2)

    def along(axis, value):
        if axis == "x":
            return (y, lo, value, hi, core)
        if axis == "y":
            return (value, lo, x, hi, core)
        return (y, value % 2, x, value // 2, core)

    partner = (y, lo, x, hi, 1 - core)
    coords = {"x": x, "y": y, "z": z}
    return row, col, core, coords, along, partner, tile


ORDERS = (("x", "y", "z"), ("y", "x", "z"))


def exchange_body(
    last, obj, probe, grad, pgrad, stats, obj_out, probe_out, stats_out,
    core_in, acc, one_in, one, two_in, two, three_in, tile_in, tile_sum, stat_core,
    col_in, row_in, mid, rdma_send, rdma_recv,
):
    row, col, core, coords, along, partner, tile = where_am_i()
    up, down = tile((row + 7) % 8, col), tile((row + 1) % 8, col)
    left, right = tile(row, (col + 15) % 16), tile(row, (col + 1) % 16)

    barrier = pltpu.get_barrier_semaphore()
    greeted = [partner, up, down, left, right]
    for axis in ("x", "y", "z"):
        for d in (1, 2, 3):
            greeted.append(along(axis, (coords[axis] + d) % 4))
    for peer in greeted:
        pl.semaphore_signal(barrier, inc=1, device_id=peer, device_id_type=pl.DeviceIdType.MESH)
    pl.semaphore_wait(barrier, len(greeted))

    count = [0]

    def send(src, dst, peer):
        n = count[0]
        count[0] += 1
        copy = pltpu.make_async_remote_copy(
            src_ref=src, dst_ref=dst, send_sem=rdma_send.at[n], recv_sem=rdma_recv.at[n],
            device_id=peer, device_id_type=pl.DeviceIdType.MESH,
        )
        copy.start()
        return copy

    def wait(copies):
        for copy in copies:
            copy.wait()

    cols_sent = [
        send(grad.at[:, 3], col_in.at[0], right),
        send(grad.at[:, 0], col_in.at[1], left),
    ]
    core_sent = [
        send(stats, stat_core, partner),
        send(pgrad.at[1 - core], core_in, partner),
    ]

    def peak_step(i, best):
        at = pl.multiple_of(i * 16, 16)
        total = None
        for p in range(2):
            for k in range(MODES):
                v = probe[p, k, pl.ds(at, 16), :]
                total = v * v if total is None else total + v * v
        return jnp.maximum(best, jnp.maximum(total[0:8], total[8:16]))

    best = lax.fori_loop(0, EXT // 16, peak_step, jnp.zeros((8, 128), F32))
    rate = object_rate / (jnp.max(best) + tiny_value)

    wait(core_sent)
    for k in range(MODES):
        acc[k] = pgrad[core, k] + core_in[k]
    tile_sum[...] = stats[...] + stat_core[...]

    def scatter(phase, source, landing, length):
        sent = []
        for d in (2, 1, 3):
            peer = along(ORDERS[0][phase], (coords[ORDERS[0][phase]] + d) % 4)
            sent.append(send(tile_sum, tile_in.at[phase, d - 1], peer))
            for g in range(2):
                axis = ORDERS[g][phase]
                to = (coords[axis] + d) % 4
                at = pl.multiple_of(to * length, length)
                sent.append(
                    send(
                        source.at[2 * g:2 * g + 2, pl.ds(at, length), :],
                        landing.at[d - 1, 2 * g:2 * g + 2],
                        along(axis, to),
                    )
                )
        return sent

    def gather_sum(phase, source, landing, length):
        out = []
        for g in range(2):
            at = pl.multiple_of(coords[ORDERS[g][phase]] * length, length)
            for k in (2 * g, 2 * g + 1):
                out.append(
                    source[k, pl.ds(at, length), :] + landing[0, k] + landing[1, k] + landing[2, k]
                )
        tile_sum[...] = tile_sum[...] + tile_in[phase, 0] + tile_in[phase, 1] + tile_in[phase, 2]
        return out

    sent = scatter(0, acc, one_in, 128)
    wait(sent)
    for k, v in enumerate(gather_sum(0, acc, one_in, 128)):
        one[k] = v
    sent = scatter(1, one, two_in, 32)

    wait(cols_sent)
    has_left, has_right = col > 0, col < 15
    for p in range(2):
        mid[p, 0] = grad[p, 1] + jnp.where(has_left, col_in[0, p], 0.0)
        mid[p, 1] = grad[p, 2] + jnp.where(has_right, col_in[1, p], 0.0)
    rows_sent = [
        send(mid.at[:, :, 0:SIDE, :], row_in.at[1], up),
        send(mid.at[:, :, SIDE:EXT, :], row_in.at[0], down),
    ]

    wait(sent)
    for k, v in enumerate(gather_sum(1, one, two_in, 32)):
        two[k] = v
    sent = scatter(2, two, three_in, 8)
    wait(sent)
    sums = gather_sum(2, two, three_in, 8)

    stats_out[...] = tile_sum[...]
    gain = probe_rate * SIDE * SIDE / jnp.sum(tile_sum[0])
    starts = []
    for g in range(2):
        a, b, c = (coords[axis] for axis in ORDERS[g])
        starts.append((a * 128, a * 128 + b * 32, a * 128 + b * 32 + c * 8))
    for k in range(MODES):
        at = pl.multiple_of(starts[k // 2][2], 8)
        probe_out[core, k, pl.ds(at, 8), :] = probe[core, k, pl.ds(at, 8), :] + gain * sums[k]

    def spread(phase, length):
        out = []
        for d in (2, 1, 3):
            for g in range(2):
                axis = ORDERS[g][phase]
                at = pl.multiple_of(starts[g][phase], length)
                block = probe_out.at[core, 2 * g:2 * g + 2, pl.ds(at, length), :]
                out.append(send(block, block, along(axis, (coords[axis] + d) % 4)))
        return out

    wait(spread(2, 8))
    out2 = spread(1, 32)

    def finish_rows():
        wait(rows_sent)
        has_up, has_down = row > 0, row < 7
        for p in range(2):
            for j in range(2):
                upper = jnp.where(has_up, row_in[0, p, j], 0.0)
                lower = jnp.where(has_down, row_in[1, p, j], 0.0)
                top = mid[p, j, 0:SIDE, :] + upper
                low = mid[p, j, SIDE:EXT, :] + lower
                old = obj[p, 1 + j]
                obj_out[p, 1 + j, 0:HALF, :] = old[0:HALF] + jnp.where(has_up, rate, 0.0) * top[0:HALF]
                obj_out[p, 1 + j, HALF:SIDE, :] = old[HALF:SIDE] + rate * top[HALF:SIDE]
                obj_out[p, 1 + j, SIDE:SIDE + HALF, :] = old[SIDE:SIDE + HALF] + rate * low[0:HALF]
                obj_out[p, 1 + j, SIDE + HALF:EXT, :] = (
                    old[SIDE + HALF:EXT] + jnp.where(has_down, rate, 0.0) * low[HALF:SIDE]
                )

    wait(out2)
    out1 = spread(0, 128)
    finish_rows()
    halo = []
    if not last:
        halo = [
            send(obj_out.at[:, 2], col_in.at[2], right),
            send(obj_out.at[:, 1], col_in.at[3], left),
        ]
    wait(out1)
    planes = probe_out.at[core]
    wait([send(planes, planes, partner)])
    if last:
        for p in range(2):
            obj_out[p, 0] = obj[p, 0]
            obj_out[p, 3] = obj[p, 3]
    else:
        wait(halo)
        for p in range(2):
            obj_out[p, 0] = jnp.where(has_left, col_in[2, p], 0.0)
            obj_out[p, 3] = jnp.where(has_right, col_in[3, p], 0.0)


def exchange(last, obj, probe, grad, pgrad, stats):
    whole = pl.BlockSpec(memory_space=pltpu.VMEM)
    messages = 64
    return pl.pallas_call(
        functools.partial(exchange_body, last),
        out_shape=(
            jax.ShapeDtypeStruct((2, 4, EXT, 128), F32),
            jax.ShapeDtypeStruct((2, MODES, EXT, 128), F32),
            jax.ShapeDtypeStruct((2, 8, 128), F32),
        ),
        in_specs=[whole] * 5,
        out_specs=(whole,) * 3,
        scratch_shapes=[
            pltpu.VMEM((MODES, EXT, 128), F32),
            pltpu.VMEM((MODES, EXT, 128), F32),
            pltpu.VMEM((3, MODES, 128, 128), F32),
            pltpu.VMEM((MODES, 128, 128), F32),
            pltpu.VMEM((3, MODES, 32, 128), F32),
            pltpu.VMEM((MODES, 32, 128), F32),
            pltpu.VMEM((3, MODES, 8, 128), F32),
            pltpu.VMEM((3, 3, 2, 8, 128), F32),
            pltpu.VMEM((2, 8, 128), F32),
            pltpu.VMEM((2, 8, 128), F32),
            pltpu.VMEM((4, 2, EXT, 128), F32),
            pltpu.VMEM((2, 2, 2, SIDE, 128), F32),
            pltpu.VMEM((2, 2, EXT, 128), F32),
            pltpu.SemaphoreType.DMA((messages,)),
            pltpu.SemaphoreType.DMA((messages,)),
        ],
        cost_estimate=pl.CostEstimate(flops=40 << 20, bytes_accessed=12 << 20, transcendentals=0),
        compiler_params=pltpu.CompilerParams(
            collective_id=1 if last else 0, has_side_effects=True, vmem_limit_bytes=48 << 20
        ),
        name="exchange_last" if last else "exchange",
    )(obj, probe, grad, pgrad, stats)


def padded(array, sides, width):
    for axis, dim in sides:
        devices, length = (lax.axis_size(axis), array.shape[dim])
        up = [(i, (i + 1) % devices) for i in range(devices - 1)]
        down = [(j, i) for i, j in up]
        last = lax.slice_in_dim(array, length - width, length, axis=dim)
        leading = lax.slice_in_dim(array, 0, width, axis=dim)
        before = lax.ppermute(last, axis, up)
        after = lax.ppermute(leading, axis, down)
        array = jnp.concatenate([before, array, after], axis=dim)
    return array


def on_device(object_field, probe, pos_rows, pos_cols, counts, magnitudes):
    tables = tuple(jnp.asarray(t) for t in transform_tables())
    rows, cols, live = pos_rows.reshape(-1), pos_cols.reshape(-1), counts.reshape(-1)
    extended = padded(object_field, ((ROW, 1), (COL, 2)), HALF)
    obj = extended.reshape(2, EXT, 4, 128).transpose(0, 2, 1, 3)
    planes = probe.reshape(2, MODES, SIDE, 2, 128).transpose(0, 1, 3, 2, 4)
    planes = planes.reshape(2, MODES, EXT, 128)
    misfits = []
    for update in range(ITERS * BATCHES):
        batch = update % BATCHES
        grad, pgrad, stats = position_work(batch, rows, cols, live, obj, planes, magnitudes, tables)
        last = update == ITERS * BATCHES - 1
        obj, planes, totals = exchange(last, obj, planes, grad, pgrad, stats)
        misfits.append(jnp.sum(totals[1]))
    out = obj[:, 1:3, HALF:HALF + SIDE, :].transpose(0, 2, 1, 3).reshape(2, SIDE, SIDE)
    probe_out = planes.reshape(2, MODES, 2, SIDE, 128).transpose(0, 1, 3, 2, 4)
    return (out, probe_out.reshape(2, MODES, SIDE, SIDE), jnp.stack(misfits))


def solution(mesh):
    finer = Mesh(mesh.devices.reshape(4, 2, 4, 2, 2), AXES)
    return jax.shard_map(
        on_device,
        mesh=finer,
        in_specs=(
            P(None, ROW, COL),
            P(),
            P(ROW, COL, None, None),
            P(ROW, COL, None, None),
            P(ROW, COL, None),
            P(ROW, COL, None, None, None, None),
        ),
        out_specs=(P(None, ROW, COL), P(), P()),
        check_vma=False,
    )
```

```python
import functools
import math

import jax
import jax.numpy as jnp
import numpy as np
from jax import lax
from jax.experimental import pallas as pl
from jax.experimental.pallas import tpu as pltpu
from jax.sharding import Mesh
from jax.sharding import PartitionSpec as P

BATCHES = 2
ITERS = 2
SLOTS = 3
MODES = 4
SIDE = 256
HALF = 128
EXT = 512
AXES = ("row_0", "row_1", "col_0", "col_1", "col_2")
ROW = ("row_0", "row_1")
COL = ("col_0", "col_1", "col_2")
F32 = jnp.float32
BF16 = jnp.bfloat16

object_rate = 0.9
probe_rate = 0.5
floor_value = 0.5
tiny_value = 1e-06


def transform_tables():
    index = np.arange(SIDE)
    angles = (index[:, None] * index[None, :] % SIDE) * (2.0 * math.pi / SIDE)
    scale = 1.0 / math.sqrt(SIDE)
    c = np.cos(angles) * scale
    s = -np.sin(angles) * scale
    left = np.block([[c, -s], [s, c]])
    return left.astype(jnp.bfloat16), left.T.astype(jnp.bfloat16)


def compute_body(
    batch, rows_ref, cols_ref, counts_ref, obj, probe, mags, left_tab, right_tab,
    grad, pgrad, stats, win, wave, half, field,
):
    CH = 16
    steps = SIDE // CH
    lane = lax.broadcasted_iota(jnp.int32, (CH, 128), 1)

    grad[...] = jnp.zeros_like(grad)
    pgrad[...] = jnp.zeros_like(pgrad)
    stats[...] = jnp.zeros_like(stats)

    def fold(x):
        total = x[0:8, :]
        for i in range(1, x.shape[0] // 8):
            total = total + x[8 * i:8 * i + 8, :]
        return total

    def visit(slot, carry):
        row0 = rows_ref[batch * SLOTS + slot]
        col0 = cols_ref[batch * SLOTS + slot]
        block = lax.shift_right_logical(col0, 7)
        shift = col0 & 127
        back = (128 - shift) & 127

        def make_exit(i, c):
            at = pl.multiple_of(i * CH, CH)
            w = []
            for p in range(2):
                rolled = [
                    pltpu.roll(obj[p, block + j, pl.ds(row0 + at, CH), :], back, 1) for j in range(3)
                ]
                keep = lane < 128 - shift
                w.append([jnp.where(keep, rolled[j], rolled[j + 1]) for j in range(2)])
            power = jnp.zeros((8, 128), F32)
            for j in range(2):
                wr, wi = w[0][j], w[1][j]
                win[0, j, pl.ds(at, CH), :] = wr
                win[1, j, pl.ds(at, CH), :] = wi
                power = power + fold(wr * wr + wi * wi)
                for k in range(MODES):
                    pr = probe[0, k, pl.ds(j * SIDE + at, CH), :]
                    pi = probe[1, k, pl.ds(j * SIDE + at, CH), :]
                    wave[k, pl.ds(at, CH), j * 128:(j + 1) * 128] = (pr * wr - pi * wi).astype(BF16)
                    wave[k, pl.ds(SIDE + at, CH), j * 128:(j + 1) * 128] = (pr * wi + pi * wr).astype(BF16)
            stats[0] = stats[0] + power
            return c

        lax.fori_loop(0, steps, make_exit, 0)

        def transform(first, second):
            def left(k, c):
                res = jnp.dot(first[...], wave[k], preferred_element_type=F32).astype(BF16)
                at = pl.multiple_of(k * SIDE, SIDE)
                half[pl.ds(at, SIDE), 0:SIDE] = res[0:SIDE]
                half[pl.ds(at, SIDE), SIDE:EXT] = res[SIDE:EXT]
                return c

            lax.fori_loop(0, MODES, left, 0)

            def right(k, c):
                at = pl.multiple_of(k * 512, 512)
                field[pl.ds(at, 512), :] = jnp.dot(
                    half[pl.ds(at, 512), :], second[...], preferred_element_type=F32
                )
                return c

            lax.fori_loop(0, 2, right, 0)

        transform(left_tab, right_tab)

        def correct(i, c):
            at = pl.multiple_of(i * CH, CH)
            parts = [
                (field[pl.ds(k * SIDE + at, CH), 0:SIDE], field[pl.ds(k * SIDE + at, CH), SIDE:EXT])
                for k in range(MODES)
            ]
            total = sum(re * re + im * im for re, im in parts)
            modulus = jnp.sqrt(total)
            amplitude = mags[0, 0, 0, slot, pl.ds(at, CH), :]
            factor = amplitude / jnp.maximum(modulus, floor_value) - 1.0
            gap = modulus - amplitude
            gap = gap * gap
            stats[1] = stats[1] + fold(gap[:, 0:128]) + fold(gap[:, 128:256])
            for k in range(MODES):
                wave[k, pl.ds(at, CH), :] = (parts[k][0] * factor).astype(BF16)
                wave[k, pl.ds(SIDE + at, CH), :] = (parts[k][1] * factor).astype(BF16)
            return c

        lax.fori_loop(0, steps, correct, 0)
        transform(right_tab, left_tab)

        def spread(i, c):
            at = pl.multiple_of(i * CH, CH)
            term = [[None, None], [None, None]]
            for j in range(2):
                wr = win[0, j, pl.ds(at, CH), :]
                wi = win[1, j, pl.ds(at, CH), :]
                tr = ti = None
                for k in range(MODES):
                    ur = field[pl.ds(k * SIDE + at, CH), j * 128:(j + 1) * 128]
                    ui = field[pl.ds(k * SIDE + at, CH), SIDE + j * 128:SIDE + (j + 1) * 128]
                    spot = pl.ds(j * SIDE + at, CH)
                    pr = probe[0, k, spot, :]
                    pi = probe[1, k, spot, :]
                    ar = pr * ur + pi * ui
                    ai = pr * ui - pi * ur
                    tr = ar if tr is None else tr + ar
                    ti = ai if ti is None else ti + ai
                    pgrad[0, k, spot, :] = pgrad[0, k, spot, :] + (wr * ur + wi * ui)
                    pgrad[1, k, spot, :] = pgrad[1, k, spot, :] + (wr * ui - wi * ur)
                term[0][j], term[1][j] = tr, ti
            low = lane < shift
            zero = jnp.zeros((CH, 128), F32)
            for p in range(2):
                a = pltpu.roll(term[p][0], shift, 1)
                b = pltpu.roll(term[p][1], shift, 1)
                adds = (jnp.where(low, zero, a), jnp.where(low, a, b), jnp.where(low, b, zero))
                for j in range(3):
                    spot = pl.ds(row0 + at, CH)
                    grad[p, block + j, spot, :] = grad[p, block + j, spot, :] + adds[j]
            return c

        lax.fori_loop(0, steps, spread, 0)
        return carry

    lax.fori_loop(0, counts_ref[batch], visit, 0)


def position_work(batch, pos_rows, pos_cols, counts, obj, probe, magnitudes, tables):
    whole = pl.BlockSpec(memory_space=pltpu.VMEM)
    smem = pl.BlockSpec(memory_space=pltpu.SMEM)
    mags = pl.BlockSpec((1, 1, 1, SLOTS, SIDE, SIDE), lambda i: (0, 0, batch, 0, 0, 0))
    flops = SLOTS * 2 * 2 * MODES * 4 * 2 * SIDE ** 3
    return pl.pallas_call(
        functools.partial(compute_body, batch),
        grid=(1,),
        out_shape=(
            jax.ShapeDtypeStruct((2, 4, EXT, 128), F32),
            jax.ShapeDtypeStruct((2, MODES, EXT, 128), F32),
            jax.ShapeDtypeStruct((2, 8, 128), F32),
        ),
        in_specs=[smem, smem, smem, whole, whole, mags, whole, whole],
        out_specs=(whole, whole, whole),
        scratch_shapes=[
            pltpu.VMEM((2, 2, SIDE, 128), F32),
            pltpu.VMEM((MODES, EXT, SIDE), BF16),
            pltpu.VMEM((MODES * SIDE, EXT), BF16),
            pltpu.VMEM((MODES * SIDE, EXT), F32),
        ],
        cost_estimate=pl.CostEstimate(flops=flops, bytes_accessed=12 << 20, transcendentals=0),
        compiler_params=pltpu.CompilerParams(vmem_limit_bytes=56 << 20),
        name="position_work",
    )(pos_rows, pos_cols, counts, obj, probe, magnitudes, *tables)


def where_am_i():
    y, lo, x, hi, core = (lax.axis_index(name) for name in AXES)
    row, col = y * 2 + lo, x * 4 + hi * 2 + core
    z = hi * 2 + lo

    def tile(r, c):
        return (r // 2, r % 2, c // 4, (c // 2) % 2, c % 2)

    def along(axis, value):
        if axis == "x":
            return (y, lo, value, hi, core)
        if axis == "y":
            return (value, lo, x, hi, core)
        return (y, value % 2, x, value // 2, core)

    partner = (y, lo, x, hi, 1 - core)
    coords = {"x": x, "y": y, "z": z}
    return row, col, core, coords, along, partner, tile


ORDERS = (("x", "y", "z"), ("y", "x", "z"))


def exchange_body(
    last, obj, probe, grad, pgrad, stats, obj_out, probe_out, stats_out,
    core_in, acc, one_in, one, two_in, z_in, tile_in, tile_z, tile_core,
    col_in, row_in, mid, rdma_send, rdma_recv,
):
    row, col, core, coords, along, partner, tile = where_am_i()
    up, down = tile((row + 7) % 8, col), tile((row + 1) % 8, col)
    left, right = tile(row, (col + 15) % 16), tile(row, (col + 1) % 16)
    has_left, has_right, has_up, has_down = col > 0, col < 15, row > 0, row < 7

    barrier = pltpu.get_barrier_semaphore()
    greeted = [partner, up, down, left, right]
    for axis in ("x", "y", "z"):
        for d in (1, 2, 3):
            greeted.append(along(axis, (coords[axis] + d) % 4))
    for peer in greeted:
        pl.semaphore_signal(barrier, inc=1, device_id=peer, device_id_type=pl.DeviceIdType.MESH)
    pl.semaphore_wait(barrier, len(greeted))

    count = [0]

    def send(src, dst, peer):
        n = count[0]
        count[0] += 1
        copy = pltpu.make_async_remote_copy(
            src_ref=src, dst_ref=dst, send_sem=rdma_send.at[n], recv_sem=rdma_recv.at[n],
            device_id=peer, device_id_type=pl.DeviceIdType.MESH,
        )
        copy.start()
        return copy

    def wait(copies):
        for copy in copies:
            copy.wait()

    core_sent = [
        send(stats, tile_core, partner),
        send(pgrad.at[1 - core], core_in, partner),
    ]
    cols_sent = [
        [send(grad.at[p, 3], col_in.at[0, p], right), send(grad.at[p, 0], col_in.at[1, p], left)]
        for p in range(2)
    ]

    def peak_step(i, best):
        at = pl.multiple_of(i * 16, 16)
        total = None
        for p in range(2):
            for k in range(MODES):
                v = probe[p, k, pl.ds(at, 16), :]
                total = v * v if total is None else total + v * v
        return jnp.maximum(best, jnp.maximum(total[0:8], total[8:16]))

    best = lax.fori_loop(0, EXT // 16, peak_step, jnp.zeros((8, 128), F32))
    rate = object_rate / (jnp.max(best) + tiny_value)

    def scatter(phase, source, landing, length, tile_value):
        me = coords[ORDERS[0][phase]]
        tile_in[phase, me] = tile_value
        slot = tile_in.at[phase, me]
        sent = []
        for d in (2, 1, 3):
            sent.append(send(slot, slot, along(ORDERS[0][phase], (me + d) % 4)))
            for g in range(2):
                axis = ORDERS[g][phase]
                to = (coords[axis] + d) % 4
                at = pl.multiple_of(to * length, length)
                sent.append(
                    send(
                        source.at[2 * g:2 * g + 2, pl.ds(at, length), :],
                        landing.at[d - 1, 2 * g:2 * g + 2],
                        along(axis, to),
                    )
                )
        return sent

    def gather_sum(phase, source, landing, length):
        out = []
        for g in range(2):
            at = pl.multiple_of(coords[ORDERS[g][phase]] * length, length)
            for k in (2 * g, 2 * g + 1):
                out.append(
                    source[k, pl.ds(at, length), :] + landing[0, k] + landing[1, k] + landing[2, k]
                )
        return out

    def tile_total(phase):
        return (tile_in[phase, 0] + tile_in[phase, 1]) + (tile_in[phase, 2] + tile_in[phase, 3])

    def send_rows(p, j):
        return [
            send(mid.at[p, j, 0:SIDE, :], row_in.at[1, p, j], up),
            send(mid.at[p, j, SIDE:EXT, :], row_in.at[0, p, j], down),
        ]

    def make_mid(p):
        wait(cols_sent[p])
        mid[p, 0] = grad[p, 1] + jnp.where(has_left, col_in[0, p], 0.0)
        mid[p, 1] = grad[p, 2] + jnp.where(has_right, col_in[1, p], 0.0)

    def update_object(p, j):
        upper = jnp.where(has_up, row_in[0, p, j], 0.0)
        lower = jnp.where(has_down, row_in[1, p, j], 0.0)
        top = mid[p, j, 0:SIDE, :] + upper
        low = mid[p, j, SIDE:EXT, :] + lower
        old = obj[p, 1 + j]
        obj_out[p, 1 + j, 0:HALF, :] = old[0:HALF] + jnp.where(has_up, rate, 0.0) * top[0:HALF]
        obj_out[p, 1 + j, HALF:SIDE, :] = old[HALF:SIDE] + rate * top[HALF:SIDE]
        obj_out[p, 1 + j, SIDE:SIDE + HALF, :] = old[SIDE:SIDE + HALF] + rate * low[0:HALF]
        obj_out[p, 1 + j, SIDE + HALF:EXT, :] = (
            old[SIDE + HALF:EXT] + jnp.where(has_down, rate, 0.0) * low[HALF:SIDE]
        )

    def send_halo(p):
        if last:
            return []
        return [
            send(obj_out.at[p, 2], col_in.at[2, p], right),
            send(obj_out.at[p, 1], col_in.at[3, p], left),
        ]

    wait(core_sent)
    for k in range(MODES):
        acc[k] = pgrad[core, k] + core_in[k]
    sent = scatter(0, acc, one_in, 128, stats[...] + tile_core[...])

    make_mid(0)
    rows_sent = [send_rows(0, 0), send_rows(0, 1)]

    wait(sent)
    for k, v in enumerate(gather_sum(0, acc, one_in, 128)):
        one[k] = v
    sent = scatter(1, one, two_in, 32, tile_total(0))

    make_mid(1)

    wait(sent)
    z = coords["z"]
    for k, v in enumerate(gather_sum(1, one, two_in, 32)):
        z_in[z, k] = v
    tile_z[z] = tile_total(1)
    sent = []
    for d in (2, 1, 3):
        peer = along("z", (z + d) % 4)
        sent.append(send(tile_z.at[z], tile_z.at[z], peer))
        sent.append(send(z_in.at[z], z_in.at[z], peer))
    rows_sent.append(send_rows(1, 0))
    wait(sent)

    totals = (tile_z[0] + tile_z[1]) + (tile_z[2] + tile_z[3])
    stats_out[...] = totals
    gain = probe_rate * SIDE * SIDE / jnp.sum(totals[0])
    starts = []
    for g in range(2):
        a, b = coords[ORDERS[g][0]], coords[ORDERS[g][1]]
        starts.append((a * 128, a * 128 + b * 32))
    for k in range(MODES):
        spot = pl.ds(pl.multiple_of(starts[k // 2][1], 32), 32)
        total = (z_in[0, k] + z_in[1, k]) + (z_in[2, k] + z_in[3, k])
        probe_out[core, k, spot, :] = probe[core, k, spot, :] + gain * total

    def block_of(g, at, length):
        at = pl.multiple_of(at, length)
        return probe_out.at[core, 2 * g:2 * g + 2, pl.ds(at, length), :]

    def spread(phase, length):
        out = {}
        for d in (2, 1, 3):
            for g in range(2):
                axis = ORDERS[g][phase]
                block = block_of(g, starts[g][phase], length)
                out[d, g] = send(block, block, along(axis, (coords[axis] + d) % 4))
        return out

    out2 = spread(1, 32)
    rows_sent.append(send_rows(1, 1))
    wait(out2.values())
    out1 = spread(0, 128)
    to_core = []
    for g in range(2):
        block = block_of(g, starts[g][0], 128)
        to_core.append(send(block, block, partner))

    wait(rows_sent[0] + rows_sent[1])
    for j in range(2):
        update_object(0, j)
    halo = send_halo(0)

    for d in (1, 3, 2):
        for g in range(2):
            out1[d, g].wait()
            axis = ORDERS[g][0]
            block = block_of(g, (coords[axis] + 4 - d) % 4 * 128, 128)
            to_core.append(send(block, block, partner))

    wait(rows_sent[2] + rows_sent[3])
    for j in range(2):
        update_object(1, j)
    halo += send_halo(1)
    wait(to_core)
    if last:
        for p in range(2):
            obj_out[p, 0] = obj[p, 0]
            obj_out[p, 3] = obj[p, 3]
    else:
        wait(halo)
        for p in range(2):
            obj_out[p, 0] = jnp.where(has_left, col_in[2, p], 0.0)
            obj_out[p, 3] = jnp.where(has_right, col_in[3, p], 0.0)


def exchange(last, obj, probe, grad, pgrad, stats):
    whole = pl.BlockSpec(memory_space=pltpu.VMEM)
    messages = 72
    return pl.pallas_call(
        functools.partial(exchange_body, last),
        out_shape=(
            jax.ShapeDtypeStruct((2, 4, EXT, 128), F32),
            jax.ShapeDtypeStruct((2, MODES, EXT, 128), F32),
            jax.ShapeDtypeStruct((2, 8, 128), F32),
        ),
        in_specs=[whole] * 5,
        out_specs=(whole,) * 3,
        scratch_shapes=[
            pltpu.VMEM((MODES, EXT, 128), F32),
            pltpu.VMEM((MODES, EXT, 128), F32),
            pltpu.VMEM((3, MODES, 128, 128), F32),
            pltpu.VMEM((MODES, 128, 128), F32),
            pltpu.VMEM((3, MODES, 32, 128), F32),
            pltpu.VMEM((4, MODES, 32, 128), F32),
            pltpu.VMEM((2, 4, 2, 8, 128), F32),
            pltpu.VMEM((4, 2, 8, 128), F32),
            pltpu.VMEM((2, 8, 128), F32),
            pltpu.VMEM((4, 2, EXT, 128), F32),
            pltpu.VMEM((2, 2, 2, SIDE, 128), F32),
            pltpu.VMEM((2, 2, EXT, 128), F32),
            pltpu.SemaphoreType.DMA((messages,)),
            pltpu.SemaphoreType.DMA((messages,)),
        ],
        cost_estimate=pl.CostEstimate(flops=40 << 20, bytes_accessed=12 << 20, transcendentals=0),
        compiler_params=pltpu.CompilerParams(
            collective_id=1 if last else 0, has_side_effects=True, vmem_limit_bytes=48 << 20
        ),
        name="exchange_last" if last else "exchange",
    )(obj, probe, grad, pgrad, stats)


def padded(array, sides, width):
    for axis, dim in sides:
        devices, length = (lax.axis_size(axis), array.shape[dim])
        up = [(i, (i + 1) % devices) for i in range(devices - 1)]
        down = [(j, i) for i, j in up]
        last = lax.slice_in_dim(array, length - width, length, axis=dim)
        leading = lax.slice_in_dim(array, 0, width, axis=dim)
        before = lax.ppermute(last, axis, up)
        after = lax.ppermute(leading, axis, down)
        array = jnp.concatenate([before, array, after], axis=dim)
    return array


def on_device(object_field, probe, pos_rows, pos_cols, counts, magnitudes):
    tables = tuple(jnp.asarray(t) for t in transform_tables())
    rows, cols, live = pos_rows.reshape(-1), pos_cols.reshape(-1), counts.reshape(-1)
    extended = padded(object_field, ((ROW, 1), (COL, 2)), HALF)
    obj = extended.reshape(2, EXT, 4, 128).transpose(0, 2, 1, 3)
    planes = probe.reshape(2, MODES, SIDE, 2, 128).transpose(0, 1, 3, 2, 4)
    planes = planes.reshape(2, MODES, EXT, 128)
    misfits = []
    for update in range(ITERS * BATCHES):
        batch = update % BATCHES
        grad, pgrad, stats = position_work(batch, rows, cols, live, obj, planes, magnitudes, tables)
        last = update == ITERS * BATCHES - 1
        obj, planes, totals = exchange(last, obj, planes, grad, pgrad, stats)
        misfits.append(jnp.sum(totals[1]))
    out = obj[:, 1:3, HALF:HALF + SIDE, :].transpose(0, 2, 1, 3).reshape(2, SIDE, SIDE)
    probe_out = planes.reshape(2, MODES, 2, SIDE, 128).transpose(0, 1, 3, 2, 4)
    return (out, probe_out.reshape(2, MODES, SIDE, SIDE), jnp.stack(misfits))


def solution(mesh):
    finer = Mesh(mesh.devices.reshape(4, 2, 4, 2, 2), AXES)
    return jax.shard_map(
        on_device,
        mesh=finer,
        in_specs=(
            P(None, ROW, COL),
            P(),
            P(ROW, COL, None, None),
            P(ROW, COL, None, None),
            P(ROW, COL, None),
            P(ROW, COL, None, None, None, None),
        ),
        out_specs=(P(None, ROW, COL), P(), P()),
        check_vma=False,
    )
```

```python
import functools
import math

import jax
import jax.numpy as jnp
import numpy as np
from jax import lax
from jax.experimental import pallas as pl
from jax.experimental.pallas import tpu as pltpu
from jax.sharding import Mesh
from jax.sharding import PartitionSpec as P

BATCHES = 2
ITERS = 2
SLOTS = 3
MODES = 4
SIDE = 256
HALF = 128
EXT = 512
AXES = ("row_0", "row_1", "col_0", "col_1", "col_2")
ROW = ("row_0", "row_1")
COL = ("col_0", "col_1", "col_2")
F32 = jnp.float32
BF16 = jnp.bfloat16

object_rate = 0.9
probe_rate = 0.5
floor_value = 0.5
tiny_value = 1e-06


def transform_tables():
    index = np.arange(SIDE)
    angles = (index[:, None] * index[None, :] % SIDE) * (2.0 * math.pi / SIDE)
    scale = 1.0 / math.sqrt(SIDE)
    c = np.cos(angles) * scale
    s = -np.sin(angles) * scale
    left = np.block([[c, -s], [s, c]])
    return left.astype(jnp.bfloat16), left.T.astype(jnp.bfloat16)


def compute_body(
    batch, rows_ref, cols_ref, counts_ref, obj, probe, mags, left_tab, right_tab,
    grad, pgrad, stats, win, wave, half, field,
):
    CH = 16
    steps = SIDE // CH
    lane = lax.broadcasted_iota(jnp.int32, (CH, 128), 1)

    grad[...] = jnp.zeros_like(grad)
    pgrad[...] = jnp.zeros_like(pgrad)
    stats[...] = jnp.zeros_like(stats)

    def fold(x):
        total = x[0:8, :]
        for i in range(1, x.shape[0] // 8):
            total = total + x[8 * i:8 * i + 8, :]
        return total

    def visit(slot, carry):
        row0 = rows_ref[batch * SLOTS + slot]
        col0 = cols_ref[batch * SLOTS + slot]
        block = lax.shift_right_logical(col0, 7)
        shift = col0 & 127
        back = (128 - shift) & 127

        def make_exit(i, c):
            at = pl.multiple_of(i * CH, CH)
            w = []
            for p in range(2):
                rolled = [
                    pltpu.roll(obj[p, block + j, pl.ds(row0 + at, CH), :], back, 1) for j in range(3)
                ]
                keep = lane < 128 - shift
                w.append([jnp.where(keep, rolled[j], rolled[j + 1]) for j in range(2)])
            power = jnp.zeros((8, 128), F32)
            for j in range(2):
                wr, wi = w[0][j], w[1][j]
                win[0, j, pl.ds(at, CH), :] = wr
                win[1, j, pl.ds(at, CH), :] = wi
                power = power + fold(wr * wr + wi * wi)
                for k in range(MODES):
                    pr = probe[0, k, pl.ds(j * SIDE + at, CH), :]
                    pi = probe[1, k, pl.ds(j * SIDE + at, CH), :]
                    wave[k, pl.ds(at, CH), j * 128:(j + 1) * 128] = (pr * wr - pi * wi).astype(BF16)
                    wave[k, pl.ds(SIDE + at, CH), j * 128:(j + 1) * 128] = (pr * wi + pi * wr).astype(BF16)
            stats[0] = stats[0] + power
            return c

        lax.fori_loop(0, steps, make_exit, 0, unroll=4)

        def transform(first, second):
            def left(k, c):
                res = jnp.dot(first[...], wave[k], preferred_element_type=F32).astype(BF16)
                at = k * SIDE
                half[pl.ds(at, SIDE), 0:SIDE] = res[0:SIDE]
                half[pl.ds(at, SIDE), SIDE:EXT] = res[SIDE:EXT]
                return c

            for k in range(MODES):
                left(k, 0)

            def right(k, c):
                at = pl.multiple_of(k * 512, 512)
                field[pl.ds(at, 512), :] = jnp.dot(
                    half[pl.ds(at, 512), :], second[...], preferred_element_type=F32
                )
                return c

            field[...] = jnp.dot(half[...], second[...], preferred_element_type=F32)

        transform(left_tab, right_tab)

        def correct(i, c):
            at = pl.multiple_of(i * CH, CH)
            parts = [
                (field[pl.ds(k * SIDE + at, CH), 0:SIDE], field[pl.ds(k * SIDE + at, CH), SIDE:EXT])
                for k in range(MODES)
            ]
            total = sum(re * re + im * im for re, im in parts)
            modulus = jnp.sqrt(total)
            amplitude = mags[0, 0, 0, slot, pl.ds(at, CH), :]
            factor = amplitude / jnp.maximum(modulus, floor_value) - 1.0
            gap = modulus - amplitude
            gap = gap * gap
            stats[1] = stats[1] + fold(gap[:, 0:128]) + fold(gap[:, 128:256])
            for k in range(MODES):
                wave[k, pl.ds(at, CH), :] = (parts[k][0] * factor).astype(BF16)
                wave[k, pl.ds(SIDE + at, CH), :] = (parts[k][1] * factor).astype(BF16)
            return c

        lax.fori_loop(0, steps, correct, 0, unroll=4)
        transform(right_tab, left_tab)

        def spread(i, c):
            at = pl.multiple_of(i * CH, CH)
            term = [[None, None], [None, None]]
            for j in range(2):
                wr = win[0, j, pl.ds(at, CH), :]
                wi = win[1, j, pl.ds(at, CH), :]
                tr = ti = None
                for k in range(MODES):
                    ur = field[pl.ds(k * SIDE + at, CH), j * 128:(j + 1) * 128]
                    ui = field[pl.ds(k * SIDE + at, CH), SIDE + j * 128:SIDE + (j + 1) * 128]
                    spot = pl.ds(j * SIDE + at, CH)
                    pr = probe[0, k, spot, :]
                    pi = probe[1, k, spot, :]
                    ar = pr * ur + pi * ui
                    ai = pr * ui - pi * ur
                    tr = ar if tr is None else tr + ar
                    ti = ai if ti is None else ti + ai
                    pgrad[0, k, spot, :] = pgrad[0, k, spot, :] + (wr * ur + wi * ui)
                    pgrad[1, k, spot, :] = pgrad[1, k, spot, :] + (wr * ui - wi * ur)
                term[0][j], term[1][j] = tr, ti
            low = lane < shift
            zero = jnp.zeros((CH, 128), F32)
            for p in range(2):
                a = pltpu.roll(term[p][0], shift, 1)
                b = pltpu.roll(term[p][1], shift, 1)
                adds = (jnp.where(low, zero, a), jnp.where(low, a, b), jnp.where(low, b, zero))
                for j in range(3):
                    spot = pl.ds(row0 + at, CH)
                    grad[p, block + j, spot, :] = grad[p, block + j, spot, :] + adds[j]
            return c

        lax.fori_loop(0, steps, spread, 0, unroll=4)
        return carry

    lax.fori_loop(0, counts_ref[batch], visit, 0)


def position_work(batch, pos_rows, pos_cols, counts, obj, probe, magnitudes, tables):
    whole = pl.BlockSpec(memory_space=pltpu.VMEM)
    smem = pl.BlockSpec(memory_space=pltpu.SMEM)
    mags = pl.BlockSpec((1, 1, 1, SLOTS, SIDE, SIDE), lambda i: (0, 0, batch, 0, 0, 0))
    flops = SLOTS * 2 * 2 * MODES * 4 * 2 * SIDE ** 3
    return pl.pallas_call(
        functools.partial(compute_body, batch),
        grid=(1,),
        out_shape=(
            jax.ShapeDtypeStruct((2, 4, EXT, 128), F32),
            jax.ShapeDtypeStruct((2, MODES, EXT, 128), F32),
            jax.ShapeDtypeStruct((2, 8, 128), F32),
        ),
        in_specs=[smem, smem, smem, whole, whole, mags, whole, whole],
        out_specs=(whole, whole, whole),
        scratch_shapes=[
            pltpu.VMEM((2, 2, SIDE, 128), F32),
            pltpu.VMEM((MODES, EXT, SIDE), BF16),
            pltpu.VMEM((MODES * SIDE, EXT), BF16),
            pltpu.VMEM((MODES * SIDE, EXT), F32),
        ],
        cost_estimate=pl.CostEstimate(flops=flops, bytes_accessed=12 << 20, transcendentals=0),
        compiler_params=pltpu.CompilerParams(vmem_limit_bytes=56 << 20),
        name="position_work",
    )(pos_rows, pos_cols, counts, obj, probe, magnitudes, *tables)


def where_am_i():
    y, lo, x, hi, core = (lax.axis_index(name) for name in AXES)
    row, col = y * 2 + lo, x * 4 + hi * 2 + core
    z = hi * 2 + lo

    def tile(r, c):
        return (r // 2, r % 2, c // 4, (c // 2) % 2, c % 2)

    def along(axis, value):
        if axis == "x":
            return (y, lo, value, hi, core)
        if axis == "y":
            return (value, lo, x, hi, core)
        return (y, value % 2, x, value // 2, core)

    partner = (y, lo, x, hi, 1 - core)
    coords = {"x": x, "y": y, "z": z}
    return row, col, core, coords, along, partner, tile


ORDERS = (("x", "y", "z"), ("y", "x", "z"))


def exchange_body(
    last, obj, probe, grad, pgrad, stats, obj_out, probe_out, stats_out,
    core_in, acc, one_in, one, two_in, z_in, tile_in, tile_z, tile_core,
    col_in, row_in, mid, rdma_send, rdma_recv,
):
    row, col, core, coords, along, partner, tile = where_am_i()
    up, down = tile((row + 7) % 8, col), tile((row + 1) % 8, col)
    left, right = tile(row, (col + 15) % 16), tile(row, (col + 1) % 16)
    has_left, has_right, has_up, has_down = col > 0, col < 15, row > 0, row < 7

    barrier = pltpu.get_barrier_semaphore()
    greeted = [partner, up, down, left, right]
    for axis in ("x", "y", "z"):
        for d in (1, 2, 3):
            greeted.append(along(axis, (coords[axis] + d) % 4))
    for peer in greeted:
        pl.semaphore_signal(barrier, inc=1, device_id=peer, device_id_type=pl.DeviceIdType.MESH)
    pl.semaphore_wait(barrier, len(greeted))

    count = [0]

    def send(src, dst, peer):
        n = count[0]
        count[0] += 1
        copy = pltpu.make_async_remote_copy(
            src_ref=src, dst_ref=dst, send_sem=rdma_send.at[n], recv_sem=rdma_recv.at[n],
            device_id=peer, device_id_type=pl.DeviceIdType.MESH,
        )
        copy.start()
        return copy

    def wait(copies):
        for copy in copies:
            copy.wait()

    core_sent = [
        send(stats, tile_core, partner),
        send(pgrad.at[1 - core], core_in, partner),
    ]
    cols_sent = [
        [send(grad.at[p, 3], col_in.at[0, p], right), send(grad.at[p, 0], col_in.at[1, p], left)]
        for p in range(2)
    ]

    def peak_step(i, best):
        at = pl.multiple_of(i * 16, 16)
        total = None
        for p in range(2):
            for k in range(MODES):
                v = probe[p, k, pl.ds(at, 16), :]
                total = v * v if total is None else total + v * v
        return jnp.maximum(best, jnp.maximum(total[0:8], total[8:16]))

    best = lax.fori_loop(0, EXT // 16, peak_step, jnp.zeros((8, 128), F32))
    rate = object_rate / (jnp.max(best) + tiny_value)

    def scatter(phase, source, landing, length, tile_value):
        me = coords[ORDERS[0][phase]]
        tile_in[phase, me] = tile_value
        slot = tile_in.at[phase, me]
        sent = []
        for d in (2, 1, 3):
            sent.append(send(slot, slot, along(ORDERS[0][phase], (me + d) % 4)))
            for g in range(2):
                axis = ORDERS[g][phase]
                to = (coords[axis] + d) % 4
                at = pl.multiple_of(to * length, length)
                sent.append(
                    send(
                        source.at[2 * g:2 * g + 2, pl.ds(at, length), :],
                        landing.at[d - 1, 2 * g:2 * g + 2],
                        along(axis, to),
                    )
                )
        return sent

    def gather_sum(phase, source, landing, length):
        out = []
        for g in range(2):
            at = pl.multiple_of(coords[ORDERS[g][phase]] * length, length)
            for k in (2 * g, 2 * g + 1):
                out.append(
                    source[k, pl.ds(at, length), :] + landing[0, k] + landing[1, k] + landing[2, k]
                )
        return out

    def tile_total(phase):
        return (tile_in[phase, 0] + tile_in[phase, 1]) + (tile_in[phase, 2] + tile_in[phase, 3])

    def send_rows(p, j):
        return [
            send(mid.at[p, j, 0:SIDE, :], row_in.at[1, p, j], up),
            send(mid.at[p, j, SIDE:EXT, :], row_in.at[0, p, j], down),
        ]

    def make_mid(p):
        wait(cols_sent[p])
        mid[p, 0] = grad[p, 1] + jnp.where(has_left, col_in[0, p], 0.0)
        mid[p, 1] = grad[p, 2] + jnp.where(has_right, col_in[1, p], 0.0)

    def update_object(p, j):
        upper = jnp.where(has_up, row_in[0, p, j], 0.0)
        lower = jnp.where(has_down, row_in[1, p, j], 0.0)
        top = mid[p, j, 0:SIDE, :] + upper
        low = mid[p, j, SIDE:EXT, :] + lower
        old = obj[p, 1 + j]
        obj_out[p, 1 + j, 0:HALF, :] = old[0:HALF] + jnp.where(has_up, rate, 0.0) * top[0:HALF]
        obj_out[p, 1 + j, HALF:SIDE, :] = old[HALF:SIDE] + rate * top[HALF:SIDE]
        obj_out[p, 1 + j, SIDE:SIDE + HALF, :] = old[SIDE:SIDE + HALF] + rate * low[0:HALF]
        obj_out[p, 1 + j, SIDE + HALF:EXT, :] = (
            old[SIDE + HALF:EXT] + jnp.where(has_down, rate, 0.0) * low[HALF:SIDE]
        )

    def send_halo(p):
        if last:
            return []
        return [
            send(obj_out.at[p, 2], col_in.at[2, p], right),
            send(obj_out.at[p, 1], col_in.at[3, p], left),
        ]

    wait(core_sent)
    for k in range(MODES):
        acc[k] = pgrad[core, k] + core_in[k]
    sent = scatter(0, acc, one_in, 128, stats[...] + tile_core[...])

    make_mid(0)
    rows_sent = [send_rows(0, 0), send_rows(0, 1)]

    wait(sent)
    for k, v in enumerate(gather_sum(0, acc, one_in, 128)):
        one[k] = v
    sent = scatter(1, one, two_in, 32, tile_total(0))

    make_mid(1)

    wait(sent)
    z = coords["z"]
    for k, v in enumerate(gather_sum(1, one, two_in, 32)):
        z_in[z, k] = v
    tile_z[z] = tile_total(1)
    sent = []
    for d in (2, 1, 3):
        peer = along("z", (z + d) % 4)
        sent.append(send(tile_z.at[z], tile_z.at[z], peer))
        sent.append(send(z_in.at[z], z_in.at[z], peer))
    rows_sent.append(send_rows(1, 0))
    wait(sent)

    totals = (tile_z[0] + tile_z[1]) + (tile_z[2] + tile_z[3])
    stats_out[...] = totals
    gain = probe_rate * SIDE * SIDE / jnp.sum(totals[0])
    starts = []
    for g in range(2):
        a, b = coords[ORDERS[g][0]], coords[ORDERS[g][1]]
        starts.append((a * 128, a * 128 + b * 32))
    for k in range(MODES):
        spot = pl.ds(pl.multiple_of(starts[k // 2][1], 32), 32)
        total = (z_in[0, k] + z_in[1, k]) + (z_in[2, k] + z_in[3, k])
        probe_out[core, k, spot, :] = probe[core, k, spot, :] + gain * total

    def block_of(g, at, length):
        at = pl.multiple_of(at, length)
        return probe_out.at[core, 2 * g:2 * g + 2, pl.ds(at, length), :]

    def spread(phase, length):
        out = {}
        for d in (2, 1, 3):
            for g in range(2):
                axis = ORDERS[g][phase]
                block = block_of(g, starts[g][phase], length)
                out[d, g] = send(block, block, along(axis, (coords[axis] + d) % 4))
        return out

    out2 = spread(1, 32)
    rows_sent.append(send_rows(1, 1))
    wait(out2.values())
    out1 = spread(0, 128)
    to_core = []
    for g in range(2):
        block = block_of(g, starts[g][0], 128)
        to_core.append(send(block, block, partner))

    wait(rows_sent[0] + rows_sent[1])
    for j in range(2):
        update_object(0, j)
    halo = send_halo(0)

    for d in (1, 3, 2):
        for g in range(2):
            out1[d, g].wait()
            axis = ORDERS[g][0]
            block = block_of(g, (coords[axis] + 4 - d) % 4 * 128, 128)
            to_core.append(send(block, block, partner))

    wait(rows_sent[2] + rows_sent[3])
    for j in range(2):
        update_object(1, j)
    halo += send_halo(1)
    wait(to_core)
    if last:
        for p in range(2):
            obj_out[p, 0] = obj[p, 0]
            obj_out[p, 3] = obj[p, 3]
    else:
        wait(halo)
        for p in range(2):
            obj_out[p, 0] = jnp.where(has_left, col_in[2, p], 0.0)
            obj_out[p, 3] = jnp.where(has_right, col_in[3, p], 0.0)


def exchange(last, obj, probe, grad, pgrad, stats):
    whole = pl.BlockSpec(memory_space=pltpu.VMEM)
    messages = 72
    return pl.pallas_call(
        functools.partial(exchange_body, last),
        out_shape=(
            jax.ShapeDtypeStruct((2, 4, EXT, 128), F32),
            jax.ShapeDtypeStruct((2, MODES, EXT, 128), F32),
            jax.ShapeDtypeStruct((2, 8, 128), F32),
        ),
        in_specs=[whole] * 5,
        out_specs=(whole,) * 3,
        scratch_shapes=[
            pltpu.VMEM((MODES, EXT, 128), F32),
            pltpu.VMEM((MODES, EXT, 128), F32),
            pltpu.VMEM((3, MODES, 128, 128), F32),
            pltpu.VMEM((MODES, 128, 128), F32),
            pltpu.VMEM((3, MODES, 32, 128), F32),
            pltpu.VMEM((4, MODES, 32, 128), F32),
            pltpu.VMEM((2, 4, 2, 8, 128), F32),
            pltpu.VMEM((4, 2, 8, 128), F32),
            pltpu.VMEM((2, 8, 128), F32),
            pltpu.VMEM((4, 2, EXT, 128), F32),
            pltpu.VMEM((2, 2, 2, SIDE, 128), F32),
            pltpu.VMEM((2, 2, EXT, 128), F32),
            pltpu.SemaphoreType.DMA((messages,)),
            pltpu.SemaphoreType.DMA((messages,)),
        ],
        cost_estimate=pl.CostEstimate(flops=40 << 20, bytes_accessed=12 << 20, transcendentals=0),
        compiler_params=pltpu.CompilerParams(
            collective_id=1 if last else 0, has_side_effects=True, vmem_limit_bytes=48 << 20
        ),
        name="exchange_last" if last else "exchange",
    )(obj, probe, grad, pgrad, stats)


def padded(array, sides, width):
    for axis, dim in sides:
        devices, length = (lax.axis_size(axis), array.shape[dim])
        up = [(i, (i + 1) % devices) for i in range(devices - 1)]
        down = [(j, i) for i, j in up]
        last = lax.slice_in_dim(array, length - width, length, axis=dim)
        leading = lax.slice_in_dim(array, 0, width, axis=dim)
        before = lax.ppermute(last, axis, up)
        after = lax.ppermute(leading, axis, down)
        array = jnp.concatenate([before, array, after], axis=dim)
    return array


def on_device(object_field, probe, pos_rows, pos_cols, counts, magnitudes):
    tables = tuple(jnp.asarray(t) for t in transform_tables())
    rows, cols, live = pos_rows.reshape(-1), pos_cols.reshape(-1), counts.reshape(-1)
    extended = padded(object_field, ((ROW, 1), (COL, 2)), HALF)
    obj = extended.reshape(2, EXT, 4, 128).transpose(0, 2, 1, 3)
    planes = probe.reshape(2, MODES, SIDE, 2, 128).transpose(0, 1, 3, 2, 4)
    planes = planes.reshape(2, MODES, EXT, 128)
    misfits = []
    for update in range(ITERS * BATCHES):
        batch = update % BATCHES
        grad, pgrad, stats = position_work(batch, rows, cols, live, obj, planes, magnitudes, tables)
        last = update == ITERS * BATCHES - 1
        obj, planes, totals = exchange(last, obj, planes, grad, pgrad, stats)
        misfits.append(jnp.sum(totals[1]))
    out = obj[:, 1:3, HALF:HALF + SIDE, :].transpose(0, 2, 1, 3).reshape(2, SIDE, SIDE)
    probe_out = planes.reshape(2, MODES, 2, SIDE, 128).transpose(0, 1, 3, 2, 4)
    return (out, probe_out.reshape(2, MODES, SIDE, SIDE), jnp.stack(misfits))


def solution(mesh):
    finer = Mesh(mesh.devices.reshape(4, 2, 4, 2, 2), AXES)
    return jax.shard_map(
        on_device,
        mesh=finer,
        in_specs=(
            P(None, ROW, COL),
            P(),
            P(ROW, COL, None, None),
            P(ROW, COL, None, None),
            P(ROW, COL, None),
            P(ROW, COL, None, None, None, None),
        ),
        out_specs=(P(None, ROW, COL), P(), P()),
        check_vma=False,
    )
```

```python
import functools
import math

import jax
import jax.numpy as jnp
import numpy as np
from jax import lax
from jax.experimental import pallas as pl
from jax.experimental.pallas import tpu as pltpu
from jax.sharding import Mesh
from jax.sharding import PartitionSpec as P

BATCHES = 2
ITERS = 2
SLOTS = 3
MODES = 4
SIDE = 256
HALF = 128
EXT = 512
UPDATES = BATCHES * ITERS
AXES = ("row_0", "row_1", "col_0", "col_1", "col_2")
ROW = ("row_0", "row_1")
COL = ("col_0", "col_1", "col_2")
F32 = jnp.float32
BF16 = jnp.bfloat16

object_rate = 0.9
probe_rate = 0.5
floor_value = 0.5
tiny_value = 1e-06


def transform_tables():
    index = np.arange(SIDE)
    angles = (index[:, None] * index[None, :] % SIDE) * (2.0 * math.pi / SIDE)
    scale = 1.0 / math.sqrt(SIDE)
    c = np.cos(angles) * scale
    s = -np.sin(angles) * scale
    left = np.block([[c, -s], [s, c]])
    return left.astype(jnp.bfloat16), left.T.astype(jnp.bfloat16)


def where_am_i():
    y, lo, x, hi, core = (lax.axis_index(name) for name in AXES)
    row, col = y * 2 + lo, x * 4 + hi * 2 + core
    z = hi * 2 + lo

    def tile(r, c):
        return (r // 2, r % 2, c // 4, (c // 2) % 2, c % 2)

    def along(axis, value):
        if axis == "x":
            return (y, lo, value, hi, core)
        if axis == "y":
            return (value, lo, x, hi, core)
        return (y, value % 2, x, value // 2, core)

    partner = (y, lo, x, hi, 1 - core)
    coords = {"x": x, "y": y, "z": z}
    return row, col, core, coords, along, partner, tile


ORDERS = (("x", "y", "z"), ("y", "x", "z"))
CH = 16
STEPS = SIDE // CH
UNROLL = 4


def fold(x):
    total = x[0:8, :]
    for i in range(1, x.shape[0] // 8):
        total = total + x[8 * i:8 * i + 8, :]
    return total


def visit(
    batch, slot, rows_ref, cols_ref, counts_ref, obj, probe, mags, left_tab, right_tab,
    terms, pgrad, stats, win, wave, half, field,
):
    lane = lax.broadcasted_iota(jnp.int32, (CH, 128), 1)
    row0 = rows_ref[batch * SLOTS + slot]
    col0 = cols_ref[batch * SLOTS + slot]
    live = jnp.where(slot < counts_ref[batch], 1.0, 0.0).astype(F32)
    block = lax.shift_right_logical(col0, 7)
    shift = col0 & 127
    back = (128 - shift) & 127
    none = jnp.zeros((8, 128), F32)

    def make_exit(i, power):
        at = pl.multiple_of(i * CH, CH)
        w = []
        keep = lane < 128 - shift
        for p in range(2):
            rolled = [
                pltpu.roll(obj[p, block + j, pl.ds(row0 + at, CH), :], back, 1) for j in range(3)
            ]
            w.append([jnp.where(keep, rolled[j], rolled[j + 1]) for j in range(2)])
        for j in range(2):
            wr, wi = w[0][j], w[1][j]
            win[0, j, pl.ds(at, CH), :] = wr
            win[1, j, pl.ds(at, CH), :] = wi
            power = power + fold(wr * wr + wi * wi)
            for k in range(MODES):
                pr = probe[0, k, pl.ds(j * SIDE + at, CH), :]
                pi = probe[1, k, pl.ds(j * SIDE + at, CH), :]
                wave[k, pl.ds(at, CH), j * 128:(j + 1) * 128] = (pr * wr - pi * wi).astype(BF16)
                wave[k, pl.ds(SIDE + at, CH), j * 128:(j + 1) * 128] = (pr * wi + pi * wr).astype(BF16)
        return power

    power = lax.fori_loop(0, STEPS, make_exit, none, unroll=UNROLL)
    stats[0] = stats[0] + live * power

    def transform(first, second):
        for k in range(MODES):
            res = jnp.dot(first[...], wave[k], preferred_element_type=F32).astype(BF16)
            half[k * SIDE:(k + 1) * SIDE, 0:SIDE] = res[0:SIDE]
            half[k * SIDE:(k + 1) * SIDE, SIDE:EXT] = res[SIDE:EXT]
        field[...] = jnp.dot(half[...], second[...], preferred_element_type=F32)

    transform(left_tab, right_tab)

    def correct(i, misfit):
        at = pl.multiple_of(i * CH, CH)
        parts = [
            (field[pl.ds(k * SIDE + at, CH), 0:SIDE], field[pl.ds(k * SIDE + at, CH), SIDE:EXT])
            for k in range(MODES)
        ]
        total = sum(re * re + im * im for re, im in parts)
        modulus = jnp.sqrt(total)
        amplitude = mags[batch, slot, pl.ds(at, CH), :]
        factor = live * (amplitude / jnp.maximum(modulus, floor_value) - 1.0)
        gap = modulus - amplitude
        gap = gap * gap
        for k in range(MODES):
            wave[k, pl.ds(at, CH), :] = (parts[k][0] * factor).astype(BF16)
            wave[k, pl.ds(SIDE + at, CH), :] = (parts[k][1] * factor).astype(BF16)
        return misfit + fold(gap[:, 0:128]) + fold(gap[:, 128:256])

    misfit = lax.fori_loop(0, STEPS, correct, none, unroll=UNROLL)
    stats[1] = stats[1] + live * misfit
    transform(right_tab, left_tab)

    def spread(i, c):
        at = pl.multiple_of(i * CH, CH)
        term = [[None, None], [None, None]]
        for j in range(2):
            wr = win[0, j, pl.ds(at, CH), :]
            wi = win[1, j, pl.ds(at, CH), :]
            tr = ti = None
            for k in range(MODES):
                ur = field[pl.ds(k * SIDE + at, CH), j * 128:(j + 1) * 128]
                ui = field[pl.ds(k * SIDE + at, CH), SIDE + j * 128:SIDE + (j + 1) * 128]
                spot = pl.ds(j * SIDE + at, CH)
                pr = probe[0, k, spot, :]
                pi = probe[1, k, spot, :]
                ar = pr * ur + pi * ui
                ai = pr * ui - pi * ur
                tr = ar if tr is None else tr + ar
                ti = ai if ti is None else ti + ai
                pgrad[0, k, spot, :] = pgrad[0, k, spot, :] + (wr * ur + wi * ui)
                pgrad[1, k, spot, :] = pgrad[1, k, spot, :] + (wr * ui - wi * ur)
            term[0][j], term[1][j] = tr, ti
        low = lane < shift
        zero = jnp.zeros((CH, 128), F32)
        spot = pl.ds(SIDE + at, CH)
        for p in range(2):
            a = pltpu.roll(term[p][0], shift, 1)
            b = pltpu.roll(term[p][1], shift, 1)
            terms[slot, p, 1, spot, :] = jnp.where(low, zero, a)
            terms[slot, p, 2, spot, :] = jnp.where(low, a, b)
            terms[slot, p, 3, spot, :] = jnp.where(low, b, zero)
        return c

    lax.fori_loop(0, STEPS, spread, 0, unroll=UNROLL)


def body(
    rows_ref, cols_ref, counts_ref, object_in, probe_in, mags_in, left_in, right_in,
    object_out, probe_out, errors,
    obj, probes, grad, pgrad, terms, stats, mags, left_tab, right_tab, win, wave, half, field,
    core_in, acc, one_in, one, two_in, z_in, tile_in, tile_z, tile_core,
    col_in, row_in, mid, rdma_send, rdma_recv, local, ready,
):
    row, col, core, coords, along, partner, tile = where_am_i()
    up, down = tile((row + 7) % 8, col), tile((row + 1) % 8, col)
    left, right = tile(row, (col + 15) % 16), tile(row, (col + 1) % 16)
    has_left, has_right, has_up, has_down = col > 0, col < 15, row > 0, row < 7
    greeted = [partner, up, down, left, right]
    for axis in ("x", "y", "z"):
        for d in (1, 2, 3):
            greeted.append(along(axis, (coords[axis] + d) % 4))

    def greet(sem):
        for peer in greeted:
            pl.semaphore_signal(sem, inc=1, device_id=peer, device_id_type=pl.DeviceIdType.MESH)

    barrier = pltpu.get_barrier_semaphore()
    greet(barrier)

    loads = []

    def load(src, dst):
        copy = pltpu.make_async_copy(src, dst, local.at[len(loads)])
        copy.start()
        loads.append(copy)

    for j in range(2):
        load(object_in.at[:, :, j * 128:(j + 1) * 128], obj.at[:, 1 + j, HALF:HALF + SIDE, :])
    for j in range(2):
        load(
            probe_in.at[:, :, :, j * 128:(j + 1) * 128],
            probes.at[0, :, :, j * SIDE:(j + 1) * SIDE, :],
        )
    load(left_in, left_tab)
    load(right_in, right_tab)
    load(mags_in.at[0, 0], mags)

    count = [0]

    def message(src, dst, peer):
        n = count[0]
        count[0] += 1
        return pltpu.make_async_remote_copy(
            src_ref=src, dst_ref=dst, send_sem=rdma_send.at[n], recv_sem=rdma_recv.at[n],
            device_id=peer, device_id_type=pl.DeviceIdType.MESH,
        )

    def send(src, dst, peer):
        copy = message(src, dst, peer)
        copy.start()
        return copy

    def wait(copies):
        for copy in copies:
            copy.wait()

    def halo_messages(p):
        return [
            message(obj.at[p, 2], col_in.at[2, p], right),
            message(obj.at[p, 1], col_in.at[3, p], left),
        ]

    def take_halo():
        for p in range(2):
            obj[p, 0] = jnp.where(has_left, col_in[2, p], 0.0)
            obj[p, 3] = jnp.where(has_right, col_in[3, p], 0.0)

    pl.semaphore_wait(barrier, len(greeted))
    wait(loads[0:2])
    first = [
        send(obj.at[:, 1:3, HALF:SIDE, :], row_in.at[1, :, :, 0:HALF, :], up),
        send(obj.at[:, 1:3, SIDE:SIDE + HALF, :], row_in.at[0, :, :, 0:HALF, :], down),
    ]

    def clear(i, c):
        at = pl.multiple_of(i * 64, 64)
        nothing = jnp.zeros((64, 128), F32)
        for s in range(SLOTS):
            for p in range(2):
                for b in range(5):
                    terms[s, p, b, pl.ds(at, 64), :] = nothing
        return c

    lax.fori_loop(0, 12, clear, 0)
    pgrad[...] = jnp.zeros_like(pgrad)
    wait(first)
    for p in range(2):
        for j in range(2):
            obj[p, 1 + j, 0:HALF, :] = jnp.where(has_up, row_in[0, p, j, 0:HALF, :], 0.0)
            obj[p, 1 + j, SIDE + HALF:EXT, :] = jnp.where(has_down, row_in[1, p, j, 0:HALF, :], 0.0)
    halo = halo_messages(0) + halo_messages(1)
    for copy in halo:
        copy.start()
    wait(halo)
    take_halo()
    greet(ready)
    wait(loads[2:7])

    base = count[0]

    def update(u, carry):
        count[0] = base
        batch = u % BATCHES
        now = u % 2
        probe, fresh = probes.at[now], probes.at[1 - now]
        stats[...] = jnp.zeros_like(stats)

        def one_slot(slot, c):
            visit(
                batch, slot, rows_ref, cols_ref, counts_ref, obj, probe, mags, left_tab, right_tab,
                terms, pgrad, stats, win, wave, half, field,
            )
            return c

        lax.fori_loop(0, SLOTS, one_slot, 0)

        spots = []
        for s in range(SLOTS):
            row0 = rows_ref[batch * SLOTS + s]
            col0 = cols_ref[batch * SLOTS + s]
            spots.append((1 - lax.shift_right_logical(col0, 7), SIDE - row0))

        def add_terms(p, b):
            def chunk(i, c):
                at = pl.multiple_of(i * 32, 32)
                grad[p, b, pl.ds(at, 32), :] = sum(
                    terms[s, p, spots[s][0] + b, pl.ds(spots[s][1] + at, 32), :] for s in range(SLOTS)
                )
                return c

            lax.fori_loop(0, EXT // 32, chunk, 0, unroll=4)

        pl.semaphore_wait(ready, len(greeted))

        core_sent = [
            send(stats, tile_core, partner),
            send(pgrad.at[1 - core], core_in, partner),
        ]
        cols_sent = []
        for p in range(2):
            add_terms(p, 3)
            cols = [send(grad.at[p, 3], col_in.at[0, p], right)]
            add_terms(p, 0)
            cols.append(send(grad.at[p, 0], col_in.at[1, p], left))
            cols_sent.append(cols)

        def scatter(phase, source, landing, length, tile_value):
            me = coords[ORDERS[0][phase]]
            tile_in[phase, me] = tile_value
            slot = tile_in.at[phase, me]
            sent = []
            for d in (2, 1, 3):
                sent.append(send(slot, slot, along(ORDERS[0][phase], (me + d) % 4)))
                for g in range(2):
                    axis = ORDERS[g][phase]
                    to = (coords[axis] + d) % 4
                    at = pl.multiple_of(to * length, length)
                    sent.append(
                        send(
                            source.at[2 * g:2 * g + 2, pl.ds(at, length), :],
                            landing.at[d - 1, 2 * g:2 * g + 2],
                            along(axis, to),
                        )
                    )
            return sent

        def gather_sum(phase, source, landing, length):
            out = []
            for g in range(2):
                at = pl.multiple_of(coords[ORDERS[g][phase]] * length, length)
                for k in (2 * g, 2 * g + 1):
                    out.append(
                        source[k, pl.ds(at, length), :] + landing[0, k] + landing[1, k] + landing[2, k]
                    )
            return out

        def tile_total(phase):
            return (tile_in[phase, 0] + tile_in[phase, 1]) + (tile_in[phase, 2] + tile_in[phase, 3])

        def send_rows(p, j):
            return [
                send(mid.at[p, j, 0:SIDE, :], row_in.at[1, p, j], up),
                send(mid.at[p, j, SIDE:EXT, :], row_in.at[0, p, j], down),
            ]

        def make_mid(p):
            wait(cols_sent[p])
            mid[p, 0] = grad[p, 1] + jnp.where(has_left, col_in[0, p], 0.0)
            mid[p, 1] = grad[p, 2] + jnp.where(has_right, col_in[1, p], 0.0)

        wait(core_sent)
        for k in range(MODES):
            acc[k] = pgrad[core, k] + core_in[k]
        sent = scatter(0, acc, one_in, 128, stats[...] + tile_core[...])

        def peak_step(i, best):
            at = pl.multiple_of(i * 16, 16)
            total = None
            for p in range(2):
                for k in range(MODES):
                    v = probe[p, k, pl.ds(at, 16), :]
                    total = v * v if total is None else total + v * v
            return jnp.maximum(best, jnp.maximum(total[0:8], total[8:16]))

        best = lax.fori_loop(0, EXT // 16, peak_step, jnp.zeros((8, 128), F32), unroll=4)
        rate = object_rate / (jnp.max(best) + tiny_value)

        def update_object(p, j):
            upper = jnp.where(has_up, row_in[0, p, j], 0.0)
            lower = jnp.where(has_down, row_in[1, p, j], 0.0)
            top = mid[p, j, 0:SIDE, :] + upper
            low = mid[p, j, SIDE:EXT, :] + lower
            rate_up = jnp.where(has_up, rate, 0.0)
            rate_down = jnp.where(has_down, rate, 0.0)
            b = 1 + j
            obj[p, b, 0:HALF, :] = obj[p, b, 0:HALF, :] + rate_up * top[0:HALF]
            obj[p, b, HALF:SIDE, :] = obj[p, b, HALF:SIDE, :] + rate * top[HALF:SIDE]
            obj[p, b, SIDE:SIDE + HALF, :] = obj[p, b, SIDE:SIDE + HALF, :] + rate * low[0:HALF]
            obj[p, b, SIDE + HALF:EXT, :] = obj[p, b, SIDE + HALF:EXT, :] + rate_down * low[HALF:SIDE]

        for p in range(2):
            add_terms(p, 1)
            add_terms(p, 2)
        make_mid(0)
        rows_sent = [send_rows(0, 0), send_rows(0, 1)]

        wait(sent)
        for k, v in enumerate(gather_sum(0, acc, one_in, 128)):
            one[k] = v
        sent = scatter(1, one, two_in, 32, tile_total(0))

        make_mid(1)

        wait(sent)
        z = coords["z"]
        for k, v in enumerate(gather_sum(1, one, two_in, 32)):
            z_in[z, k] = v
        tile_z[z] = tile_total(1)
        sent = []
        for d in (2, 1, 3):
            peer = along("z", (z + d) % 4)
            sent.append(send(tile_z.at[z], tile_z.at[z], peer))
            sent.append(send(z_in.at[z], z_in.at[z], peer))
        rows_sent.append(send_rows(1, 0))
        pgrad[...] = jnp.zeros_like(pgrad)
        wait(sent)

        totals = (tile_z[0] + tile_z[1]) + (tile_z[2] + tile_z[3])
        errors[u] = totals[1]
        gain = probe_rate * SIDE * SIDE / jnp.sum(totals[0])
        starts = []
        for g in range(2):
            a, b = coords[ORDERS[g][0]], coords[ORDERS[g][1]]
            starts.append((a * 128, a * 128 + b * 32))
        for k in range(MODES):
            spot = pl.ds(pl.multiple_of(starts[k // 2][1], 32), 32)
            total = (z_in[0, k] + z_in[1, k]) + (z_in[2, k] + z_in[3, k])
            fresh[core, k, spot, :] = probe[core, k, spot, :] + gain * total

        def block_of(g, at, length):
            at = pl.multiple_of(at, length)
            return fresh.at[core, 2 * g:2 * g + 2, pl.ds(at, length), :]

        def spread(phase, length):
            out = {}
            for d in (2, 1, 3):
                for g in range(2):
                    axis = ORDERS[g][phase]
                    block = block_of(g, starts[g][phase], length)
                    out[d, g] = send(block, block, along(axis, (coords[axis] + d) % 4))
            return out

        out2 = spread(1, 32)
        rows_sent.append(send_rows(1, 1))
        wait(out2.values())
        out1 = spread(0, 128)
        to_core = []
        for g in range(2):
            block = block_of(g, starts[g][0], 128)
            to_core.append(send(block, block, partner))

        halo = halo_messages(0) + halo_messages(1)
        wait(rows_sent[0] + rows_sent[1])
        for j in range(2):
            update_object(0, j)

        @pl.when(u < UPDATES - 1)
        def _():
            halo[0].start()
            halo[1].start()

        for d in (1, 3, 2):
            for g in range(2):
                out1[d, g].wait()
                axis = ORDERS[g][0]
                block = block_of(g, (coords[axis] + 4 - d) % 4 * 128, 128)
                to_core.append(send(block, block, partner))

        wait(rows_sent[2] + rows_sent[3])
        for j in range(2):
            update_object(1, j)

        @pl.when(u < UPDATES - 1)
        def _():
            halo[2].start()
            halo[3].start()

        wait(to_core)

        @pl.when(u < UPDATES - 1)
        def _():
            wait(halo)
            take_halo()
            greet(ready)

        return carry

    lax.fori_loop(0, UPDATES, update, 0)

    stores = []
    for j in range(2):
        stores.append(
            pltpu.make_async_copy(
                obj.at[:, 1 + j, HALF:HALF + SIDE, :], object_out.at[:, :, j * 128:(j + 1) * 128], local.at[j]
            )
        )
        stores.append(
            pltpu.make_async_copy(
                probes.at[UPDATES % 2, :, :, j * SIDE:(j + 1) * SIDE, :],
                probe_out.at[:, :, :, j * 128:(j + 1) * 128],
                local.at[2 + j],
            )
        )
    for copy in stores:
        copy.start()
    wait(stores)


def on_device(object_field, probe, pos_rows, pos_cols, counts, magnitudes):
    tables = tuple(jnp.asarray(t) for t in transform_tables())
    anywhere = pl.BlockSpec(memory_space=pl.ANY)
    whole = pl.BlockSpec(memory_space=pltpu.VMEM)
    smem = pl.BlockSpec(memory_space=pltpu.SMEM)
    messages = 80
    out, probe_out, errors = pl.pallas_call(
        body,
        out_shape=(
            jax.ShapeDtypeStruct((2, SIDE, SIDE), F32),
            jax.ShapeDtypeStruct((2, MODES, SIDE, SIDE), F32),
            jax.ShapeDtypeStruct((UPDATES, 8, 128), F32),
        ),
        in_specs=[smem, smem, smem] + [anywhere] * 5,
        out_specs=(anywhere, anywhere, whole),
        scratch_shapes=[
            pltpu.VMEM((2, 4, EXT, 128), F32),
            pltpu.VMEM((2, 2, MODES, EXT, 128), F32),
            pltpu.VMEM((2, 4, EXT, 128), F32),
            pltpu.VMEM((2, MODES, EXT, 128), F32),
            pltpu.VMEM((SLOTS, 2, 5, 3 * SIDE, 128), F32),
            pltpu.VMEM((2, 8, 128), F32),
            pltpu.VMEM((BATCHES, SLOTS, SIDE, SIDE), F32),
            pltpu.VMEM((EXT, EXT), BF16),
            pltpu.VMEM((EXT, EXT), BF16),
            pltpu.VMEM((2, 2, SIDE, 128), F32),
            pltpu.VMEM((MODES, EXT, SIDE), BF16),
            pltpu.VMEM((MODES * SIDE, EXT), BF16),
            pltpu.VMEM((MODES * SIDE, EXT), F32),
            pltpu.VMEM((MODES, EXT, 128), F32),
            pltpu.VMEM((MODES, EXT, 128), F32),
            pltpu.VMEM((3, MODES, 128, 128), F32),
            pltpu.VMEM((MODES, 128, 128), F32),
            pltpu.VMEM((3, MODES, 32, 128), F32),
            pltpu.VMEM((4, MODES, 32, 128), F32),
            pltpu.VMEM((2, 4, 2, 8, 128), F32),
            pltpu.VMEM((4, 2, 8, 128), F32),
            pltpu.VMEM((2, 8, 128), F32),
            pltpu.VMEM((4, 2, EXT, 128), F32),
            pltpu.VMEM((2, 2, 2, SIDE, 128), F32),
            pltpu.VMEM((2, 2, EXT, 128), F32),
            pltpu.SemaphoreType.DMA((messages,)),
            pltpu.SemaphoreType.DMA((messages,)),
            pltpu.SemaphoreType.DMA((8,)),
            pltpu.SemaphoreType.REGULAR,
        ],
        cost_estimate=pl.CostEstimate(flops=80 << 30, bytes_accessed=12 << 20, transcendentals=0),
        compiler_params=pltpu.CompilerParams(
            collective_id=0, has_side_effects=True, vmem_limit_bytes=60 << 20
        ),
        name="whole_sweep",
    )(
        pos_rows.reshape(-1), pos_cols.reshape(-1), counts.reshape(-1),
        object_field, probe, magnitudes, *tables,
    )
    return (out, probe_out, jnp.sum(errors, axis=(1, 2)))


def solution(mesh):
    finer = Mesh(mesh.devices.reshape(4, 2, 4, 2, 2), AXES)
    return jax.shard_map(
        on_device,
        mesh=finer,
        in_specs=(
            P(None, ROW, COL),
            P(),
            P(ROW, COL, None, None),
            P(ROW, COL, None, None),
            P(ROW, COL, None),
            P(ROW, COL, None, None, None, None),
        ),
        out_specs=(P(None, ROW, COL), P(), P()),
        check_vma=False,
    )
```

```python
import functools
import math

import jax
import jax.numpy as jnp
import numpy as np
from jax import lax
from jax.experimental import pallas as pl
from jax.experimental.pallas import tpu as pltpu
from jax.sharding import Mesh
from jax.sharding import PartitionSpec as P

BATCHES = 2
ITERS = 2
SLOTS = 3
MODES = 4
SIDE = 256
HALF = 128
EXT = 512
UPDATES = BATCHES * ITERS
AXES = ("row_0", "row_1", "col_0", "col_1", "col_2")
ROW = ("row_0", "row_1")
COL = ("col_0", "col_1", "col_2")
F32 = jnp.float32
BF16 = jnp.bfloat16

object_rate = 0.9
probe_rate = 0.5
floor_value = 0.5
tiny_value = 1e-06


def transform_tables():
    index = np.arange(SIDE)
    angles = (index[:, None] * index[None, :] % SIDE) * (2.0 * math.pi / SIDE)
    scale = 1.0 / math.sqrt(SIDE)
    c = np.cos(angles) * scale
    s = -np.sin(angles) * scale
    left = np.block([[c, -s], [s, c]])
    return left.astype(jnp.bfloat16), left.T.astype(jnp.bfloat16)


def where_am_i():
    y, lo, x, hi, core = (lax.axis_index(name) for name in AXES)
    row, col = y * 2 + lo, x * 4 + hi * 2 + core
    z = hi * 2 + lo

    def tile(r, c):
        return (r // 2, r % 2, c // 4, (c // 2) % 2, c % 2)

    def along(axis, value):
        if axis == "x":
            return (y, lo, value, hi, core)
        if axis == "y":
            return (value, lo, x, hi, core)
        return (y, value % 2, x, value // 2, core)

    partner = (y, lo, x, hi, 1 - core)
    coords = {"x": x, "y": y, "z": z}
    return row, col, core, coords, along, partner, tile


ORDERS = (("x", "y", "z"), ("y", "x", "z"))
CH = 16
STEPS = SIDE // CH
UNROLL = 4


def fold(x):
    total = x[0:8, :]
    for i in range(1, x.shape[0] // 8):
        total = total + x[8 * i:8 * i + 8, :]
    return total


def visit(
    batch, slot, rows_ref, cols_ref, counts_ref, obj, probe, mags, left_tab, right_tab,
    terms, pgrad, stats, win, wave, half, field,
):
    lane = lax.broadcasted_iota(jnp.int32, (CH, 128), 1)
    row0 = rows_ref[0, 0, batch, slot]
    col0 = cols_ref[0, 0, batch, slot]
    live = jnp.where(slot < counts_ref[0, 0, batch], 1.0, 0.0).astype(F32)
    block = lax.shift_right_logical(col0, 7)
    shift = col0 & 127
    back = (128 - shift) & 127
    none = jnp.zeros((8, 128), F32)

    def make_exit(i, power):
        at = pl.multiple_of(i * CH, CH)
        w = []
        keep = lane < 128 - shift
        for p in range(2):
            rolled = [
                pltpu.roll(obj[p, block + j, pl.ds(row0 + at, CH), :], back, 1) for j in range(3)
            ]
            w.append([jnp.where(keep, rolled[j], rolled[j + 1]) for j in range(2)])
        for j in range(2):
            wr, wi = w[0][j], w[1][j]
            win[0, j, pl.ds(at, CH), :] = wr
            win[1, j, pl.ds(at, CH), :] = wi
            power = power + fold(wr * wr + wi * wi)
            for k in range(MODES):
                pr = probe[0, k, pl.ds(j * SIDE + at, CH), :]
                pi = probe[1, k, pl.ds(j * SIDE + at, CH), :]
                wave[k, pl.ds(at, CH), j * 128:(j + 1) * 128] = (pr * wr - pi * wi).astype(BF16)
                wave[k, pl.ds(SIDE + at, CH), j * 128:(j + 1) * 128] = (pr * wi + pi * wr).astype(BF16)
        return power

    power = lax.fori_loop(0, STEPS, make_exit, none, unroll=UNROLL)
    stats[0] = stats[0] + live * power

    def transform(first, second):
        for k in range(MODES):
            res = jnp.dot(first[...], wave[k], preferred_element_type=F32).astype(BF16)
            half[k * SIDE:(k + 1) * SIDE, 0:SIDE] = res[0:SIDE]
            half[k * SIDE:(k + 1) * SIDE, SIDE:EXT] = res[SIDE:EXT]
        field[...] = jnp.dot(half[...], second[...], preferred_element_type=F32)

    transform(left_tab, right_tab)

    def correct(i, misfit):
        at = pl.multiple_of(i * CH, CH)
        parts = [
            (field[pl.ds(k * SIDE + at, CH), 0:SIDE], field[pl.ds(k * SIDE + at, CH), SIDE:EXT])
            for k in range(MODES)
        ]
        total = sum(re * re + im * im for re, im in parts)
        modulus = jnp.sqrt(total)
        amplitude = mags[batch, slot, pl.ds(at, CH), :]
        factor = live * (amplitude / jnp.maximum(modulus, floor_value) - 1.0)
        gap = modulus - amplitude
        gap = gap * gap
        for k in range(MODES):
            wave[k, pl.ds(at, CH), :] = (parts[k][0] * factor).astype(BF16)
            wave[k, pl.ds(SIDE + at, CH), :] = (parts[k][1] * factor).astype(BF16)
        return misfit + fold(gap[:, 0:128]) + fold(gap[:, 128:256])

    misfit = lax.fori_loop(0, STEPS, correct, none, unroll=UNROLL)
    stats[1] = stats[1] + live * misfit
    transform(right_tab, left_tab)

    def spread(i, c):
        at = pl.multiple_of(i * CH, CH)
        term = [[None, None], [None, None]]
        for j in range(2):
            wr = win[0, j, pl.ds(at, CH), :]
            wi = win[1, j, pl.ds(at, CH), :]
            tr = ti = None
            for k in range(MODES):
                ur = field[pl.ds(k * SIDE + at, CH), j * 128:(j + 1) * 128]
                ui = field[pl.ds(k * SIDE + at, CH), SIDE + j * 128:SIDE + (j + 1) * 128]
                spot = pl.ds(j * SIDE + at, CH)
                pr = probe[0, k, spot, :]
                pi = probe[1, k, spot, :]
                ar = pr * ur + pi * ui
                ai = pr * ui - pi * ur
                tr = ar if tr is None else tr + ar
                ti = ai if ti is None else ti + ai
                pgrad[0, k, spot, :] = pgrad[0, k, spot, :] + (wr * ur + wi * ui)
                pgrad[1, k, spot, :] = pgrad[1, k, spot, :] + (wr * ui - wi * ur)
            term[0][j], term[1][j] = tr, ti
        low = lane < shift
        zero = jnp.zeros((CH, 128), F32)
        spot = pl.ds(SIDE + at, CH)
        for p in range(2):
            a = pltpu.roll(term[p][0], shift, 1)
            b = pltpu.roll(term[p][1], shift, 1)
            terms[slot, p, 1, spot, :] = jnp.where(low, zero, a)
            terms[slot, p, 2, spot, :] = jnp.where(low, a, b)
            terms[slot, p, 3, spot, :] = jnp.where(low, b, zero)
        return c

    lax.fori_loop(0, STEPS, spread, 0, unroll=UNROLL)


def body(
    rows_ref, cols_ref, counts_ref, object_in, probe_in, mags_in, left_in, right_in,
    object_out, probe_out, errors,
    obj, probes, grad, pgrad, terms, stats, mags, left_tab, right_tab, win, wave, half, field,
    core_in, acc, one_in, one, two_in, z_in, tile_in, tile_z, tile_core,
    col_in, row_in, mid, rdma_send, rdma_recv, local, ready,
):
    row, col, core, coords, along, partner, tile = where_am_i()
    up, down = tile((row + 7) % 8, col), tile((row + 1) % 8, col)
    left, right = tile(row, (col + 15) % 16), tile(row, (col + 1) % 16)
    has_left, has_right, has_up, has_down = col > 0, col < 15, row > 0, row < 7
    greeted = [partner, up, down, left, right]
    for axis in ("x", "y", "z"):
        for d in (1, 2, 3):
            greeted.append(along(axis, (coords[axis] + d) % 4))

    def greet(sem):
        for peer in greeted:
            pl.semaphore_signal(sem, inc=1, device_id=peer, device_id_type=pl.DeviceIdType.MESH)

    barrier = pltpu.get_barrier_semaphore()
    greet(barrier)

    loads = []

    def load(src, dst):
        copy = pltpu.make_async_copy(src, dst, local.at[len(loads)])
        copy.start()
        loads.append(copy)

    for j in range(2):
        load(object_in.at[:, :, j * 128:(j + 1) * 128], obj.at[:, 1 + j, HALF:HALF + SIDE, :])
    for j in range(2):
        load(
            probe_in.at[:, :, :, j * 128:(j + 1) * 128],
            probes.at[0, :, :, j * SIDE:(j + 1) * SIDE, :],
        )
    load(left_in, left_tab)
    load(right_in, right_tab)
    load(mags_in.at[0, 0], mags)

    count = [0]

    def message(src, dst, peer):
        n = count[0]
        count[0] += 1
        return pltpu.make_async_remote_copy(
            src_ref=src, dst_ref=dst, send_sem=rdma_send.at[n], recv_sem=rdma_recv.at[n],
            device_id=peer, device_id_type=pl.DeviceIdType.MESH,
        )

    def send(src, dst, peer):
        copy = message(src, dst, peer)
        copy.start()
        return copy

    def wait(copies):
        for copy in copies:
            copy.wait()

    def halo_messages(p):
        return [
            message(obj.at[p, 2], obj.at[p, 0], right),
            message(obj.at[p, 1], obj.at[p, 3], left),
        ]

    def start_halo(pair):
        @pl.when(has_right)
        def _():
            pair[0].start()

        @pl.when(has_left)
        def _():
            pair[1].start()

    def wait_halo(pair):
        @pl.when(has_right)
        def _():
            pair[0].wait_send()
            pair[1].wait_recv()

        @pl.when(has_left)
        def _():
            pair[1].wait_send()
            pair[0].wait_recv()

    pl.semaphore_wait(barrier, len(greeted))
    wait(loads[0:2])
    first = [
        [
            send(obj.at[p, 1:3, HALF:SIDE, :], row_in.at[1, p, :, 0:HALF, :], up),
            send(obj.at[p, 1:3, SIDE:SIDE + HALF, :], row_in.at[0, p, :, 0:HALF, :], down),
        ]
        for p in range(2)
    ]

    @pl.when(jnp.logical_not(has_left))
    def _():
        obj[:, 0] = jnp.zeros((2, EXT, 128), F32)

    @pl.when(jnp.logical_not(has_right))
    def _():
        obj[:, 3] = jnp.zeros((2, EXT, 128), F32)

    def clear(i, c):
        at = pl.multiple_of(i * 64, 64)
        nothing = jnp.zeros((64, 128), F32)
        for s in range(SLOTS):
            for p in range(2):
                for b in range(5):
                    terms[s, p, b, pl.ds(at, 64), :] = nothing
        return c

    lax.fori_loop(0, 12, clear, 0)
    pgrad[...] = jnp.zeros_like(pgrad)
    halo = [halo_messages(p) for p in range(2)]
    for p in range(2):
        wait(first[p])
        for j in range(2):
            obj[p, 1 + j, 0:HALF, :] = jnp.where(has_up, row_in[0, p, j, 0:HALF, :], 0.0)
            obj[p, 1 + j, SIDE + HALF:EXT, :] = jnp.where(has_down, row_in[1, p, j, 0:HALF, :], 0.0)
        start_halo(halo[p])
    for p in range(2):
        wait_halo(halo[p])
    greet(ready)
    wait(loads[2:7])

    base = count[0]

    def update(u, carry):
        count[0] = base
        batch = u % BATCHES
        now = u % 2
        probe, fresh = probes.at[now], probes.at[1 - now]
        stats[...] = jnp.zeros_like(stats)

        def one_slot(slot, c):
            visit(
                batch, slot, rows_ref, cols_ref, counts_ref, obj, probe, mags, left_tab, right_tab,
                terms, pgrad, stats, win, wave, half, field,
            )
            return c

        lax.fori_loop(0, SLOTS, one_slot, 0)

        spots = []
        for s in range(SLOTS):
            row0 = rows_ref[0, 0, batch, s]
            col0 = cols_ref[0, 0, batch, s]
            spots.append((1 - lax.shift_right_logical(col0, 7), SIDE - row0))

        def add_terms(p, b):
            def chunk(i, c):
                at = pl.multiple_of(i * 32, 32)
                grad[p, b, pl.ds(at, 32), :] = sum(
                    terms[s, p, spots[s][0] + b, pl.ds(spots[s][1] + at, 32), :] for s in range(SLOTS)
                )
                return c

            lax.fori_loop(0, EXT // 32, chunk, 0, unroll=4)

        pl.semaphore_wait(ready, len(greeted))

        core_sent = [
            send(stats, tile_core, partner),
            send(pgrad.at[1 - core], core_in, partner),
        ]
        cols_sent = []
        for p in range(2):
            add_terms(p, 3)
            cols = [send(grad.at[p, 3], col_in.at[0, p], right)]
            add_terms(p, 0)
            cols.append(send(grad.at[p, 0], col_in.at[1, p], left))
            cols_sent.append(cols)

        def scatter(phase, source, landing, length, tile_value):
            me = coords[ORDERS[0][phase]]
            tile_in[phase, me] = tile_value
            slot = tile_in.at[phase, me]
            sent = []
            for d in (2, 1, 3):
                sent.append(send(slot, slot, along(ORDERS[0][phase], (me + d) % 4)))
                for g in range(2):
                    axis = ORDERS[g][phase]
                    to = (coords[axis] + d) % 4
                    at = pl.multiple_of(to * length, length)
                    sent.append(
                        send(
                            source.at[2 * g:2 * g + 2, pl.ds(at, length), :],
                            landing.at[d - 1, 2 * g:2 * g + 2],
                            along(axis, to),
                        )
                    )
            return sent

        def gather_sum(phase, source, landing, length):
            out = []
            for g in range(2):
                at = pl.multiple_of(coords[ORDERS[g][phase]] * length, length)
                for k in (2 * g, 2 * g + 1):
                    out.append(
                        source[k, pl.ds(at, length), :] + landing[0, k] + landing[1, k] + landing[2, k]
                    )
            return out

        def tile_total(phase):
            return (tile_in[phase, 0] + tile_in[phase, 1]) + (tile_in[phase, 2] + tile_in[phase, 3])

        def send_rows(p, j):
            outer = [
                send(mid.at[p, j, 0:HALF, :], row_in.at[1, p, j, 0:HALF], up),
                send(mid.at[p, j, SIDE + HALF:EXT, :], row_in.at[0, p, j, HALF:SIDE], down),
            ]
            inner = [
                message(mid.at[p, j, HALF:SIDE, :], row_in.at[1, p, j, HALF:SIDE], up),
                message(mid.at[p, j, SIDE:SIDE + HALF, :], row_in.at[0, p, j, 0:HALF], down),
            ]

            @pl.when(u < UPDATES - 1)
            def _():
                inner[0].start()
                inner[1].start()

            return (outer, inner)

        def wait_rows(pair):
            for outer, inner in pair:
                wait(outer)

            @pl.when(u < UPDATES - 1)
            def _():
                for outer, inner in pair:
                    wait(inner)

        def make_mid(p):
            wait(cols_sent[p])
            mid[p, 0] = grad[p, 1] + jnp.where(has_left, col_in[0, p], 0.0)
            mid[p, 1] = grad[p, 2] + jnp.where(has_right, col_in[1, p], 0.0)

        wait(core_sent)
        for k in range(MODES):
            acc[k] = pgrad[core, k] + core_in[k]
        sent = scatter(0, acc, one_in, 128, stats[...] + tile_core[...])

        def peak_step(i, best):
            at = pl.multiple_of(i * 16, 16)
            total = None
            for p in range(2):
                for k in range(MODES):
                    v = probe[p, k, pl.ds(at, 16), :]
                    total = v * v if total is None else total + v * v
            return jnp.maximum(best, jnp.maximum(total[0:8], total[8:16]))

        best = lax.fori_loop(0, EXT // 16, peak_step, jnp.zeros((8, 128), F32), unroll=4)
        rate = object_rate / (jnp.max(best) + tiny_value)

        def update_object(p, j):
            upper = jnp.where(has_up, row_in[0, p, j], 0.0)
            lower = jnp.where(has_down, row_in[1, p, j], 0.0)
            top = mid[p, j, 0:SIDE, :] + upper
            low = mid[p, j, SIDE:EXT, :] + lower
            rate_up = jnp.where(has_up, rate, 0.0)
            rate_down = jnp.where(has_down, rate, 0.0)
            b = 1 + j
            obj[p, b, 0:HALF, :] = obj[p, b, 0:HALF, :] + rate_up * top[0:HALF]
            obj[p, b, HALF:SIDE, :] = obj[p, b, HALF:SIDE, :] + rate * top[HALF:SIDE]
            obj[p, b, SIDE:SIDE + HALF, :] = obj[p, b, SIDE:SIDE + HALF, :] + rate * low[0:HALF]
            obj[p, b, SIDE + HALF:EXT, :] = obj[p, b, SIDE + HALF:EXT, :] + rate_down * low[HALF:SIDE]

        for p in range(2):
            add_terms(p, 1)
            add_terms(p, 2)
        make_mid(0)
        rows_sent = [send_rows(0, 0), send_rows(0, 1)]

        wait(sent)
        for k, v in enumerate(gather_sum(0, acc, one_in, 128)):
            one[k] = v
        sent = scatter(1, one, two_in, 32, tile_total(0))

        make_mid(1)

        wait(sent)
        z = coords["z"]
        for k, v in enumerate(gather_sum(1, one, two_in, 32)):
            z_in[z, k] = v
        tile_z[z] = tile_total(1)
        sent = []
        for d in (2, 1, 3):
            peer = along("z", (z + d) % 4)
            sent.append(send(tile_z.at[z], tile_z.at[z], peer))
            sent.append(send(z_in.at[z], z_in.at[z], peer))
        pgrad[...] = jnp.zeros_like(pgrad)
        rows_sent.append(send_rows(1, 0))
        wait(sent)

        totals = (tile_z[0] + tile_z[1]) + (tile_z[2] + tile_z[3])
        errors[u] = totals[1]
        gain = probe_rate * SIDE * SIDE / jnp.sum(totals[0])
        starts = []
        for g in range(2):
            a, b = coords[ORDERS[g][0]], coords[ORDERS[g][1]]
            starts.append((a * 128, a * 128 + b * 32))
        for k in range(MODES):
            spot = pl.ds(pl.multiple_of(starts[k // 2][1], 32), 32)
            total = (z_in[0, k] + z_in[1, k]) + (z_in[2, k] + z_in[3, k])
            fresh[core, k, spot, :] = probe[core, k, spot, :] + gain * total

        def block_of(g, at, length):
            at = pl.multiple_of(at, length)
            return fresh.at[core, 2 * g:2 * g + 2, pl.ds(at, length), :]

        def spread(phase, length):
            out = {}
            for d in (2, 1, 3):
                for g in range(2):
                    axis = ORDERS[g][phase]
                    block = block_of(g, starts[g][phase], length)
                    out[d, g] = send(block, block, along(axis, (coords[axis] + d) % 4))
            return out

        out2 = spread(1, 32)
        rows_sent.append(send_rows(1, 1))
        halo = [halo_messages(p) for p in range(2)]

        def finish_object(p):
            wait_rows(rows_sent[2 * p:2 * p + 2])
            for j in range(2):
                update_object(p, j)

            @pl.when(u < UPDATES - 1)
            def _():
                start_halo(halo[p])

        wait(out2.values())
        out1 = spread(0, 128)
        finish_object(0)
        to_core = []
        for g in range(2):
            block = block_of(g, starts[g][0], 128)
            to_core.append(send(block, block, partner))

        for d in (1, 3, 2):
            for g in range(2):
                out1[d, g].wait()
                axis = ORDERS[g][0]
                block = block_of(g, (coords[axis] + 4 - d) % 4 * 128, 128)
                to_core.append(send(block, block, partner))

        finish_object(1)
        wait(to_core)

        @pl.when(u < UPDATES - 1)
        def _():
            for p in range(2):
                wait_halo(halo[p])
            greet(ready)

        return carry

    lax.fori_loop(0, UPDATES, update, 0)

    stores = []
    for j in range(2):
        stores.append(
            pltpu.make_async_copy(
                obj.at[:, 1 + j, HALF:HALF + SIDE, :], object_out.at[:, :, j * 128:(j + 1) * 128], local.at[j]
            )
        )
        stores.append(
            pltpu.make_async_copy(
                probes.at[UPDATES % 2, :, :, j * SIDE:(j + 1) * SIDE, :],
                probe_out.at[:, :, :, j * 128:(j + 1) * 128],
                local.at[2 + j],
            )
        )
    for copy in stores:
        copy.start()
    wait(stores)


def on_device(object_field, probe, pos_rows, pos_cols, counts, magnitudes):
    tables = tuple(jnp.asarray(t) for t in transform_tables())
    anywhere = pl.BlockSpec(memory_space=pl.ANY)
    whole = pl.BlockSpec(memory_space=pltpu.VMEM)
    smem = pl.BlockSpec(memory_space=pltpu.SMEM)
    messages = 96
    out, probe_out, errors = pl.pallas_call(
        body,
        out_shape=(
            jax.ShapeDtypeStruct((2, SIDE, SIDE), F32),
            jax.ShapeDtypeStruct((2, MODES, SIDE, SIDE), F32),
            jax.ShapeDtypeStruct((UPDATES, 8, 128), F32),
        ),
        in_specs=[smem, smem, smem] + [anywhere] * 5,
        out_specs=(anywhere, anywhere, whole),
        scratch_shapes=[
            pltpu.VMEM((2, 4, EXT, 128), F32),
            pltpu.VMEM((2, 2, MODES, EXT, 128), F32),
            pltpu.VMEM((2, 4, EXT, 128), F32),
            pltpu.VMEM((2, MODES, EXT, 128), F32),
            pltpu.VMEM((SLOTS, 2, 5, 3 * SIDE, 128), F32),
            pltpu.VMEM((2, 8, 128), F32),
            pltpu.VMEM((BATCHES, SLOTS, SIDE, SIDE), F32),
            pltpu.VMEM((EXT, EXT), BF16),
            pltpu.VMEM((EXT, EXT), BF16),
            pltpu.VMEM((2, 2, SIDE, 128), F32),
            pltpu.VMEM((MODES, EXT, SIDE), BF16),
            pltpu.VMEM((MODES * SIDE, EXT), BF16),
            pltpu.VMEM((MODES * SIDE, EXT), F32),
            pltpu.VMEM((MODES, EXT, 128), F32),
            pltpu.VMEM((MODES, EXT, 128), F32),
            pltpu.VMEM((3, MODES, 128, 128), F32),
            pltpu.VMEM((MODES, 128, 128), F32),
            pltpu.VMEM((3, MODES, 32, 128), F32),
            pltpu.VMEM((4, MODES, 32, 128), F32),
            pltpu.VMEM((2, 4, 2, 8, 128), F32),
            pltpu.VMEM((4, 2, 8, 128), F32),
            pltpu.VMEM((2, 8, 128), F32),
            pltpu.VMEM((2, 2, EXT, 128), F32),
            pltpu.VMEM((2, 2, 2, SIDE, 128), F32),
            pltpu.VMEM((2, 2, EXT, 128), F32),
            pltpu.SemaphoreType.DMA((messages,)),
            pltpu.SemaphoreType.DMA((messages,)),
            pltpu.SemaphoreType.DMA((8,)),
            pltpu.SemaphoreType.REGULAR,
        ],
        cost_estimate=pl.CostEstimate(flops=80 << 30, bytes_accessed=12 << 20, transcendentals=0),
        compiler_params=pltpu.CompilerParams(
            collective_id=0, has_side_effects=True, vmem_limit_bytes=60 << 20
        ),
        name="whole_sweep",
    )(
        pos_rows, pos_cols, counts,
        object_field, probe, magnitudes, *tables,
    )
    return (out, probe_out, jnp.sum(errors, axis=(1, 2)))


def solution(mesh):
    finer = Mesh(mesh.devices.reshape(4, 2, 4, 2, 2), AXES)
    return jax.shard_map(
        on_device,
        mesh=finer,
        in_specs=(
            P(None, ROW, COL),
            P(),
            P(ROW, COL, None, None),
            P(ROW, COL, None, None),
            P(ROW, COL, None),
            P(ROW, COL, None, None, None, None),
        ),
        out_specs=(P(None, ROW, COL), P(), P()),
        check_vma=False,
    )
```

```python
import functools
import math

import jax
import jax.numpy as jnp
import numpy as np
from jax import lax
from jax.experimental import pallas as pl
from jax.experimental.pallas import tpu as pltpu
from jax.sharding import Mesh
from jax.sharding import PartitionSpec as P

BATCHES = 2
ITERS = 2
SLOTS = 3
MODES = 4
SIDE = 256
HALF = 128
EXT = 512
UPDATES = BATCHES * ITERS
AXES = ("row_0", "row_1", "col_0", "col_1", "col_2")
ROW = ("row_0", "row_1")
COL = ("col_0", "col_1", "col_2")
F32 = jnp.float32
BF16 = jnp.bfloat16

object_rate = 0.9
probe_rate = 0.5
floor_value = 0.5
tiny_value = 1e-06


def transform_tables():
    index = np.arange(SIDE)
    angles = (index[:, None] * index[None, :] % SIDE) * (2.0 * math.pi / SIDE)
    scale = 1.0 / math.sqrt(SIDE)
    c = np.cos(angles) * scale
    s = -np.sin(angles) * scale
    near = np.arange(HALF)
    tables = []
    for parity in range(2):
        pick = np.arange(parity, SIDE, 2)
        cr, sr = c[np.ix_(pick, near)], s[np.ix_(pick, near)]
        tables.append(np.block([[cr, -sr], [sr, cr]]))
    for parity in range(2):
        pick = np.arange(parity, SIDE, 2)
        cr, sr = c[np.ix_(near, pick)], s[np.ix_(near, pick)]
        tables.append(np.block([[cr, sr], [-sr, cr]]))
    tables = tables + [t.T for t in tables]
    order = np.concatenate([np.arange(0, SIDE, 2), np.arange(1, SIDE, 2)])
    sort = np.eye(SIDE)[order]
    return (np.stack(tables).astype(jnp.bfloat16), np.stack([sort, sort.T]).astype(jnp.bfloat16))


def where_am_i():
    y, lo, x, hi, core = (lax.axis_index(name) for name in AXES)
    row, col = y * 2 + lo, x * 4 + hi * 2 + core
    z = hi * 2 + lo

    def tile(r, c):
        return (r // 2, r % 2, c // 4, (c // 2) % 2, c % 2)

    def along(axis, value):
        if axis == "x":
            return (y, lo, value, hi, core)
        if axis == "y":
            return (value, lo, x, hi, core)
        return (y, value % 2, x, value // 2, core)

    partner = (y, lo, x, hi, 1 - core)
    coords = {"x": x, "y": y, "z": z}
    return row, col, core, coords, along, partner, tile


ORDERS = (("x", "y", "z"), ("y", "x", "z"))
CH = 16
STEPS = SIDE // CH
UNROLL = 4


def fold(x):
    total = x[0:8, :]
    for i in range(1, x.shape[0] // 8):
        total = total + x[8 * i:8 * i + 8, :]
    return total


def visit(
    batch, slot, rows_ref, cols_ref, counts_ref, obj, probe, mags, tables,
    terms, pgrad, stats, win, wave, half, field,
):
    lane = lax.broadcasted_iota(jnp.int32, (CH, 128), 1)
    row0 = rows_ref[0, 0, batch, slot]
    col0 = cols_ref[0, 0, batch, slot]
    live = jnp.where(slot < counts_ref[0, 0, batch], 1.0, 0.0).astype(F32)
    block = lax.shift_right_logical(col0, 7)
    shift = col0 & 127
    back = (128 - shift) & 127
    none = jnp.zeros((8, 128), F32)

    def make_exit(i, power):
        at = pl.multiple_of(i * CH, CH)
        keep = lane < 128 - shift
        w = []
        for h in range(2):
            for p in range(2):
                rolled = [
                    pltpu.roll(obj[p, block + j, pl.ds(row0 + h * HALF + at, CH), :], back, 1)
                    for j in range(3)
                ]
                w.append([jnp.where(keep, rolled[j], rolled[j + 1]) for j in range(2)])
        for j in range(2):
            for h in range(2):
                wr, wi = w[2 * h][j], w[2 * h + 1][j]
                win[0, j, pl.ds(h * HALF + at, CH), :] = wr
                win[1, j, pl.ds(h * HALF + at, CH), :] = wi
                power = power + fold(wr * wr + wi * wi)
            for k in range(MODES):
                re, im = [], []
                for h in range(2):
                    wr, wi = w[2 * h][j], w[2 * h + 1][j]
                    pr = probe[0, k, pl.ds(j * SIDE + h * HALF + at, CH), :]
                    pi = probe[1, k, pl.ds(j * SIDE + h * HALF + at, CH), :]
                    re.append(pr * wr - pi * wi)
                    im.append(pr * wi + pi * wr)
                cols = slice(j * 128, (j + 1) * 128)
                wave[k, 0, pl.ds(at, CH), cols] = (re[0] + re[1]).astype(BF16)
                wave[k, 0, pl.ds(HALF + at, CH), cols] = (im[0] + im[1]).astype(BF16)
                wave[k, 1, pl.ds(at, CH), cols] = (re[0] - re[1]).astype(BF16)
                wave[k, 1, pl.ds(HALF + at, CH), cols] = (im[0] - im[1]).astype(BF16)
        return power

    power = lax.fori_loop(0, STEPS // 2, make_exit, none, unroll=UNROLL // 2)
    stats[0] = stats[0] + live * power

    for k in range(MODES):
        for parity in range(2):
            res = jnp.dot(tables[parity], wave[k, parity], preferred_element_type=F32)
            spot = slice(k * SIDE + parity * HALF, k * SIDE + (parity + 1) * HALF)
            for o in range(2):
                near = res[o * HALF:(o + 1) * HALF, 0:HALF]
                far = res[o * HALF:(o + 1) * HALF, HALF:SIDE]
                half[0, spot, o * HALF:(o + 1) * HALF] = (near + far).astype(BF16)
                half[1, spot, o * HALF:(o + 1) * HALF] = (near - far).astype(BF16)
    for parity in range(2):
        field[parity] = jnp.dot(half[parity], tables[4 + parity], preferred_element_type=F32)

    def correct(i, misfit):
        at = pl.multiple_of(i * CH, CH)
        parity = i // (STEPS // 2)
        to = pl.multiple_of((i % (STEPS // 2)) * CH, CH)
        for q in range(2):
            parts = [
                (field[q, pl.ds(k * SIDE + at, CH), 0:HALF], field[q, pl.ds(k * SIDE + at, CH), HALF:SIDE])
                for k in range(MODES)
            ]
            total = sum(re * re + im * im for re, im in parts)
            modulus = jnp.sqrt(total)
            amplitude = mags[batch, slot, pl.ds(at, CH), q * HALF:(q + 1) * HALF]
            factor = live * (amplitude / jnp.maximum(modulus, floor_value) - 1.0)
            gap = modulus - amplitude
            misfit = misfit + fold(gap * gap)
            cols = slice(q * HALF, (q + 1) * HALF)
            for k in range(MODES):
                wave[k, parity, pl.ds(to, CH), cols] = (parts[k][0] * factor).astype(BF16)
                wave[k, parity, pl.ds(HALF + to, CH), cols] = (parts[k][1] * factor).astype(BF16)
        return misfit

    misfit = lax.fori_loop(0, STEPS, correct, none, unroll=UNROLL)
    stats[1] = stats[1] + live * misfit

    for k in range(MODES):
        even = jnp.dot(tables[2], wave[k, 0], preferred_element_type=F32)
        odd = jnp.dot(tables[3], wave[k, 1], preferred_element_type=F32)
        for h, value in enumerate(((even + odd).astype(BF16), (even - odd).astype(BF16))):
            spot = slice(k * SIDE + h * HALF, k * SIDE + (h + 1) * HALF)
            for o in range(2):
                for q in range(2):
                    half[q, spot, o * HALF:(o + 1) * HALF] = value[
                        o * HALF:(o + 1) * HALF, q * HALF:(q + 1) * HALF
                    ]
    for parity in range(2):
        field[parity] = jnp.dot(half[parity], tables[6 + parity], preferred_element_type=F32)

    def spread(i, c):
        at = pl.multiple_of(i * CH, CH)
        term = [[None, None], [None, None]]
        for j in range(2):
            wr = win[0, j, pl.ds(at, CH), :]
            wi = win[1, j, pl.ds(at, CH), :]
            tr = ti = None
            for k in range(MODES):
                source = pl.ds(k * SIDE + at, CH)
                if j == 0:
                    ur = field[0, source, 0:HALF] + field[1, source, 0:HALF]
                    ui = field[0, source, HALF:SIDE] + field[1, source, HALF:SIDE]
                else:
                    ur = field[0, source, 0:HALF] - field[1, source, 0:HALF]
                    ui = field[0, source, HALF:SIDE] - field[1, source, HALF:SIDE]
                spot = pl.ds(j * SIDE + at, CH)
                pr = probe[0, k, spot, :]
                pi = probe[1, k, spot, :]
                ar = pr * ur + pi * ui
                ai = pr * ui - pi * ur
                tr = ar if tr is None else tr + ar
                ti = ai if ti is None else ti + ai
                pgrad[0, k, spot, :] = pgrad[0, k, spot, :] + (wr * ur + wi * ui)
                pgrad[1, k, spot, :] = pgrad[1, k, spot, :] + (wr * ui - wi * ur)
            term[0][j], term[1][j] = tr, ti
        low = lane < shift
        zero = jnp.zeros((CH, 128), F32)
        spot = pl.ds(SIDE + at, CH)
        for p in range(2):
            a = pltpu.roll(term[p][0], shift, 1)
            b = pltpu.roll(term[p][1], shift, 1)
            terms[slot, p, 1, spot, :] = jnp.where(low, zero, a)
            terms[slot, p, 2, spot, :] = jnp.where(low, a, b)
            terms[slot, p, 3, spot, :] = jnp.where(low, b, zero)
        return c

    lax.fori_loop(0, STEPS, spread, 0, unroll=UNROLL)


def body(
    rows_ref, cols_ref, counts_ref, object_in, probe_in, mags_in, tables_in, sort_in,
    object_out, probe_out, errors,
    obj, probes, grad, pgrad, terms, stats, mags, tables, sort, win, wave, half, field,
    core_in, acc, one_in, one, two_in, z_in, tile_in, tile_z, tile_core,
    col_in, row_in, mid, rdma_send, rdma_recv, local, ready,
):
    row, col, core, coords, along, partner, tile = where_am_i()
    up, down = tile((row + 7) % 8, col), tile((row + 1) % 8, col)
    left, right = tile(row, (col + 15) % 16), tile(row, (col + 1) % 16)
    has_left, has_right, has_up, has_down = col > 0, col < 15, row > 0, row < 7
    greeted = [partner, up, down, left, right]
    for axis in ("x", "y", "z"):
        for d in (1, 2, 3):
            greeted.append(along(axis, (coords[axis] + d) % 4))

    def greet(sem):
        for peer in greeted:
            pl.semaphore_signal(sem, inc=1, device_id=peer, device_id_type=pl.DeviceIdType.MESH)

    barrier = pltpu.get_barrier_semaphore()
    greet(barrier)

    loads = []

    def load(src, dst):
        copy = pltpu.make_async_copy(src, dst, local.at[len(loads)])
        copy.start()
        loads.append(copy)

    for j in range(2):
        load(object_in.at[:, :, j * 128:(j + 1) * 128], obj.at[:, 1 + j, HALF:HALF + SIDE, :])
    for j in range(2):
        load(
            probe_in.at[:, :, :, j * 128:(j + 1) * 128],
            probes.at[0, :, :, j * SIDE:(j + 1) * SIDE, :],
        )
    load(tables_in, tables)
    load(sort_in, sort)
    load(mags_in.at[0, 0], mags)

    count = [0]

    def message(src, dst, peer):
        n = count[0]
        count[0] += 1
        return pltpu.make_async_remote_copy(
            src_ref=src, dst_ref=dst, send_sem=rdma_send.at[n], recv_sem=rdma_recv.at[n],
            device_id=peer, device_id_type=pl.DeviceIdType.MESH,
        )

    def send(src, dst, peer):
        copy = message(src, dst, peer)
        copy.start()
        return copy

    def wait(copies):
        for copy in copies:
            copy.wait()

    def halo_messages(p):
        return [
            message(obj.at[p, 2], obj.at[p, 0], right),
            message(obj.at[p, 1], obj.at[p, 3], left),
        ]

    def start_halo(pair):
        @pl.when(has_right)
        def _():
            pair[0].start()

        @pl.when(has_left)
        def _():
            pair[1].start()

    def wait_halo(pair):
        @pl.when(has_right)
        def _():
            pair[0].wait_send()
            pair[1].wait_recv()

        @pl.when(has_left)
        def _():
            pair[1].wait_send()
            pair[0].wait_recv()

    pl.semaphore_wait(barrier, len(greeted))
    wait(loads[0:2])
    first = [
        [
            send(obj.at[p, 1:3, HALF:SIDE, :], row_in.at[1, p, :, 0:HALF, :], up),
            send(obj.at[p, 1:3, SIDE:SIDE + HALF, :], row_in.at[0, p, :, 0:HALF, :], down),
        ]
        for p in range(2)
    ]

    @pl.when(jnp.logical_not(has_left))
    def _():
        obj[:, 0] = jnp.zeros((2, EXT, 128), F32)

    @pl.when(jnp.logical_not(has_right))
    def _():
        obj[:, 3] = jnp.zeros((2, EXT, 128), F32)

    def clear(i, c):
        at = pl.multiple_of(i * 64, 64)
        nothing = jnp.zeros((64, 128), F32)
        for s in range(SLOTS):
            for p in range(2):
                for b in range(5):
                    terms[s, p, b, pl.ds(at, 64), :] = nothing
        return c

    lax.fori_loop(0, 12, clear, 0)
    pgrad[...] = jnp.zeros_like(pgrad)
    wait(loads[2:7])

    def pieces(x):
        high = x.astype(BF16)
        rest = x - high.astype(F32)
        middle = rest.astype(BF16)
        return (high, middle, (rest - middle.astype(F32)).astype(BF16))

    def arrange(n, c):
        b, s = n // SLOTS, n % SLOTS
        x = sum(jnp.dot(sort[0], v, preferred_element_type=F32) for v in pieces(mags[b, s]))
        mags[b, s] = sum(jnp.dot(v, sort[1], preferred_element_type=F32) for v in pieces(x))
        return c

    lax.fori_loop(0, BATCHES * SLOTS, arrange, 0)

    halo = [halo_messages(p) for p in range(2)]
    for p in range(2):
        wait(first[p])
        for j in range(2):
            obj[p, 1 + j, 0:HALF, :] = jnp.where(has_up, row_in[0, p, j, 0:HALF, :], 0.0)
            obj[p, 1 + j, SIDE + HALF:EXT, :] = jnp.where(has_down, row_in[1, p, j, 0:HALF, :], 0.0)
        start_halo(halo[p])
    for p in range(2):
        wait_halo(halo[p])
    greet(ready)

    base = count[0]

    def update(u, carry):
        count[0] = base
        batch = u % BATCHES
        now = u % 2
        probe, fresh = probes.at[now], probes.at[1 - now]
        stats[...] = jnp.zeros_like(stats)

        def one_slot(slot, c):
            visit(
                batch, slot, rows_ref, cols_ref, counts_ref, obj, probe, mags, tables,
                terms, pgrad, stats, win, wave, half, field,
            )
            return c

        lax.fori_loop(0, SLOTS, one_slot, 0)

        spots = []
        for s in range(SLOTS):
            row0 = rows_ref[0, 0, batch, s]
            col0 = cols_ref[0, 0, batch, s]
            spots.append((1 - lax.shift_right_logical(col0, 7), SIDE - row0))

        def add_terms(p, b):
            def chunk(i, c):
                at = pl.multiple_of(i * 32, 32)
                grad[p, b, pl.ds(at, 32), :] = sum(
                    terms[s, p, spots[s][0] + b, pl.ds(spots[s][1] + at, 32), :] for s in range(SLOTS)
                )
                return c

            lax.fori_loop(0, EXT // 32, chunk, 0, unroll=4)

        pl.semaphore_wait(ready, len(greeted))

        core_sent = [
            send(stats, tile_core, partner),
            send(pgrad.at[1 - core], core_in, partner),
        ]
        cols_sent = []
        for p in range(2):
            add_terms(p, 3)
            cols = [send(grad.at[p, 3], col_in.at[0, p], right)]
            add_terms(p, 0)
            cols.append(send(grad.at[p, 0], col_in.at[1, p], left))
            cols_sent.append(cols)

        def scatter(phase, source, landing, length, tile_value):
            me = coords[ORDERS[0][phase]]
            tile_in[phase, me] = tile_value
            slot = tile_in.at[phase, me]
            sent = []
            for d in (2, 1, 3):
                sent.append(send(slot, slot, along(ORDERS[0][phase], (me + d) % 4)))
                for g in range(2):
                    axis = ORDERS[g][phase]
                    to = (coords[axis] + d) % 4
                    at = pl.multiple_of(to * length, length)
                    sent.append(
                        send(
                            source.at[2 * g:2 * g + 2, pl.ds(at, length), :],
                            landing.at[d - 1, 2 * g:2 * g + 2],
                            along(axis, to),
                        )
                    )
            return sent

        def gather_sum(phase, source, landing, length):
            out = []
            for g in range(2):
                at = pl.multiple_of(coords[ORDERS[g][phase]] * length, length)
                for k in (2 * g, 2 * g + 1):
                    out.append(
                        source[k, pl.ds(at, length), :] + landing[0, k] + landing[1, k] + landing[2, k]
                    )
            return out

        def tile_total(phase):
            return (tile_in[phase, 0] + tile_in[phase, 1]) + (tile_in[phase, 2] + tile_in[phase, 3])

        def send_rows(p, j):
            outer = [
                send(mid.at[p, j, 0:HALF, :], row_in.at[1, p, j, 0:HALF], up),
                send(mid.at[p, j, SIDE + HALF:EXT, :], row_in.at[0, p, j, HALF:SIDE], down),
            ]
            inner = [
                message(mid.at[p, j, HALF:SIDE, :], row_in.at[1, p, j, HALF:SIDE], up),
                message(mid.at[p, j, SIDE:SIDE + HALF, :], row_in.at[0, p, j, 0:HALF], down),
            ]

            @pl.when(u < UPDATES - 1)
            def _():
                inner[0].start()
                inner[1].start()

            return (outer, inner)

        def wait_rows(pair):
            for outer, inner in pair:
                wait(outer)

            @pl.when(u < UPDATES - 1)
            def _():
                for outer, inner in pair:
                    wait(inner)

        def make_mid(p):
            wait(cols_sent[p])
            mid[p, 0] = grad[p, 1] + jnp.where(has_left, col_in[0, p], 0.0)
            mid[p, 1] = grad[p, 2] + jnp.where(has_right, col_in[1, p], 0.0)

        wait(core_sent)
        for k in range(MODES):
            acc[k] = pgrad[core, k] + core_in[k]
        sent = scatter(0, acc, one_in, 128, stats[...] + tile_core[...])

        def peak_step(i, best):
            at = pl.multiple_of(i * 16, 16)
            total = None
            for p in range(2):
                for k in range(MODES):
                    v = probe[p, k, pl.ds(at, 16), :]
                    total = v * v if total is None else total + v * v
            return jnp.maximum(best, jnp.maximum(total[0:8], total[8:16]))

        best = lax.fori_loop(0, EXT // 16, peak_step, jnp.zeros((8, 128), F32), unroll=4)
        rate = object_rate / (jnp.max(best) + tiny_value)

        def update_object(p, j):
            upper = jnp.where(has_up, row_in[0, p, j], 0.0)
            lower = jnp.where(has_down, row_in[1, p, j], 0.0)
            top = mid[p, j, 0:SIDE, :] + upper
            low = mid[p, j, SIDE:EXT, :] + lower
            rate_up = jnp.where(has_up, rate, 0.0)
            rate_down = jnp.where(has_down, rate, 0.0)
            b = 1 + j
            obj[p, b, 0:HALF, :] = obj[p, b, 0:HALF, :] + rate_up * top[0:HALF]
            obj[p, b, HALF:SIDE, :] = obj[p, b, HALF:SIDE, :] + rate * top[HALF:SIDE]
            obj[p, b, SIDE:SIDE + HALF, :] = obj[p, b, SIDE:SIDE + HALF, :] + rate * low[0:HALF]
            obj[p, b, SIDE + HALF:EXT, :] = obj[p, b, SIDE + HALF:EXT, :] + rate_down * low[HALF:SIDE]

        for p in range(2):
            add_terms(p, 1)
            add_terms(p, 2)
        make_mid(0)
        rows_sent = [send_rows(0, 0), send_rows(0, 1)]

        wait(sent)
        for k, v in enumerate(gather_sum(0, acc, one_in, 128)):
            one[k] = v
        sent = scatter(1, one, two_in, 32, tile_total(0))

        make_mid(1)

        wait(sent)
        z = coords["z"]
        for k, v in enumerate(gather_sum(1, one, two_in, 32)):
            z_in[z, k] = v
        tile_z[z] = tile_total(1)
        sent = []
        for d in (2, 1, 3):
            peer = along("z", (z + d) % 4)
            sent.append(send(tile_z.at[z], tile_z.at[z], peer))
            sent.append(send(z_in.at[z], z_in.at[z], peer))
        pgrad[...] = jnp.zeros_like(pgrad)
        rows_sent.append(send_rows(1, 0))
        wait(sent)

        totals = (tile_z[0] + tile_z[1]) + (tile_z[2] + tile_z[3])
        errors[u] = totals[1]
        gain = probe_rate * SIDE * SIDE / jnp.sum(totals[0])
        starts = []
        for g in range(2):
            a, b = coords[ORDERS[g][0]], coords[ORDERS[g][1]]
            starts.append((a * 128, a * 128 + b * 32))
        for k in range(MODES):
            spot = pl.ds(pl.multiple_of(starts[k // 2][1], 32), 32)
            total = (z_in[0, k] + z_in[1, k]) + (z_in[2, k] + z_in[3, k])
            fresh[core, k, spot, :] = probe[core, k, spot, :] + gain * total

        def block_of(g, at, length):
            at = pl.multiple_of(at, length)
            return fresh.at[core, 2 * g:2 * g + 2, pl.ds(at, length), :]

        def spread(phase, length):
            out = {}
            for d in (2, 1, 3):
                for g in range(2):
                    axis = ORDERS[g][phase]
                    block = block_of(g, starts[g][phase], length)
                    out[d, g] = send(block, block, along(axis, (coords[axis] + d) % 4))
            return out

        out2 = spread(1, 32)
        rows_sent.append(send_rows(1, 1))
        halo = [halo_messages(p) for p in range(2)]

        def finish_object(p):
            wait_rows(rows_sent[2 * p:2 * p + 2])
            for j in range(2):
                update_object(p, j)

            @pl.when(u < UPDATES - 1)
            def _():
                start_halo(halo[p])

        wait(out2.values())
        out1 = spread(0, 128)
        finish_object(0)
        to_core = []
        for g in range(2):
            block = block_of(g, starts[g][0], 128)
            to_core.append(send(block, block, partner))

        for d in (1, 3, 2):
            for g in range(2):
                out1[d, g].wait()
                axis = ORDERS[g][0]
                block = block_of(g, (coords[axis] + 4 - d) % 4 * 128, 128)
                to_core.append(send(block, block, partner))

        finish_object(1)
        wait(to_core)

        @pl.when(u < UPDATES - 1)
        def _():
            for p in range(2):
                wait_halo(halo[p])
            greet(ready)

        return carry

    lax.fori_loop(0, UPDATES, update, 0)

    stores = []
    for j in range(2):
        stores.append(
            pltpu.make_async_copy(
                obj.at[:, 1 + j, HALF:HALF + SIDE, :], object_out.at[:, :, j * 128:(j + 1) * 128], local.at[j]
            )
        )
        stores.append(
            pltpu.make_async_copy(
                probes.at[UPDATES % 2, :, :, j * SIDE:(j + 1) * SIDE, :],
                probe_out.at[:, :, :, j * 128:(j + 1) * 128],
                local.at[2 + j],
            )
        )
    for copy in stores:
        copy.start()
    wait(stores)


def on_device(object_field, probe, pos_rows, pos_cols, counts, magnitudes):
    tables = tuple(jnp.asarray(t) for t in transform_tables())
    anywhere = pl.BlockSpec(memory_space=pl.ANY)
    whole = pl.BlockSpec(memory_space=pltpu.VMEM)
    smem = pl.BlockSpec(memory_space=pltpu.SMEM)
    messages = 96
    out, probe_out, errors = pl.pallas_call(
        body,
        out_shape=(
            jax.ShapeDtypeStruct((2, SIDE, SIDE), F32),
            jax.ShapeDtypeStruct((2, MODES, SIDE, SIDE), F32),
            jax.ShapeDtypeStruct((UPDATES, 8, 128), F32),
        ),
        in_specs=[smem, smem, smem] + [anywhere] * 5,
        out_specs=(anywhere, anywhere, whole),
        scratch_shapes=[
            pltpu.VMEM((2, 4, EXT, 128), F32),
            pltpu.VMEM((2, 2, MODES, EXT, 128), F32),
            pltpu.VMEM((2, 4, EXT, 128), F32),
            pltpu.VMEM((2, MODES, EXT, 128), F32),
            pltpu.VMEM((SLOTS, 2, 5, 3 * SIDE, 128), F32),
            pltpu.VMEM((2, 8, 128), F32),
            pltpu.VMEM((BATCHES, SLOTS, SIDE, SIDE), F32),
            pltpu.VMEM((8, SIDE, SIDE), BF16),
            pltpu.VMEM((2, SIDE, SIDE), BF16),
            pltpu.VMEM((2, 2, SIDE, 128), F32),
            pltpu.VMEM((MODES, 2, SIDE, SIDE), BF16),
            pltpu.VMEM((2, MODES * SIDE, SIDE), BF16),
            pltpu.VMEM((2, MODES * SIDE, SIDE), F32),
            pltpu.VMEM((MODES, EXT, 128), F32),
            pltpu.VMEM((MODES, EXT, 128), F32),
            pltpu.VMEM((3, MODES, 128, 128), F32),
            pltpu.VMEM((MODES, 128, 128), F32),
            pltpu.VMEM((3, MODES, 32, 128), F32),
            pltpu.VMEM((4, MODES, 32, 128), F32),
            pltpu.VMEM((2, 4, 2, 8, 128), F32),
            pltpu.VMEM((4, 2, 8, 128), F32),
            pltpu.VMEM((2, 8, 128), F32),
            pltpu.VMEM((2, 2, EXT, 128), F32),
            pltpu.VMEM((2, 2, 2, SIDE, 128), F32),
            pltpu.VMEM((2, 2, EXT, 128), F32),
            pltpu.SemaphoreType.DMA((messages,)),
            pltpu.SemaphoreType.DMA((messages,)),
            pltpu.SemaphoreType.DMA((8,)),
            pltpu.SemaphoreType.REGULAR,
        ],
        cost_estimate=pl.CostEstimate(flops=80 << 30, bytes_accessed=12 << 20, transcendentals=0),
        compiler_params=pltpu.CompilerParams(
            collective_id=0, has_side_effects=True, vmem_limit_bytes=60 << 20
        ),
        name="whole_sweep",
    )(
        pos_rows, pos_cols, counts,
        object_field, probe, magnitudes, *tables,
    )
    return (out, probe_out, jnp.sum(errors, axis=(1, 2)))


def solution(mesh):
    finer = Mesh(mesh.devices.reshape(4, 2, 4, 2, 2), AXES)
    return jax.shard_map(
        on_device,
        mesh=finer,
        in_specs=(
            P(None, ROW, COL),
            P(),
            P(ROW, COL, None, None),
            P(ROW, COL, None, None),
            P(ROW, COL, None),
            P(ROW, COL, None, None, None, None),
        ),
        out_specs=(P(None, ROW, COL), P(), P()),
        check_vma=False,
    )
```

```python
import functools
import math

import jax
import jax.numpy as jnp
import numpy as np
from jax import lax
from jax.experimental import pallas as pl
from jax.experimental.pallas import tpu as pltpu
from jax.sharding import Mesh
from jax.sharding import PartitionSpec as P

BATCHES = 2
ITERS = 2
SLOTS = 3
MODES = 4
SIDE = 256
HALF = 128
EXT = 512
UPDATES = BATCHES * ITERS
AXES = ("row_0", "row_1", "col_0", "col_1", "col_2")
ROW = ("row_0", "row_1")
COL = ("col_0", "col_1", "col_2")
F32 = jnp.float32
BF16 = jnp.bfloat16

object_rate = 0.9
probe_rate = 0.5
floor_value = 0.5
tiny_value = 1e-06


def transform_tables():
    index = np.arange(SIDE)
    angles = (index[:, None] * index[None, :] % SIDE) * (2.0 * math.pi / SIDE)
    scale = 1.0 / math.sqrt(SIDE)
    c = np.cos(angles) * scale
    s = -np.sin(angles) * scale
    near = np.arange(HALF)
    tables = []
    for parity in range(2):
        pick = np.arange(parity, SIDE, 2)
        cr, sr = c[np.ix_(pick, near)], s[np.ix_(pick, near)]
        tables.append(np.block([[cr, -sr], [sr, cr]]))
    for parity in range(2):
        pick = np.arange(parity, SIDE, 2)
        cr, sr = c[np.ix_(near, pick)], s[np.ix_(near, pick)]
        tables.append(np.block([[cr, sr], [-sr, cr]]))
    tables = tables + [t.T for t in tables]
    order = np.concatenate([np.arange(0, SIDE, 2), np.arange(1, SIDE, 2)])
    sort = np.eye(SIDE)[order]
    return (np.stack(tables).astype(jnp.bfloat16), np.stack([sort, sort.T]).astype(jnp.bfloat16))


def where_am_i():
    y, lo, x, hi, core = (lax.axis_index(name) for name in AXES)
    row, col = y * 2 + lo, x * 4 + hi * 2 + core
    z = hi * 2 + lo

    def tile(r, c):
        return (r // 2, r % 2, c // 4, (c // 2) % 2, c % 2)

    def along(axis, value):
        if axis == "x":
            return (y, lo, value, hi, core)
        if axis == "y":
            return (value, lo, x, hi, core)
        return (y, value % 2, x, value // 2, core)

    partner = (y, lo, x, hi, 1 - core)
    coords = {"x": x, "y": y, "z": z}
    return row, col, core, coords, along, partner, tile


ORDERS = (("x", "y", "z"), ("y", "x", "z"))
CH = 16
STEPS = SIDE // CH
UNROLL = 4


def fold(x):
    total = x[0:8, :]
    for i in range(1, x.shape[0] // 8):
        total = total + x[8 * i:8 * i + 8, :]
    return total


def visit(
    batch, slot, rows_ref, cols_ref, counts_ref, obj, probe, mags, tables,
    terms, pgrad, stats, win, wave, half, field,
):
    lane = lax.broadcasted_iota(jnp.int32, (CH, 128), 1)
    row0 = rows_ref[0, 0, batch, slot]
    col0 = cols_ref[0, 0, batch, slot]
    live = jnp.where(slot < counts_ref[0, 0, batch], 1.0, 0.0).astype(F32)
    block = lax.shift_right_logical(col0, 7)
    shift = col0 & 127
    back = (128 - shift) & 127
    none = jnp.zeros((8, 128), F32)

    def make_exit(i, power):
        at = pl.multiple_of(i * CH, CH)
        keep = lane < 128 - shift
        w = []
        for h in range(2):
            for p in range(2):
                rolled = [
                    pltpu.roll(obj[p, block + j, pl.ds(row0 + h * HALF + at, CH), :], back, 1)
                    for j in range(3)
                ]
                w.append([jnp.where(keep, rolled[j], rolled[j + 1]) for j in range(2)])
        for j in range(2):
            for h in range(2):
                wr, wi = w[2 * h][j], w[2 * h + 1][j]
                win[0, j, pl.ds(h * HALF + at, CH), :] = wr
                win[1, j, pl.ds(h * HALF + at, CH), :] = wi
                power = power + fold(wr * wr + wi * wi)
            for k in range(MODES):
                re, im = [], []
                for h in range(2):
                    wr, wi = w[2 * h][j], w[2 * h + 1][j]
                    pr = probe[0, k, pl.ds(j * SIDE + h * HALF + at, CH), :]
                    pi = probe[1, k, pl.ds(j * SIDE + h * HALF + at, CH), :]
                    re.append(pr * wr - pi * wi)
                    im.append(pr * wi + pi * wr)
                cols = slice(j * 128, (j + 1) * 128)
                wave[k, 0, pl.ds(at, CH), cols] = (re[0] + re[1]).astype(BF16)
                wave[k, 0, pl.ds(HALF + at, CH), cols] = (im[0] + im[1]).astype(BF16)
                wave[k, 1, pl.ds(at, CH), cols] = (re[0] - re[1]).astype(BF16)
                wave[k, 1, pl.ds(HALF + at, CH), cols] = (im[0] - im[1]).astype(BF16)
        return power

    power = lax.fori_loop(0, STEPS // 2, make_exit, none, unroll=UNROLL // 2)
    stats[0] = stats[0] + live * power

    for k in range(MODES):
        for parity in range(2):
            res = jnp.dot(tables[parity], wave[k, parity], preferred_element_type=F32)
            spot = slice(k * SIDE + parity * HALF, k * SIDE + (parity + 1) * HALF)
            for o in range(2):
                near = res[o * HALF:(o + 1) * HALF, 0:HALF]
                far = res[o * HALF:(o + 1) * HALF, HALF:SIDE]
                half[0, spot, o * HALF:(o + 1) * HALF] = (near + far).astype(BF16)
                half[1, spot, o * HALF:(o + 1) * HALF] = (near - far).astype(BF16)
    for parity in range(2):
        field[parity] = jnp.dot(half[parity], tables[4 + parity], preferred_element_type=F32)

    def correct(i, misfit):
        at = pl.multiple_of(i * CH, CH)
        parity = i // (STEPS // 2)
        to = pl.multiple_of((i % (STEPS // 2)) * CH, CH)
        for q in range(2):
            parts = [
                (field[q, pl.ds(k * SIDE + at, CH), 0:HALF], field[q, pl.ds(k * SIDE + at, CH), HALF:SIDE])
                for k in range(MODES)
            ]
            total = sum(re * re + im * im for re, im in parts)
            modulus = jnp.sqrt(total)
            amplitude = mags[batch, slot, pl.ds(at, CH), q * HALF:(q + 1) * HALF]
            factor = live * (amplitude / jnp.maximum(modulus, floor_value) - 1.0)
            gap = modulus - amplitude
            misfit = misfit + fold(gap * gap)
            cols = slice(q * HALF, (q + 1) * HALF)
            for k in range(MODES):
                wave[k, parity, pl.ds(to, CH), cols] = (parts[k][0] * factor).astype(BF16)
                wave[k, parity, pl.ds(HALF + to, CH), cols] = (parts[k][1] * factor).astype(BF16)
        return misfit

    misfit = lax.fori_loop(0, STEPS, correct, none, unroll=UNROLL)
    stats[1] = stats[1] + live * misfit

    for k in range(MODES):
        even = jnp.dot(tables[2], wave[k, 0], preferred_element_type=F32)
        odd = jnp.dot(tables[3], wave[k, 1], preferred_element_type=F32)
        for h, value in enumerate(((even + odd).astype(BF16), (even - odd).astype(BF16))):
            spot = slice(k * SIDE + h * HALF, k * SIDE + (h + 1) * HALF)
            for o in range(2):
                for q in range(2):
                    half[q, spot, o * HALF:(o + 1) * HALF] = value[
                        o * HALF:(o + 1) * HALF, q * HALF:(q + 1) * HALF
                    ]
    for parity in range(2):
        field[parity] = jnp.dot(half[parity], tables[6 + parity], preferred_element_type=F32)

    def spread(i, c):
        at = pl.multiple_of(i * CH, CH)
        term = [[None, None], [None, None]]
        for j in range(2):
            wr = win[0, j, pl.ds(at, CH), :]
            wi = win[1, j, pl.ds(at, CH), :]
            tr = ti = None
            for k in range(MODES):
                source = pl.ds(k * SIDE + at, CH)
                if j == 0:
                    ur = field[0, source, 0:HALF] + field[1, source, 0:HALF]
                    ui = field[0, source, HALF:SIDE] + field[1, source, HALF:SIDE]
                else:
                    ur = field[0, source, 0:HALF] - field[1, source, 0:HALF]
                    ui = field[0, source, HALF:SIDE] - field[1, source, HALF:SIDE]
                spot = pl.ds(j * SIDE + at, CH)
                pr = probe[0, k, spot, :]
                pi = probe[1, k, spot, :]
                ar = pr * ur + pi * ui
                ai = pr * ui - pi * ur
                tr = ar if tr is None else tr + ar
                ti = ai if ti is None else ti + ai
                pgrad[0, k, spot, :] = pgrad[0, k, spot, :] + (wr * ur + wi * ui)
                pgrad[1, k, spot, :] = pgrad[1, k, spot, :] + (wr * ui - wi * ur)
            term[0][j], term[1][j] = tr, ti
        low = lane < shift
        zero = jnp.zeros((CH, 128), F32)
        spot = pl.ds(SIDE + at, CH)
        for p in range(2):
            a = pltpu.roll(term[p][0], shift, 1)
            b = pltpu.roll(term[p][1], shift, 1)
            terms[slot, p, 1, spot, :] = jnp.where(low, zero, a)
            terms[slot, p, 2, spot, :] = jnp.where(low, a, b)
            terms[slot, p, 3, spot, :] = jnp.where(low, b, zero)
        return c

    lax.fori_loop(0, STEPS, spread, 0, unroll=UNROLL)


def body(
    rows_ref, cols_ref, counts_ref, object_in, probe_in, mags_in, tables_in, sort_in,
    object_out, probe_out, errors,
    obj, probes, grad, pgrad, terms, stats, mags, tables, sort, win, wave, half, field,
    core_in, acc, one_in, one, two_in, z_in, tile_in, tile_z, tile_core,
    inner_in, side_in, corner_in, row_in, rdma_send, rdma_recv, local, ready,
):
    row, col, core, coords, along, partner, tile = where_am_i()
    up, down = tile((row + 7) % 8, col), tile((row + 1) % 8, col)
    beside = (col + 15 + 2 * core) % 16
    outer = tile(row, beside)
    outer_up, outer_down = tile((row + 7) % 8, beside), tile((row + 1) % 8, beside)
    has_up, has_down = row > 0, row < 7
    has_outer = jnp.where(core == 0, col > 0, col < 15)
    inner_halo, outer_halo = 3 * (1 - core), 3 * core
    inner_own, outer_own = 2 - core, 1 + core
    greeted = [partner, outer, up, down, outer_up, outer_down]
    for axis in ("x", "y", "z"):
        for d in (1, 2, 3):
            greeted.append(along(axis, (coords[axis] + d) % 4))

    def greet(sem):
        for peer in greeted:
            pl.semaphore_signal(sem, inc=1, device_id=peer, device_id_type=pl.DeviceIdType.MESH)

    for p in range(2):
        for b in (0, 3):
            obj[p, b] = jnp.zeros((EXT, 128), F32)
        for b in (1, 2):
            obj[p, b, 0:HALF, :] = jnp.zeros((HALF, 128), F32)
            obj[p, b, SIDE + HALF:EXT, :] = jnp.zeros((HALF, 128), F32)
    barrier = pltpu.get_barrier_semaphore()
    greet(barrier)

    loads = []

    def load(src, dst):
        copy = pltpu.make_async_copy(src, dst, local.at[len(loads)])
        copy.start()
        loads.append(copy)

    for j in range(2):
        load(object_in.at[:, :, j * 128:(j + 1) * 128], obj.at[:, 1 + j, HALF:HALF + SIDE, :])
    for j in range(2):
        load(
            probe_in.at[:, :, :, j * 128:(j + 1) * 128],
            probes.at[0, :, :, j * SIDE:(j + 1) * SIDE, :],
        )
    load(tables_in, tables)
    load(sort_in, sort)
    load(mags_in.at[0, 0], mags)

    count = [0]

    def message(src, dst, peer):
        n = count[0]
        count[0] += 1
        return pltpu.make_async_remote_copy(
            src_ref=src, dst_ref=dst, send_sem=rdma_send.at[n], recv_sem=rdma_recv.at[n],
            device_id=peer, device_id_type=pl.DeviceIdType.MESH,
        )

    def send(src, dst, peer):
        copy = message(src, dst, peer)
        copy.start()
        return copy

    def wait(copies):
        for copy in copies:
            copy.wait()

    class Halo:
        def __init__(self, p):
            both = jnp.logical_and
            own, top, low = slice(HALF, SIDE + HALF), slice(HALF, SIDE), slice(SIDE, SIDE + HALF)
            above, below = slice(0, HALF), slice(SIDE + HALF, EXT)
            there = 3 * (1 - core)
            self.parts = [
                (message(obj.at[p, 1:3, top, :], obj.at[p, 1:3, below, :], up), has_up, has_down),
                (message(obj.at[p, 1:3, low, :], obj.at[p, 1:3, above, :], down), has_down, has_up),
                (message(obj.at[p, outer_own, own, :], obj.at[p, there, own, :], outer), has_outer, has_outer),
                (
                    message(obj.at[p, outer_own, top, :], obj.at[p, there, below, :], outer_up),
                    both(has_up, has_outer), both(has_down, has_outer),
                ),
                (
                    message(obj.at[p, outer_own, low, :], obj.at[p, there, above, :], outer_down),
                    both(has_down, has_outer), both(has_up, has_outer),
                ),
            ]
            self.inner = message(obj.at[p, inner_own], obj.at[p, 3 * core], partner)

        def start(self):
            for copy, sends, _ in self.parts:
                @pl.when(sends)
                def _():
                    copy.start()

        def wait_some(self, parts):
            for copy, sends, takes in parts:
                @pl.when(sends)
                def _():
                    copy.wait_send()

                @pl.when(takes)
                def _():
                    copy.wait_recv()

        def turn(self):
            self.wait_some(self.parts[0:2])
            self.inner.start()

        def finish(self):
            self.wait_some(self.parts[2:])
            self.inner.wait()

    pl.semaphore_wait(barrier, len(greeted))
    wait(loads[0:2])
    halo = [Halo(p) for p in range(2)]
    for p in range(2):
        halo[p].start()

    def clear(i, c):
        at = pl.multiple_of(i * 64, 64)
        nothing = jnp.zeros((64, 128), F32)
        for s in range(SLOTS):
            for p in range(2):
                for b in range(5):
                    terms[s, p, b, pl.ds(at, 64), :] = nothing
        return c

    lax.fori_loop(0, 12, clear, 0)
    pgrad[...] = jnp.zeros_like(pgrad)
    wait(loads[2:7])

    def pieces(x):
        high = x.astype(BF16)
        rest = x - high.astype(F32)
        middle = rest.astype(BF16)
        return (high, middle, (rest - middle.astype(F32)).astype(BF16))

    def arrange(n, c):
        b, s = n // SLOTS, n % SLOTS
        x = sum(jnp.dot(sort[0], v, preferred_element_type=F32) for v in pieces(mags[b, s]))
        mags[b, s] = sum(jnp.dot(v, sort[1], preferred_element_type=F32) for v in pieces(x))
        return c

    lax.fori_loop(0, BATCHES * SLOTS, arrange, 0)

    for p in range(2):
        halo[p].turn()
    for p in range(2):
        halo[p].finish()
    greet(ready)

    base = count[0]

    def update(u, carry):
        count[0] = base
        batch = u % BATCHES
        now = u % 2
        probe, fresh = probes.at[now], probes.at[1 - now]
        stats[...] = jnp.zeros_like(stats)

        def one_slot(slot, c):
            visit(
                batch, slot, rows_ref, cols_ref, counts_ref, obj, probe, mags, tables,
                terms, pgrad, stats, win, wave, half, field,
            )
            return c

        lax.fori_loop(0, SLOTS, one_slot, 0)

        spots = []
        for s in range(SLOTS):
            row0 = rows_ref[0, 0, batch, s]
            col0 = cols_ref[0, 0, batch, s]
            spots.append((1 - lax.shift_right_logical(col0, 7), SIDE - row0))

        def add_terms(p, b):
            def chunk(i, c):
                at = pl.multiple_of(i * 32, 32)
                grad[p, b, pl.ds(at, 32), :] = sum(
                    terms[s, p, spots[s][0] + b, pl.ds(spots[s][1] + at, 32), :] for s in range(SLOTS)
                )
                return c

            lax.fori_loop(0, EXT // 32, chunk, 0, unroll=4)

        pl.semaphore_wait(ready, len(greeted))

        inner_sent, outer_sent = [], []
        for p in range(2):
            add_terms(p, inner_halo)
            inner_sent.append(send(grad.at[p, inner_halo], inner_in.at[p], partner))
        core_sent = [
            send(stats, tile_core, partner),
            send(pgrad.at[1 - core], core_in, partner),
        ]
        for p in range(2):
            add_terms(p, outer_halo)
            outer_sent.append([
                send(grad.at[p, outer_halo, HALF:SIDE + HALF, :], side_in.at[p], outer),
                send(grad.at[p, outer_halo, 0:HALF, :], corner_in.at[p, HALF:SIDE, :], outer_up),
                send(grad.at[p, outer_halo, SIDE + HALF:EXT, :], corner_in.at[p, 0:HALF, :], outer_down),
            ])

        def scatter(phase, source, landing, length, tile_value):
            me = coords[ORDERS[0][phase]]
            tile_in[phase, me] = tile_value
            slot = tile_in.at[phase, me]
            sent = []
            for d in (2, 1, 3):
                sent.append(send(slot, slot, along(ORDERS[0][phase], (me + d) % 4)))
                for g in range(2):
                    axis = ORDERS[g][phase]
                    to = (coords[axis] + d) % 4
                    at = pl.multiple_of(to * length, length)
                    sent.append(
                        send(
                            source.at[2 * g:2 * g + 2, pl.ds(at, length), :],
                            landing.at[d - 1, 2 * g:2 * g + 2],
                            along(axis, to),
                        )
                    )
            return sent

        def gather_sum(phase, source, landing, length):
            out = []
            for g in range(2):
                at = pl.multiple_of(coords[ORDERS[g][phase]] * length, length)
                for k in (2 * g, 2 * g + 1):
                    out.append(
                        source[k, pl.ds(at, length), :] + landing[0, k] + landing[1, k] + landing[2, k]
                    )
            return out

        def tile_total(phase):
            return (tile_in[phase, 0] + tile_in[phase, 1]) + (tile_in[phase, 2] + tile_in[phase, 3])

        def send_rows(p):
            inner_sent[p].wait()
            grad[p, inner_own] = grad[p, inner_own] + inner_in[p]
            return [
                send(grad.at[p, 1:3, 0:HALF, :], row_in.at[p, :, HALF:SIDE, :], up),
                send(grad.at[p, 1:3, SIDE + HALF:EXT, :], row_in.at[p, :, 0:HALF, :], down),
            ]

        wait(core_sent)
        for k in range(MODES):
            acc[k] = pgrad[core, k] + core_in[k]
        sent = scatter(0, acc, one_in, 128, stats[...] + tile_core[...])

        def peak_step(i, best):
            at = pl.multiple_of(i * 16, 16)
            total = None
            for p in range(2):
                for k in range(MODES):
                    v = probe[p, k, pl.ds(at, 16), :]
                    total = v * v if total is None else total + v * v
            return jnp.maximum(best, jnp.maximum(total[0:8], total[8:16]))

        best = lax.fori_loop(0, EXT // 16, peak_step, jnp.zeros((8, 128), F32), unroll=4)
        rate = object_rate / (jnp.max(best) + tiny_value)

        def finish_object(p):
            wait(rows_sent[p] + outer_sent[p])
            for h, has in ((0, has_up), (1, has_down)):
                there = slice(h * HALF, (h + 1) * HALF)
                here = slice((h + 1) * HALF, (h + 2) * HALF)
                for b in (1, 2):
                    total = grad[p, b, here, :] + jnp.where(has, row_in[p, b - 1, there, :], 0.0)
                    side = side_in[p, there, :] + jnp.where(has, corner_in[p, there, :], 0.0)
                    total = total + jnp.where(jnp.logical_and(has_outer, outer_own == b), side, 0.0)
                    obj[p, b, here, :] = obj[p, b, here, :] + rate * total

            @pl.when(u < UPDATES - 1)
            def _():
                halo[p].start()

        for p in range(2):
            add_terms(p, 1)
            add_terms(p, 2)
        rows_sent = [send_rows(p) for p in range(2)]

        wait(sent)
        for k, v in enumerate(gather_sum(0, acc, one_in, 128)):
            one[k] = v
        sent = scatter(1, one, two_in, 32, tile_total(0))

        wait(sent)
        z = coords["z"]
        for k, v in enumerate(gather_sum(1, one, two_in, 32)):
            z_in[z, k] = v
        tile_z[z] = tile_total(1)
        sent = []
        for d in (2, 1, 3):
            peer = along("z", (z + d) % 4)
            sent.append(send(tile_z.at[z], tile_z.at[z], peer))
            sent.append(send(z_in.at[z], z_in.at[z], peer))
        pgrad[...] = jnp.zeros_like(pgrad)
        halo = [Halo(p) for p in range(2)]
        for p in range(2):
            finish_object(p)
        wait(sent)

        totals = (tile_z[0] + tile_z[1]) + (tile_z[2] + tile_z[3])
        errors[u] = totals[1]
        gain = probe_rate * SIDE * SIDE / jnp.sum(totals[0])
        starts = []
        for g in range(2):
            a, b = coords[ORDERS[g][0]], coords[ORDERS[g][1]]
            starts.append((a * 128, a * 128 + b * 32))
        for k in range(MODES):
            spot = pl.ds(pl.multiple_of(starts[k // 2][1], 32), 32)
            total = (z_in[0, k] + z_in[1, k]) + (z_in[2, k] + z_in[3, k])
            fresh[core, k, spot, :] = probe[core, k, spot, :] + gain * total

        def block_of(g, at, length):
            at = pl.multiple_of(at, length)
            return fresh.at[core, 2 * g:2 * g + 2, pl.ds(at, length), :]

        def spread(phase, length):
            out = {}
            for d in (2, 1, 3):
                for g in range(2):
                    axis = ORDERS[g][phase]
                    block = block_of(g, starts[g][phase], length)
                    out[d, g] = send(block, block, along(axis, (coords[axis] + d) % 4))
            return out

        out2 = spread(1, 32)
        wait(out2.values())
        out1 = spread(0, 128)
        to_core = []
        for g in range(2):
            block = block_of(g, starts[g][0], 128)
            to_core.append(send(block, block, partner))

        @pl.when(u < UPDATES - 1)
        def _():
            for p in range(2):
                halo[p].turn()

        for d in (1, 3, 2):
            for g in range(2):
                out1[d, g].wait()
                axis = ORDERS[g][0]
                block = block_of(g, (coords[axis] + 4 - d) % 4 * 128, 128)
                to_core.append(send(block, block, partner))

        wait(to_core)

        @pl.when(u < UPDATES - 1)
        def _():
            for p in range(2):
                halo[p].finish()
            greet(ready)

        return carry

    lax.fori_loop(0, UPDATES, update, 0)

    stores = []
    for j in range(2):
        stores.append(
            pltpu.make_async_copy(
                obj.at[:, 1 + j, HALF:HALF + SIDE, :], object_out.at[:, :, j * 128:(j + 1) * 128], local.at[j]
            )
        )
        stores.append(
            pltpu.make_async_copy(
                probes.at[UPDATES % 2, :, :, j * SIDE:(j + 1) * SIDE, :],
                probe_out.at[:, :, :, j * 128:(j + 1) * 128],
                local.at[2 + j],
            )
        )
    for copy in stores:
        copy.start()
    wait(stores)


def on_device(object_field, probe, pos_rows, pos_cols, counts, magnitudes):
    tables = tuple(jnp.asarray(t) for t in transform_tables())
    anywhere = pl.BlockSpec(memory_space=pl.ANY)
    whole = pl.BlockSpec(memory_space=pltpu.VMEM)
    smem = pl.BlockSpec(memory_space=pltpu.SMEM)
    messages = 96
    out, probe_out, errors = pl.pallas_call(
        body,
        out_shape=(
            jax.ShapeDtypeStruct((2, SIDE, SIDE), F32),
            jax.ShapeDtypeStruct((2, MODES, SIDE, SIDE), F32),
            jax.ShapeDtypeStruct((UPDATES, 8, 128), F32),
        ),
        in_specs=[smem, smem, smem] + [anywhere] * 5,
        out_specs=(anywhere, anywhere, whole),
        scratch_shapes=[
            pltpu.VMEM((2, 4, EXT, 128), F32),
            pltpu.VMEM((2, 2, MODES, EXT, 128), F32),
            pltpu.VMEM((2, 4, EXT, 128), F32),
            pltpu.VMEM((2, MODES, EXT, 128), F32),
            pltpu.VMEM((SLOTS, 2, 5, 3 * SIDE, 128), F32),
            pltpu.VMEM((2, 8, 128), F32),
            pltpu.VMEM((BATCHES, SLOTS, SIDE, SIDE), F32),
            pltpu.VMEM((8, SIDE, SIDE), BF16),
            pltpu.VMEM((2, SIDE, SIDE), BF16),
            pltpu.VMEM((2, 2, SIDE, 128), F32),
            pltpu.VMEM((MODES, 2, SIDE, SIDE), BF16),
            pltpu.VMEM((2, MODES * SIDE, SIDE), BF16),
            pltpu.VMEM((2, MODES * SIDE, SIDE), F32),
            pltpu.VMEM((MODES, EXT, 128), F32),
            pltpu.VMEM((MODES, EXT, 128), F32),
            pltpu.VMEM((3, MODES, 128, 128), F32),
            pltpu.VMEM((MODES, 128, 128), F32),
            pltpu.VMEM((3, MODES, 32, 128), F32),
            pltpu.VMEM((4, MODES, 32, 128), F32),
            pltpu.VMEM((2, 4, 2, 8, 128), F32),
            pltpu.VMEM((4, 2, 8, 128), F32),
            pltpu.VMEM((2, 8, 128), F32),
            pltpu.VMEM((2, EXT, 128), F32),
            pltpu.VMEM((2, SIDE, 128), F32),
            pltpu.VMEM((2, SIDE, 128), F32),
            pltpu.VMEM((2, 2, SIDE, 128), F32),
            pltpu.SemaphoreType.DMA((messages,)),
            pltpu.SemaphoreType.DMA((messages,)),
            pltpu.SemaphoreType.DMA((8,)),
            pltpu.SemaphoreType.REGULAR,
        ],
        cost_estimate=pl.CostEstimate(flops=80 << 30, bytes_accessed=12 << 20, transcendentals=0),
        compiler_params=pltpu.CompilerParams(
            collective_id=0, has_side_effects=True, vmem_limit_bytes=60 << 20
        ),
        name="whole_sweep",
    )(
        pos_rows, pos_cols, counts,
        object_field, probe, magnitudes, *tables,
    )
    return (out, probe_out, jnp.sum(errors, axis=(1, 2)))


def solution(mesh):
    finer = Mesh(mesh.devices.reshape(4, 2, 4, 2, 2), AXES)
    return jax.shard_map(
        on_device,
        mesh=finer,
        in_specs=(
            P(None, ROW, COL),
            P(),
            P(ROW, COL, None, None),
            P(ROW, COL, None, None),
            P(ROW, COL, None),
            P(ROW, COL, None, None, None, None),
        ),
        out_specs=(P(None, ROW, COL), P(), P()),
        check_vma=False,
    )
```

```python
import functools
import math

import jax
import jax.numpy as jnp
import numpy as np
from jax import lax
from jax.experimental import pallas as pl
from jax.experimental.pallas import tpu as pltpu
from jax.sharding import Mesh
from jax.sharding import PartitionSpec as P

BATCHES = 2
ITERS = 2
SLOTS = 3
MODES = 4
SIDE = 256
HALF = 128
EXT = 512
UPDATES = BATCHES * ITERS
AXES = ("row_0", "row_1", "col_0", "col_1", "col_2")
ROW = ("row_0", "row_1")
COL = ("col_0", "col_1", "col_2")
F32 = jnp.float32
BF16 = jnp.bfloat16

object_rate = 0.9
probe_rate = 0.5
floor_value = 0.5
tiny_value = 1e-06


def transform_tables():
    index = np.arange(SIDE)
    angles = (index[:, None] * index[None, :] % SIDE) * (2.0 * math.pi / SIDE)
    scale = 1.0 / math.sqrt(SIDE)
    c = np.cos(angles) * scale
    s = -np.sin(angles) * scale
    near = np.arange(HALF)
    tables = []
    for parity in range(2):
        pick = np.arange(parity, SIDE, 2)
        cr, sr = c[np.ix_(pick, near)], s[np.ix_(pick, near)]
        tables.append(np.block([[cr, -sr], [sr, cr]]))
    for parity in range(2):
        pick = np.arange(parity, SIDE, 2)
        cr, sr = c[np.ix_(near, pick)], s[np.ix_(near, pick)]
        tables.append(np.block([[cr, sr], [-sr, cr]]))
    tables = tables + [t.T for t in tables]
    order = np.concatenate([np.arange(0, SIDE, 2), np.arange(1, SIDE, 2)])
    sort = np.eye(SIDE)[order]
    return (np.stack(tables).astype(jnp.bfloat16), np.stack([sort, sort.T]).astype(jnp.bfloat16))


def where_am_i():
    y, lo, x, hi, core = (lax.axis_index(name) for name in AXES)
    row, col = y * 2 + lo, x * 4 + hi * 2 + core
    z = hi * 2 + lo

    def tile(r, c):
        return (r // 2, r % 2, c // 4, (c // 2) % 2, c % 2)

    def along(axis, value):
        if axis == "x":
            return (y, lo, value, hi, core)
        if axis == "y":
            return (value, lo, x, hi, core)
        return (y, value % 2, x, value // 2, core)

    partner = (y, lo, x, hi, 1 - core)
    coords = {"x": x, "y": y, "z": z}
    return row, col, core, coords, along, partner, tile


ORDERS = (("x", "y", "z"), ("y", "x", "z"))
CH = 16
STEPS = SIDE // CH
UNROLL = 4


def fold(x):
    total = x[0:8, :]
    for i in range(1, x.shape[0] // 8):
        total = total + x[8 * i:8 * i + 8, :]
    return total


def visit(
    batch, slot, rows_ref, cols_ref, counts_ref, obj, probe, mags, tables,
    terms, pgrad, stats, win, wave, half, field,
):
    lane = lax.broadcasted_iota(jnp.int32, (CH, 128), 1)
    row0 = rows_ref[0, 0, batch, slot]
    col0 = cols_ref[0, 0, batch, slot]
    live = jnp.where(slot < counts_ref[0, 0, batch], 1.0, 0.0).astype(F32)
    block = lax.shift_right_logical(col0, 7)
    shift = col0 & 127
    back = (128 - shift) & 127
    none = jnp.zeros((8, 128), F32)

    def make_exit(i, power):
        at = pl.multiple_of(i * CH, CH)
        keep = lane < 128 - shift
        w = []
        for h in range(2):
            for p in range(2):
                rolled = [
                    pltpu.roll(obj[p, block + j, pl.ds(row0 + h * HALF + at, CH), :], back, 1)
                    for j in range(3)
                ]
                w.append([jnp.where(keep, rolled[j], rolled[j + 1]) for j in range(2)])
        for j in range(2):
            for h in range(2):
                wr, wi = w[2 * h][j], w[2 * h + 1][j]
                win[0, j, pl.ds(h * HALF + at, CH), :] = wr
                win[1, j, pl.ds(h * HALF + at, CH), :] = wi
                power = power + fold(wr * wr + wi * wi)
            for k in range(MODES):
                re, im = [], []
                for h in range(2):
                    wr, wi = w[2 * h][j], w[2 * h + 1][j]
                    pr = probe[0, k, pl.ds(j * SIDE + h * HALF + at, CH), :]
                    pi = probe[1, k, pl.ds(j * SIDE + h * HALF + at, CH), :]
                    re.append(pr * wr - pi * wi)
                    im.append(pr * wi + pi * wr)
                cols = slice(j * 128, (j + 1) * 128)
                wave[k, 0, pl.ds(at, CH), cols] = (re[0] + re[1]).astype(BF16)
                wave[k, 0, pl.ds(HALF + at, CH), cols] = (im[0] + im[1]).astype(BF16)
                wave[k, 1, pl.ds(at, CH), cols] = (re[0] - re[1]).astype(BF16)
                wave[k, 1, pl.ds(HALF + at, CH), cols] = (im[0] - im[1]).astype(BF16)
        return power

    power = lax.fori_loop(0, STEPS // 2, make_exit, none, unroll=UNROLL // 2)
    stats[0] = stats[0] + live * power

    for k in range(MODES):
        for parity in range(2):
            res = jnp.dot(tables[parity], wave[k, parity], preferred_element_type=F32)
            spot = slice(k * SIDE + parity * HALF, k * SIDE + (parity + 1) * HALF)
            for o in range(2):
                near = res[o * HALF:(o + 1) * HALF, 0:HALF]
                far = res[o * HALF:(o + 1) * HALF, HALF:SIDE]
                half[0, spot, o * HALF:(o + 1) * HALF] = (near + far).astype(BF16)
                half[1, spot, o * HALF:(o + 1) * HALF] = (near - far).astype(BF16)
    for parity in range(2):
        field[parity] = jnp.dot(half[parity], tables[4 + parity], preferred_element_type=F32)

    def correct(i, misfit):
        at = pl.multiple_of(i * CH, CH)
        parity = i // (STEPS // 2)
        to = pl.multiple_of((i % (STEPS // 2)) * CH, CH)
        for q in range(2):
            parts = [
                (field[q, pl.ds(k * SIDE + at, CH), 0:HALF], field[q, pl.ds(k * SIDE + at, CH), HALF:SIDE])
                for k in range(MODES)
            ]
            total = sum(re * re + im * im for re, im in parts)
            modulus = jnp.sqrt(total)
            amplitude = mags[batch, slot, pl.ds(at, CH), q * HALF:(q + 1) * HALF]
            factor = live * (amplitude / jnp.maximum(modulus, floor_value) - 1.0)
            gap = modulus - amplitude
            misfit = misfit + fold(gap * gap)
            cols = slice(q * HALF, (q + 1) * HALF)
            for k in range(MODES):
                wave[k, parity, pl.ds(to, CH), cols] = (parts[k][0] * factor).astype(BF16)
                wave[k, parity, pl.ds(HALF + to, CH), cols] = (parts[k][1] * factor).astype(BF16)
        return misfit

    misfit = lax.fori_loop(0, STEPS, correct, none, unroll=UNROLL)
    stats[1] = stats[1] + live * misfit

    for k in range(MODES):
        even = jnp.dot(tables[2], wave[k, 0], preferred_element_type=F32)
        odd = jnp.dot(tables[3], wave[k, 1], preferred_element_type=F32)
        for h, value in enumerate(((even + odd).astype(BF16), (even - odd).astype(BF16))):
            spot = slice(k * SIDE + h * HALF, k * SIDE + (h + 1) * HALF)
            for o in range(2):
                for q in range(2):
                    half[q, spot, o * HALF:(o + 1) * HALF] = value[
                        o * HALF:(o + 1) * HALF, q * HALF:(q + 1) * HALF
                    ]
    for parity in range(2):
        field[parity] = jnp.dot(half[parity], tables[6 + parity], preferred_element_type=F32)

    def spread(i, c):
        at = pl.multiple_of(i * CH, CH)
        term = [[None, None], [None, None]]
        for j in range(2):
            wr = win[0, j, pl.ds(at, CH), :]
            wi = win[1, j, pl.ds(at, CH), :]
            tr = ti = None
            for k in range(MODES):
                source = pl.ds(k * SIDE + at, CH)
                if j == 0:
                    ur = field[0, source, 0:HALF] + field[1, source, 0:HALF]
                    ui = field[0, source, HALF:SIDE] + field[1, source, HALF:SIDE]
                else:
                    ur = field[0, source, 0:HALF] - field[1, source, 0:HALF]
                    ui = field[0, source, HALF:SIDE] - field[1, source, HALF:SIDE]
                spot = pl.ds(j * SIDE + at, CH)
                pr = probe[0, k, spot, :]
                pi = probe[1, k, spot, :]
                ar = pr * ur + pi * ui
                ai = pr * ui - pi * ur
                tr = ar if tr is None else tr + ar
                ti = ai if ti is None else ti + ai
                pgrad[0, k, spot, :] = pgrad[0, k, spot, :] + (wr * ur + wi * ui)
                pgrad[1, k, spot, :] = pgrad[1, k, spot, :] + (wr * ui - wi * ur)
            term[0][j], term[1][j] = tr, ti
        low = lane < shift
        zero = jnp.zeros((CH, 128), F32)
        spot = pl.ds(SIDE + at, CH)
        for p in range(2):
            a = pltpu.roll(term[p][0], shift, 1)
            b = pltpu.roll(term[p][1], shift, 1)
            terms[slot, p, 1, spot, :] = jnp.where(low, zero, a)
            terms[slot, p, 2, spot, :] = jnp.where(low, a, b)
            terms[slot, p, 3, spot, :] = jnp.where(low, b, zero)
        return c

    lax.fori_loop(0, STEPS, spread, 0, unroll=UNROLL)


def body(
    rows_ref, cols_ref, counts_ref, object_in, probe_in, mags_in, tables_in, sort_in,
    object_out, probe_out, errors,
    obj, probes, grad, pgrad, terms, stats, mags, tables, sort, win, wave, half, field,
    core_in, acc, one_in, one, two_in, z_in, tile_in, tile_z, tile_core,
    inner_in, side_in, corner_in, row_in, rdma_send, rdma_recv, local, ready,
):
    row, col, core, coords, along, partner, tile = where_am_i()
    up, down = tile((row + 7) % 8, col), tile((row + 1) % 8, col)
    beside = (col + 15 + 2 * core) % 16
    outer = tile(row, beside)
    outer_up, outer_down = tile((row + 7) % 8, beside), tile((row + 1) % 8, beside)
    has_up, has_down = row > 0, row < 7
    has_outer = jnp.where(core == 0, col > 0, col < 15)
    inner_halo, outer_halo = 3 * (1 - core), 3 * core
    inner_own, outer_own = 2 - core, 1 + core
    greeted = [partner, outer, up, down, outer_up, outer_down]
    for axis in ("x", "y", "z"):
        for d in (1, 2, 3):
            greeted.append(along(axis, (coords[axis] + d) % 4))

    def greet(sem):
        for peer in greeted:
            pl.semaphore_signal(sem, inc=1, device_id=peer, device_id_type=pl.DeviceIdType.MESH)

    for p in range(2):
        for b in (0, 3):
            obj[p, b] = jnp.zeros((EXT, 128), F32)
        for b in (1, 2):
            obj[p, b, 0:HALF, :] = jnp.zeros((HALF, 128), F32)
            obj[p, b, SIDE + HALF:EXT, :] = jnp.zeros((HALF, 128), F32)
    barrier = pltpu.get_barrier_semaphore()
    greet(barrier)

    loads = []

    def load(src, dst):
        copy = pltpu.make_async_copy(src, dst, local.at[len(loads)])
        copy.start()
        loads.append(copy)

    for j in range(2):
        load(object_in.at[:, :, j * 128:(j + 1) * 128], obj.at[:, 1 + j, HALF:HALF + SIDE, :])
    for j in range(2):
        load(
            probe_in.at[:, :, :, j * 128:(j + 1) * 128],
            probes.at[0, :, :, j * SIDE:(j + 1) * SIDE, :],
        )
    load(tables_in, tables)
    load(sort_in, sort)
    load(mags_in.at[0, 0], mags)

    count = [0]

    def message(src, dst, peer):
        n = count[0]
        count[0] += 1
        return pltpu.make_async_remote_copy(
            src_ref=src, dst_ref=dst, send_sem=rdma_send.at[n], recv_sem=rdma_recv.at[n],
            device_id=peer, device_id_type=pl.DeviceIdType.MESH,
        )

    def send(src, dst, peer):
        copy = message(src, dst, peer)
        copy.start()
        return copy

    def wait(copies):
        for copy in copies:
            copy.wait()

    class Halo:
        def __init__(self, p):
            both = jnp.logical_and
            own, top, low = slice(HALF, SIDE + HALF), slice(HALF, SIDE), slice(SIDE, SIDE + HALF)
            above, below = slice(0, HALF), slice(SIDE + HALF, EXT)
            there = 3 * (1 - core)
            self.parts = [
                (message(obj.at[p, 1:3, top, :], obj.at[p, 1:3, below, :], up), has_up, has_down),
                (message(obj.at[p, 1:3, low, :], obj.at[p, 1:3, above, :], down), has_down, has_up),
                (message(obj.at[p, outer_own, own, :], obj.at[p, there, own, :], outer), has_outer, has_outer),
                (
                    message(obj.at[p, outer_own, top, :], obj.at[p, there, below, :], outer_up),
                    both(has_up, has_outer), both(has_down, has_outer),
                ),
                (
                    message(obj.at[p, outer_own, low, :], obj.at[p, there, above, :], outer_down),
                    both(has_down, has_outer), both(has_up, has_outer),
                ),
            ]
            self.inner = message(obj.at[p, inner_own], obj.at[p, 3 * core], partner)

        def start(self):
            for copy, sends, _ in self.parts:
                @pl.when(sends)
                def _():
                    copy.start()

        def wait_some(self, parts):
            for copy, sends, takes in parts:
                @pl.when(sends)
                def _():
                    copy.wait_send()

                @pl.when(takes)
                def _():
                    copy.wait_recv()

        def turn(self):
            self.wait_some(self.parts[0:2])
            self.inner.start()

        def finish(self):
            self.wait_some(self.parts[2:])
            self.inner.wait()

    pl.semaphore_wait(barrier, len(greeted))
    wait(loads[0:2])
    halo = [Halo(p) for p in range(2)]
    for p in range(2):
        halo[p].start()

    def clear(i, c):
        at = pl.multiple_of(i * 64, 64)
        nothing = jnp.zeros((64, 128), F32)
        for s in range(SLOTS):
            for p in range(2):
                for b in range(5):
                    terms[s, p, b, pl.ds(at, 64), :] = nothing
        return c

    lax.fori_loop(0, 12, clear, 0)
    pgrad[...] = jnp.zeros_like(pgrad)
    wait(loads[2:7])

    def pieces(x):
        high = x.astype(BF16)
        rest = x - high.astype(F32)
        middle = rest.astype(BF16)
        return (high, middle, (rest - middle.astype(F32)).astype(BF16))

    def arrange(n, c):
        b, s = n // SLOTS, n % SLOTS
        x = sum(jnp.dot(sort[0], v, preferred_element_type=F32) for v in pieces(mags[b, s]))
        mags[b, s] = sum(jnp.dot(v, sort[1], preferred_element_type=F32) for v in pieces(x))
        return c

    lax.fori_loop(0, BATCHES * SLOTS, arrange, 0)

    for p in range(2):
        halo[p].turn()
    for p in range(2):
        halo[p].finish()
    greet(ready)

    base = count[0]

    def update(u, carry):
        count[0] = base
        batch = u % BATCHES
        now = u % 2
        probe, fresh = probes.at[now], probes.at[1 - now]
        stats[...] = jnp.zeros_like(stats)

        def one_slot(slot, c):
            visit(
                batch, slot, rows_ref, cols_ref, counts_ref, obj, probe, mags, tables,
                terms, pgrad, stats, win, wave, half, field,
            )
            return c

        lax.fori_loop(0, SLOTS, one_slot, 0)

        spots = []
        for s in range(SLOTS):
            row0 = rows_ref[0, 0, batch, s]
            col0 = cols_ref[0, 0, batch, s]
            spots.append((1 - lax.shift_right_logical(col0, 7), SIDE - row0))

        def add_terms(p, b):
            def chunk(i, c):
                at = pl.multiple_of(i * 32, 32)
                grad[p, b, pl.ds(at, 32), :] = sum(
                    terms[s, p, spots[s][0] + b, pl.ds(spots[s][1] + at, 32), :] for s in range(SLOTS)
                )
                return c

            lax.fori_loop(0, EXT // 32, chunk, 0, unroll=4)

        pl.semaphore_wait(ready, len(greeted))

        inner_sent, outer_sent = [], []
        core_sent = [
            send(stats, tile_core, partner),
            send(pgrad.at[1 - core], core_in, partner),
        ]
        for p in range(2):
            add_terms(p, inner_halo)
            inner_sent.append(send(grad.at[p, inner_halo], inner_in.at[p], partner))
        for p in range(2):
            add_terms(p, outer_halo)
            outer_sent.append([
                send(grad.at[p, outer_halo, HALF:SIDE + HALF, :], side_in.at[p], outer),
                send(grad.at[p, outer_halo, 0:HALF, :], corner_in.at[p, HALF:SIDE, :], outer_up),
                send(grad.at[p, outer_halo, SIDE + HALF:EXT, :], corner_in.at[p, 0:HALF, :], outer_down),
            ])

        def scatter(phase, source, landing, length, tile_value):
            me = coords[ORDERS[0][phase]]
            tile_in[phase, me] = tile_value
            slot = tile_in.at[phase, me]
            sent = []
            for d in (2, 1, 3):
                sent.append(send(slot, slot, along(ORDERS[0][phase], (me + d) % 4)))
                for g in range(2):
                    axis = ORDERS[g][phase]
                    to = (coords[axis] + d) % 4
                    at = pl.multiple_of(to * length, length)
                    sent.append(
                        send(
                            source.at[2 * g:2 * g + 2, pl.ds(at, length), :],
                            landing.at[d - 1, 2 * g:2 * g + 2],
                            along(axis, to),
                        )
                    )
            return sent

        def gather_sum(phase, source, landing, length):
            out = []
            for g in range(2):
                at = pl.multiple_of(coords[ORDERS[g][phase]] * length, length)
                for k in (2 * g, 2 * g + 1):
                    out.append(
                        source[k, pl.ds(at, length), :] + landing[0, k] + landing[1, k] + landing[2, k]
                    )
            return out

        def tile_total(phase):
            return (tile_in[phase, 0] + tile_in[phase, 1]) + (tile_in[phase, 2] + tile_in[phase, 3])

        def send_rows(p):
            inner_sent[p].wait()
            grad[p, inner_own] = grad[p, inner_own] + inner_in[p]
            return [
                send(grad.at[p, 1:3, 0:HALF, :], row_in.at[p, :, HALF:SIDE, :], up),
                send(grad.at[p, 1:3, SIDE + HALF:EXT, :], row_in.at[p, :, 0:HALF, :], down),
            ]

        wait(core_sent)
        for k in range(MODES):
            acc[k] = pgrad[core, k] + core_in[k]
        sent = scatter(0, acc, one_in, 128, stats[...] + tile_core[...])

        def peak_step(i, best):
            at = pl.multiple_of(i * 16, 16)
            total = None
            for p in range(2):
                for k in range(MODES):
                    v = probe[p, k, pl.ds(at, 16), :]
                    total = v * v if total is None else total + v * v
            return jnp.maximum(best, jnp.maximum(total[0:8], total[8:16]))

        best = lax.fori_loop(0, EXT // 16, peak_step, jnp.zeros((8, 128), F32), unroll=4)
        rate = object_rate / (jnp.max(best) + tiny_value)

        def finish_object(p):
            wait(rows_sent[p] + outer_sent[p])
            for h, has in ((0, has_up), (1, has_down)):
                there = slice(h * HALF, (h + 1) * HALF)
                here = slice((h + 1) * HALF, (h + 2) * HALF)
                for b in (1, 2):
                    total = grad[p, b, here, :] + jnp.where(has, row_in[p, b - 1, there, :], 0.0)
                    side = side_in[p, there, :] + jnp.where(has, corner_in[p, there, :], 0.0)
                    total = total + jnp.where(jnp.logical_and(has_outer, outer_own == b), side, 0.0)
                    obj[p, b, here, :] = obj[p, b, here, :] + rate * total

            @pl.when(u < UPDATES - 1)
            def _():
                halo[p].start()

        for p in range(2):
            add_terms(p, 1)
            add_terms(p, 2)
        rows_sent = [send_rows(p) for p in range(2)]

        wait(sent)
        for k, v in enumerate(gather_sum(0, acc, one_in, 128)):
            one[k] = v
        sent = scatter(1, one, two_in, 32, tile_total(0))

        wait(sent)
        z = coords["z"]
        for k, v in enumerate(gather_sum(1, one, two_in, 32)):
            z_in[z, k] = v
        tile_z[z] = tile_total(1)
        sent = []
        for d in (2, 1, 3):
            peer = along("z", (z + d) % 4)
            sent.append(send(tile_z.at[z], tile_z.at[z], peer))
            sent.append(send(z_in.at[z], z_in.at[z], peer))
        pgrad[...] = jnp.zeros_like(pgrad)
        halo = [Halo(p) for p in range(2)]
        wait(sent)

        totals = (tile_z[0] + tile_z[1]) + (tile_z[2] + tile_z[3])
        errors[u] = totals[1]
        gain = probe_rate * SIDE * SIDE / jnp.sum(totals[0])
        starts = []
        for g in range(2):
            a, b = coords[ORDERS[g][0]], coords[ORDERS[g][1]]
            starts.append((a * 128, a * 128 + b * 32))
        for k in range(MODES):
            spot = pl.ds(pl.multiple_of(starts[k // 2][1], 32), 32)
            total = (z_in[0, k] + z_in[1, k]) + (z_in[2, k] + z_in[3, k])
            fresh[core, k, spot, :] = probe[core, k, spot, :] + gain * total

        def block_of(g, at, length):
            at = pl.multiple_of(at, length)
            return fresh.at[core, 2 * g:2 * g + 2, pl.ds(at, length), :]

        def spread(phase, length):
            out = {}
            for d in (2, 1, 3):
                for g in range(2):
                    axis = ORDERS[g][phase]
                    block = block_of(g, starts[g][phase], length)
                    out[d, g] = send(block, block, along(axis, (coords[axis] + d) % 4))
            return out

        out2 = spread(1, 32)
        finish_object(0)
        wait(out2.values())
        out1 = spread(0, 128)
        finish_object(1)
        to_core = []
        for g in range(2):
            block = block_of(g, starts[g][0], 128)
            to_core.append(send(block, block, partner))

        @pl.when(u < UPDATES - 1)
        def _():
            for p in range(2):
                halo[p].turn()

        for d in (1, 3, 2):
            for g in range(2):
                out1[d, g].wait()
                axis = ORDERS[g][0]
                block = block_of(g, (coords[axis] + 4 - d) % 4 * 128, 128)
                to_core.append(send(block, block, partner))

        wait(to_core)

        @pl.when(u < UPDATES - 1)
        def _():
            for p in range(2):
                halo[p].finish()
            greet(ready)

        return carry

    lax.fori_loop(0, UPDATES, update, 0)

    stores = []
    for j in range(2):
        stores.append(
            pltpu.make_async_copy(
                obj.at[:, 1 + j, HALF:HALF + SIDE, :], object_out.at[:, :, j * 128:(j + 1) * 128], local.at[j]
            )
        )
        stores.append(
            pltpu.make_async_copy(
                probes.at[UPDATES % 2, :, :, j * SIDE:(j + 1) * SIDE, :],
                probe_out.at[:, :, :, j * 128:(j + 1) * 128],
                local.at[2 + j],
            )
        )
    for copy in stores:
        copy.start()
    wait(stores)


def on_device(object_field, probe, pos_rows, pos_cols, counts, magnitudes):
    tables = tuple(jnp.asarray(t) for t in transform_tables())
    anywhere = pl.BlockSpec(memory_space=pl.ANY)
    whole = pl.BlockSpec(memory_space=pltpu.VMEM)
    smem = pl.BlockSpec(memory_space=pltpu.SMEM)
    messages = 96
    out, probe_out, errors = pl.pallas_call(
        body,
        out_shape=(
            jax.ShapeDtypeStruct((2, SIDE, SIDE), F32),
            jax.ShapeDtypeStruct((2, MODES, SIDE, SIDE), F32),
            jax.ShapeDtypeStruct((UPDATES, 8, 128), F32),
        ),
        in_specs=[smem, smem, smem] + [anywhere] * 5,
        out_specs=(anywhere, anywhere, whole),
        scratch_shapes=[
            pltpu.VMEM((2, 4, EXT, 128), F32),
            pltpu.VMEM((2, 2, MODES, EXT, 128), F32),
            pltpu.VMEM((2, 4, EXT, 128), F32),
            pltpu.VMEM((2, MODES, EXT, 128), F32),
            pltpu.VMEM((SLOTS, 2, 5, 3 * SIDE, 128), F32),
            pltpu.VMEM((2, 8, 128), F32),
            pltpu.VMEM((BATCHES, SLOTS, SIDE, SIDE), F32),
            pltpu.VMEM((8, SIDE, SIDE), BF16),
            pltpu.VMEM((2, SIDE, SIDE), BF16),
            pltpu.VMEM((2, 2, SIDE, 128), F32),
            pltpu.VMEM((MODES, 2, SIDE, SIDE), BF16),
            pltpu.VMEM((2, MODES * SIDE, SIDE), BF16),
            pltpu.VMEM((2, MODES * SIDE, SIDE), F32),
            pltpu.VMEM((MODES, EXT, 128), F32),
            pltpu.VMEM((MODES, EXT, 128), F32),
            pltpu.VMEM((3, MODES, 128, 128), F32),
            pltpu.VMEM((MODES, 128, 128), F32),
            pltpu.VMEM((3, MODES, 32, 128), F32),
            pltpu.VMEM((4, MODES, 32, 128), F32),
            pltpu.VMEM((2, 4, 2, 8, 128), F32),
            pltpu.VMEM((4, 2, 8, 128), F32),
            pltpu.VMEM((2, 8, 128), F32),
            pltpu.VMEM((2, EXT, 128), F32),
            pltpu.VMEM((2, SIDE, 128), F32),
            pltpu.VMEM((2, SIDE, 128), F32),
            pltpu.VMEM((2, 2, SIDE, 128), F32),
            pltpu.SemaphoreType.DMA((messages,)),
            pltpu.SemaphoreType.DMA((messages,)),
            pltpu.SemaphoreType.DMA((8,)),
            pltpu.SemaphoreType.REGULAR,
        ],
        cost_estimate=pl.CostEstimate(flops=80 << 30, bytes_accessed=12 << 20, transcendentals=0),
        compiler_params=pltpu.CompilerParams(
            collective_id=0, has_side_effects=True, vmem_limit_bytes=60 << 20
        ),
        name="whole_sweep",
    )(
        pos_rows, pos_cols, counts,
        object_field, probe, magnitudes, *tables,
    )
    return (out, probe_out, jnp.sum(errors, axis=(1, 2)))


def solution(mesh):
    finer = Mesh(mesh.devices.reshape(4, 2, 4, 2, 2), AXES)
    return jax.shard_map(
        on_device,
        mesh=finer,
        in_specs=(
            P(None, ROW, COL),
            P(),
            P(ROW, COL, None, None),
            P(ROW, COL, None, None),
            P(ROW, COL, None),
            P(ROW, COL, None, None, None, None),
        ),
        out_specs=(P(None, ROW, COL), P(), P()),
        check_vma=False,
    )
```

```python
import functools
import math

import jax
import jax.numpy as jnp
import numpy as np
from jax import lax
from jax.experimental import pallas as pl
from jax.experimental.pallas import tpu as pltpu
from jax.sharding import Mesh
from jax.sharding import PartitionSpec as P

BATCHES = 2
ITERS = 2
SLOTS = 3
MODES = 4
SIDE = 256
HALF = 128
EXT = 512
UPDATES = BATCHES * ITERS
AXES = ("row_0", "row_1", "col_0", "col_1", "col_2")
ROW = ("row_0", "row_1")
COL = ("col_0", "col_1", "col_2")
F32 = jnp.float32
BF16 = jnp.bfloat16

object_rate = 0.9
probe_rate = 0.5
floor_value = 0.5
tiny_value = 1e-06


def transform_tables():
    index = np.arange(SIDE)
    angles = (index[:, None] * index[None, :] % SIDE) * (2.0 * math.pi / SIDE)
    scale = 1.0 / math.sqrt(SIDE)
    c = np.cos(angles) * scale
    s = -np.sin(angles) * scale
    near = np.arange(HALF)
    tables = []
    for parity in range(2):
        pick = np.arange(parity, SIDE, 2)
        cr, sr = c[np.ix_(pick, near)], s[np.ix_(pick, near)]
        tables.append(np.block([[cr, -sr], [sr, cr]]))
    for parity in range(2):
        pick = np.arange(parity, SIDE, 2)
        cr, sr = c[np.ix_(near, pick)], s[np.ix_(near, pick)]
        tables.append(np.block([[cr, sr], [-sr, cr]]))
    tables = tables + [t.T for t in tables]
    order = np.concatenate([np.arange(0, SIDE, 2), np.arange(1, SIDE, 2)])
    sort = np.eye(SIDE)[order]
    return (np.stack(tables).astype(jnp.bfloat16), np.stack([sort, sort.T]).astype(jnp.bfloat16))


def where_am_i():
    y, lo, x, hi, core = (lax.axis_index(name) for name in AXES)
    row, col = y * 2 + lo, x * 4 + hi * 2 + core
    z = hi * 2 + lo

    def tile(r, c):
        return (r // 2, r % 2, c // 4, (c // 2) % 2, c % 2)

    def along(axis, value):
        if axis == "x":
            return (y, lo, value, hi, core)
        if axis == "y":
            return (value, lo, x, hi, core)
        return (y, value % 2, x, value // 2, core)

    partner = (y, lo, x, hi, 1 - core)
    coords = {"x": x, "y": y, "z": z}
    return row, col, core, coords, along, partner, tile


ORDERS = (("x", "y", "z"), ("y", "x", "z"))
CH = 16
STEPS = SIDE // CH
UNROLL = 8


def fold(x):
    total = x[0:8, :]
    for i in range(1, x.shape[0] // 8):
        total = total + x[8 * i:8 * i + 8, :]
    return total


def visit(
    batch, slot, rows_ref, cols_ref, counts_ref, obj, probe, mags, tables,
    terms, pgrad, stats, win, wave, half, field,
):
    lane = lax.broadcasted_iota(jnp.int32, (CH, 128), 1)
    row0 = rows_ref[0, 0, batch, slot]
    col0 = cols_ref[0, 0, batch, slot]
    live = jnp.where(slot < counts_ref[0, 0, batch], 1.0, 0.0).astype(F32)
    block = lax.shift_right_logical(col0, 7)
    shift = col0 & 127
    back = (128 - shift) & 127
    none = jnp.zeros((8, 128), F32)

    def make_exit(i, power):
        at = pl.multiple_of(i * CH, CH)
        keep = lane < 128 - shift
        w = []
        for h in range(2):
            for p in range(2):
                rolled = [
                    pltpu.roll(obj[p, block + j, pl.ds(row0 + h * HALF + at, CH), :], back, 1)
                    for j in range(3)
                ]
                w.append([jnp.where(keep, rolled[j], rolled[j + 1]) for j in range(2)])
        for j in range(2):
            for h in range(2):
                wr, wi = w[2 * h][j], w[2 * h + 1][j]
                win[0, j, pl.ds(h * HALF + at, CH), :] = wr
                win[1, j, pl.ds(h * HALF + at, CH), :] = wi
                power = power + fold(wr * wr + wi * wi)
            for k in range(MODES):
                re, im = [], []
                for h in range(2):
                    wr, wi = w[2 * h][j], w[2 * h + 1][j]
                    pr = probe[0, k, pl.ds(j * SIDE + h * HALF + at, CH), :]
                    pi = probe[1, k, pl.ds(j * SIDE + h * HALF + at, CH), :]
                    re.append(pr * wr - pi * wi)
                    im.append(pr * wi + pi * wr)
                cols = slice(j * 128, (j + 1) * 128)
                wave[k, 0, pl.ds(at, CH), cols] = (re[0] + re[1]).astype(BF16)
                wave[k, 0, pl.ds(HALF + at, CH), cols] = (im[0] + im[1]).astype(BF16)
                wave[k, 1, pl.ds(at, CH), cols] = (re[0] - re[1]).astype(BF16)
                wave[k, 1, pl.ds(HALF + at, CH), cols] = (im[0] - im[1]).astype(BF16)
        return power

    power = lax.fori_loop(0, STEPS // 2, make_exit, none, unroll=UNROLL // 2)
    stats[0] = stats[0] + live * power

    for k in range(MODES):
        for parity in range(2):
            res = jnp.dot(tables[parity], wave[k, parity], preferred_element_type=F32)
            spot = slice(k * SIDE + parity * HALF, k * SIDE + (parity + 1) * HALF)
            for o in range(2):
                near = res[o * HALF:(o + 1) * HALF, 0:HALF]
                far = res[o * HALF:(o + 1) * HALF, HALF:SIDE]
                half[0, spot, o * HALF:(o + 1) * HALF] = (near + far).astype(BF16)
                half[1, spot, o * HALF:(o + 1) * HALF] = (near - far).astype(BF16)
    for parity in range(2):
        field[parity] = jnp.dot(half[parity], tables[4 + parity], preferred_element_type=F32)

    def correct(i, misfit):
        at = pl.multiple_of(i * CH, CH)
        parity = i // (STEPS // 2)
        to = pl.multiple_of((i % (STEPS // 2)) * CH, CH)
        for q in range(2):
            parts = [
                (field[q, pl.ds(k * SIDE + at, CH), 0:HALF], field[q, pl.ds(k * SIDE + at, CH), HALF:SIDE])
                for k in range(MODES)
            ]
            total = sum(re * re + im * im for re, im in parts)
            modulus = jnp.sqrt(total)
            amplitude = mags[batch, slot, pl.ds(at, CH), q * HALF:(q + 1) * HALF]
            factor = live * (amplitude / jnp.maximum(modulus, floor_value) - 1.0)
            gap = modulus - amplitude
            misfit = misfit + fold(gap * gap)
            cols = slice(q * HALF, (q + 1) * HALF)
            for k in range(MODES):
                wave[k, parity, pl.ds(to, CH), cols] = (parts[k][0] * factor).astype(BF16)
                wave[k, parity, pl.ds(HALF + to, CH), cols] = (parts[k][1] * factor).astype(BF16)
        return misfit

    misfit = lax.fori_loop(0, STEPS, correct, none, unroll=UNROLL)
    stats[1] = stats[1] + live * misfit

    for k in range(MODES):
        even = jnp.dot(tables[2], wave[k, 0], preferred_element_type=F32)
        odd = jnp.dot(tables[3], wave[k, 1], preferred_element_type=F32)
        for h, value in enumerate(((even + odd).astype(BF16), (even - odd).astype(BF16))):
            spot = slice(k * SIDE + h * HALF, k * SIDE + (h + 1) * HALF)
            for o in range(2):
                for q in range(2):
                    half[q, spot, o * HALF:(o + 1) * HALF] = value[
                        o * HALF:(o + 1) * HALF, q * HALF:(q + 1) * HALF
                    ]
    for parity in range(2):
        field[parity] = jnp.dot(half[parity], tables[6 + parity], preferred_element_type=F32)

    def spread(i, c):
        at = pl.multiple_of(i * CH, CH)
        term = [[None, None], [None, None]]
        for j in range(2):
            wr = win[0, j, pl.ds(at, CH), :]
            wi = win[1, j, pl.ds(at, CH), :]
            tr = ti = None
            for k in range(MODES):
                source = pl.ds(k * SIDE + at, CH)
                if j == 0:
                    ur = field[0, source, 0:HALF] + field[1, source, 0:HALF]
                    ui = field[0, source, HALF:SIDE] + field[1, source, HALF:SIDE]
                else:
                    ur = field[0, source, 0:HALF] - field[1, source, 0:HALF]
                    ui = field[0, source, HALF:SIDE] - field[1, source, HALF:SIDE]
                spot = pl.ds(j * SIDE + at, CH)
                pr = probe[0, k, spot, :]
                pi = probe[1, k, spot, :]
                ar = pr * ur + pi * ui
                ai = pr * ui - pi * ur
                tr = ar if tr is None else tr + ar
                ti = ai if ti is None else ti + ai
                pgrad[0, k, spot, :] = pgrad[0, k, spot, :] + (wr * ur + wi * ui)
                pgrad[1, k, spot, :] = pgrad[1, k, spot, :] + (wr * ui - wi * ur)
            term[0][j], term[1][j] = tr, ti
        low = lane < shift
        zero = jnp.zeros((CH, 128), F32)
        spot = pl.ds(SIDE + at, CH)
        for p in range(2):
            a = pltpu.roll(term[p][0], shift, 1)
            b = pltpu.roll(term[p][1], shift, 1)
            terms[slot, p, 1, spot, :] = jnp.where(low, zero, a)
            terms[slot, p, 2, spot, :] = jnp.where(low, a, b)
            terms[slot, p, 3, spot, :] = jnp.where(low, b, zero)
        return c

    lax.fori_loop(0, STEPS, spread, 0, unroll=UNROLL)


def body(
    rows_ref, cols_ref, counts_ref, object_in, probe_in, mags_in, tables_in, sort_in,
    object_out, probe_out, errors,
    obj, probes, grad, pgrad, terms, stats, mags, tables, sort, win, wave, half, field,
    core_in, acc, one_in, one, two_in, z_in, tile_in, tile_z, tile_core,
    inner_in, side_in, corner_in, row_in, rdma_send, rdma_recv, local, ready,
):
    row, col, core, coords, along, partner, tile = where_am_i()
    up, down = tile((row + 7) % 8, col), tile((row + 1) % 8, col)
    beside = (col + 15 + 2 * core) % 16
    outer = tile(row, beside)
    outer_up, outer_down = tile((row + 7) % 8, beside), tile((row + 1) % 8, beside)
    has_up, has_down = row > 0, row < 7
    has_outer = jnp.where(core == 0, col > 0, col < 15)
    inner_halo, outer_halo = 3 * (1 - core), 3 * core
    inner_own, outer_own = 2 - core, 1 + core
    greeted = [partner, outer, up, down, outer_up, outer_down]
    for axis in ("x", "y", "z"):
        for d in (1, 2, 3):
            greeted.append(along(axis, (coords[axis] + d) % 4))

    def greet(sem):
        for peer in greeted:
            pl.semaphore_signal(sem, inc=1, device_id=peer, device_id_type=pl.DeviceIdType.MESH)

    for p in range(2):
        for b in (0, 3):
            obj[p, b] = jnp.zeros((EXT, 128), F32)
        for b in (1, 2):
            obj[p, b, 0:HALF, :] = jnp.zeros((HALF, 128), F32)
            obj[p, b, SIDE + HALF:EXT, :] = jnp.zeros((HALF, 128), F32)
    barrier = pltpu.get_barrier_semaphore()
    greet(barrier)

    loads = []

    def load(src, dst):
        copy = pltpu.make_async_copy(src, dst, local.at[len(loads)])
        copy.start()
        loads.append(copy)

    for j in range(2):
        load(object_in.at[:, :, j * 128:(j + 1) * 128], obj.at[:, 1 + j, HALF:HALF + SIDE, :])
    for j in range(2):
        load(
            probe_in.at[:, :, :, j * 128:(j + 1) * 128],
            probes.at[0, :, :, j * SIDE:(j + 1) * SIDE, :],
        )
    load(tables_in, tables)
    load(sort_in, sort)
    load(mags_in.at[0, 0], mags)

    count = [0]

    def message(src, dst, peer):
        n = count[0]
        count[0] += 1
        return pltpu.make_async_remote_copy(
            src_ref=src, dst_ref=dst, send_sem=rdma_send.at[n], recv_sem=rdma_recv.at[n],
            device_id=peer, device_id_type=pl.DeviceIdType.MESH,
        )

    def send(src, dst, peer):
        copy = message(src, dst, peer)
        copy.start()
        return copy

    def wait(copies):
        for copy in copies:
            copy.wait()

    class Halo:
        def __init__(self, p):
            both = jnp.logical_and
            own, top, low = slice(HALF, SIDE + HALF), slice(HALF, SIDE), slice(SIDE, SIDE + HALF)
            above, below = slice(0, HALF), slice(SIDE + HALF, EXT)
            there = 3 * (1 - core)
            self.parts = [
                (message(obj.at[p, 1:3, top, :], obj.at[p, 1:3, below, :], up), has_up, has_down),
                (message(obj.at[p, 1:3, low, :], obj.at[p, 1:3, above, :], down), has_down, has_up),
                (message(obj.at[p, outer_own, own, :], obj.at[p, there, own, :], outer), has_outer, has_outer),
                (
                    message(obj.at[p, outer_own, top, :], obj.at[p, there, below, :], outer_up),
                    both(has_up, has_outer), both(has_down, has_outer),
                ),
                (
                    message(obj.at[p, outer_own, low, :], obj.at[p, there, above, :], outer_down),
                    both(has_down, has_outer), both(has_up, has_outer),
                ),
            ]
            self.inner = message(obj.at[p, inner_own], obj.at[p, 3 * core], partner)

        def start(self):
            for copy, sends, _ in self.parts:
                @pl.when(sends)
                def _():
                    copy.start()

        def wait_some(self, parts):
            for copy, sends, takes in parts:
                @pl.when(sends)
                def _():
                    copy.wait_send()

                @pl.when(takes)
                def _():
                    copy.wait_recv()

        def turn(self):
            self.wait_some(self.parts[0:2])
            self.inner.start()

        def finish(self):
            self.wait_some(self.parts[2:])
            self.inner.wait()

    pl.semaphore_wait(barrier, len(greeted))
    wait(loads[0:2])
    halo = [Halo(p) for p in range(2)]
    for p in range(2):
        halo[p].start()

    def clear(i, c):
        at = pl.multiple_of(i * 64, 64)
        nothing = jnp.zeros((64, 128), F32)
        for s in range(SLOTS):
            for p in range(2):
                for b in range(5):
                    terms[s, p, b, pl.ds(at, 64), :] = nothing
        return c

    lax.fori_loop(0, 12, clear, 0)
    pgrad[...] = jnp.zeros_like(pgrad)
    wait(loads[2:7])

    def pieces(x):
        high = x.astype(BF16)
        rest = x - high.astype(F32)
        middle = rest.astype(BF16)
        return (high, middle, (rest - middle.astype(F32)).astype(BF16))

    def arrange(n, c):
        b, s = n // SLOTS, n % SLOTS
        x = sum(jnp.dot(sort[0], v, preferred_element_type=F32) for v in pieces(mags[b, s]))
        mags[b, s] = sum(jnp.dot(v, sort[1], preferred_element_type=F32) for v in pieces(x))
        return c

    lax.fori_loop(0, BATCHES * SLOTS, arrange, 0)

    for p in range(2):
        halo[p].turn()
    for p in range(2):
        halo[p].finish()
    greet(ready)

    base = count[0]

    def update(u, carry):
        count[0] = base
        batch = u % BATCHES
        now = u % 2
        probe, fresh = probes.at[now], probes.at[1 - now]
        stats[...] = jnp.zeros_like(stats)

        def one_slot(slot, c):
            visit(
                batch, slot, rows_ref, cols_ref, counts_ref, obj, probe, mags, tables,
                terms, pgrad, stats, win, wave, half, field,
            )
            return c

        lax.fori_loop(0, SLOTS, one_slot, 0)

        spots = []
        for s in range(SLOTS):
            row0 = rows_ref[0, 0, batch, s]
            col0 = cols_ref[0, 0, batch, s]
            spots.append((1 - lax.shift_right_logical(col0, 7), SIDE - row0))

        def add_terms(p, b):
            def chunk(i, c):
                at = pl.multiple_of(i * 32, 32)
                grad[p, b, pl.ds(at, 32), :] = sum(
                    terms[s, p, spots[s][0] + b, pl.ds(spots[s][1] + at, 32), :] for s in range(SLOTS)
                )
                return c

            lax.fori_loop(0, EXT // 32, chunk, 0, unroll=4)

        pl.semaphore_wait(ready, len(greeted))

        inner_sent, outer_sent = [], []
        core_sent = [
            send(stats, tile_core, partner),
            send(pgrad.at[1 - core, 0:2], core_in.at[0:2], partner),
            send(pgrad.at[1 - core, 2:4], core_in.at[2:4], partner),
        ]
        for p in range(2):
            add_terms(p, inner_halo)
            inner_sent.append(send(grad.at[p, inner_halo], inner_in.at[p], partner))
        for p in range(2):
            add_terms(p, outer_halo)
            outer_sent.append([
                send(grad.at[p, outer_halo, HALF:SIDE + HALF, :], side_in.at[p], outer),
                send(grad.at[p, outer_halo, 0:HALF, :], corner_in.at[p, HALF:SIDE, :], outer_up),
                send(grad.at[p, outer_halo, SIDE + HALF:EXT, :], corner_in.at[p, 0:HALF, :], outer_down),
            ])

        def scatter(phase, source, landing, length, tile_value, groups=(0, 1)):
            me = coords[ORDERS[0][phase]]
            slot = tile_in.at[phase, me]
            if tile_value is not None:
                tile_in[phase, me] = tile_value
            sent = []
            for d in (2, 1, 3):
                if tile_value is not None:
                    sent.append(send(slot, slot, along(ORDERS[0][phase], (me + d) % 4)))
                for g in groups:
                    axis = ORDERS[g][phase]
                    to = (coords[axis] + d) % 4
                    at = pl.multiple_of(to * length, length)
                    sent.append(
                        send(
                            source.at[2 * g:2 * g + 2, pl.ds(at, length), :],
                            landing.at[d - 1, 2 * g:2 * g + 2],
                            along(axis, to),
                        )
                    )
            return sent

        def gather_sum(phase, source, landing, length):
            out = []
            for g in range(2):
                at = pl.multiple_of(coords[ORDERS[g][phase]] * length, length)
                for k in (2 * g, 2 * g + 1):
                    out.append(
                        source[k, pl.ds(at, length), :] + landing[0, k] + landing[1, k] + landing[2, k]
                    )
            return out

        def tile_total(phase):
            return (tile_in[phase, 0] + tile_in[phase, 1]) + (tile_in[phase, 2] + tile_in[phase, 3])

        def send_rows(p):
            inner_sent[p].wait()
            grad[p, inner_own] = grad[p, inner_own] + inner_in[p]
            return [
                send(grad.at[p, 1:3, 0:HALF, :], row_in.at[p, :, HALF:SIDE, :], up),
                send(grad.at[p, 1:3, SIDE + HALF:EXT, :], row_in.at[p, :, 0:HALF, :], down),
            ]

        wait(core_sent[0:2])
        for k in (0, 1):
            acc[k] = pgrad[core, k] + core_in[k]
        sent = scatter(0, acc, one_in, 128, stats[...] + tile_core[...], (0,))
        wait(core_sent[2:3])
        for k in (2, 3):
            acc[k] = pgrad[core, k] + core_in[k]
        sent += scatter(0, acc, one_in, 128, None, (1,))

        def peak_step(i, best):
            at = pl.multiple_of(i * 16, 16)
            total = None
            for p in range(2):
                for k in range(MODES):
                    v = probe[p, k, pl.ds(at, 16), :]
                    total = v * v if total is None else total + v * v
            return jnp.maximum(best, jnp.maximum(total[0:8], total[8:16]))

        best = lax.fori_loop(0, EXT // 16, peak_step, jnp.zeros((8, 128), F32), unroll=4)
        rate = object_rate / (jnp.max(best) + tiny_value)

        def finish_object(p):
            wait(rows_sent[p] + outer_sent[p])
            for h, has in ((0, has_up), (1, has_down)):
                there = slice(h * HALF, (h + 1) * HALF)
                here = slice((h + 1) * HALF, (h + 2) * HALF)
                for b in (1, 2):
                    total = grad[p, b, here, :] + jnp.where(has, row_in[p, b - 1, there, :], 0.0)
                    side = side_in[p, there, :] + jnp.where(has, corner_in[p, there, :], 0.0)
                    total = total + jnp.where(jnp.logical_and(has_outer, outer_own == b), side, 0.0)
                    obj[p, b, here, :] = obj[p, b, here, :] + rate * total

            @pl.when(u < UPDATES - 1)
            def _():
                halo[p].start()

        for p in range(2):
            add_terms(p, 1)
            add_terms(p, 2)
        rows_sent = [send_rows(p) for p in range(2)]

        wait(sent)
        for k, v in enumerate(gather_sum(0, acc, one_in, 128)):
            one[k] = v
        sent = scatter(1, one, two_in, 32, tile_total(0))

        wait(sent)
        z = coords["z"]
        for k, v in enumerate(gather_sum(1, one, two_in, 32)):
            z_in[z, k] = v
        tile_z[z] = tile_total(1)
        sent = []
        for d in (2, 1, 3):
            peer = along("z", (z + d) % 4)
            sent.append(send(tile_z.at[z], tile_z.at[z], peer))
            sent.append(send(z_in.at[z], z_in.at[z], peer))
        pgrad[...] = jnp.zeros_like(pgrad)
        halo = [Halo(p) for p in range(2)]
        wait(sent)

        totals = (tile_z[0] + tile_z[1]) + (tile_z[2] + tile_z[3])
        errors[u] = totals[1]
        gain = probe_rate * SIDE * SIDE / jnp.sum(totals[0])
        starts = []
        for g in range(2):
            a, b = coords[ORDERS[g][0]], coords[ORDERS[g][1]]
            starts.append((a * 128, a * 128 + b * 32))
        for k in range(MODES):
            spot = pl.ds(pl.multiple_of(starts[k // 2][1], 32), 32)
            total = (z_in[0, k] + z_in[1, k]) + (z_in[2, k] + z_in[3, k])
            fresh[core, k, spot, :] = probe[core, k, spot, :] + gain * total

        def block_of(g, at, length):
            at = pl.multiple_of(at, length)
            return fresh.at[core, 2 * g:2 * g + 2, pl.ds(at, length), :]

        def spread(phase, length):
            out = {}
            for d in (2, 1, 3):
                for g in range(2):
                    axis = ORDERS[g][phase]
                    block = block_of(g, starts[g][phase], length)
                    out[d, g] = send(block, block, along(axis, (coords[axis] + d) % 4))
            return out

        out2 = spread(1, 32)
        finish_object(0)
        wait(out2.values())
        out1 = spread(0, 128)
        finish_object(1)
        to_core = []
        for g in range(2):
            block = block_of(g, starts[g][0], 128)
            to_core.append(send(block, block, partner))

        @pl.when(u < UPDATES - 1)
        def _():
            for p in range(2):
                halo[p].turn()

        for d in (1, 3, 2):
            for g in range(2):
                out1[d, g].wait()
                axis = ORDERS[g][0]
                block = block_of(g, (coords[axis] + 4 - d) % 4 * 128, 128)
                to_core.append(send(block, block, partner))

        wait(to_core)

        @pl.when(u < UPDATES - 1)
        def _():
            for p in range(2):
                halo[p].finish()
            greet(ready)

        return carry

    lax.fori_loop(0, UPDATES, update, 0)

    stores = []
    for j in range(2):
        stores.append(
            pltpu.make_async_copy(
                obj.at[:, 1 + j, HALF:HALF + SIDE, :], object_out.at[:, :, j * 128:(j + 1) * 128], local.at[j]
            )
        )
        stores.append(
            pltpu.make_async_copy(
                probes.at[UPDATES % 2, :, :, j * SIDE:(j + 1) * SIDE, :],
                probe_out.at[:, :, :, j * 128:(j + 1) * 128],
                local.at[2 + j],
            )
        )
    for copy in stores:
        copy.start()
    wait(stores)


def on_device(object_field, probe, pos_rows, pos_cols, counts, magnitudes):
    tables = tuple(jnp.asarray(t) for t in transform_tables())
    anywhere = pl.BlockSpec(memory_space=pl.ANY)
    whole = pl.BlockSpec(memory_space=pltpu.VMEM)
    smem = pl.BlockSpec(memory_space=pltpu.SMEM)
    messages = 96
    out, probe_out, errors = pl.pallas_call(
        body,
        out_shape=(
            jax.ShapeDtypeStruct((2, SIDE, SIDE), F32),
            jax.ShapeDtypeStruct((2, MODES, SIDE, SIDE), F32),
            jax.ShapeDtypeStruct((UPDATES, 8, 128), F32),
        ),
        in_specs=[smem, smem, smem] + [anywhere] * 5,
        out_specs=(anywhere, anywhere, whole),
        scratch_shapes=[
            pltpu.VMEM((2, 4, EXT, 128), F32),
            pltpu.VMEM((2, 2, MODES, EXT, 128), F32),
            pltpu.VMEM((2, 4, EXT, 128), F32),
            pltpu.VMEM((2, MODES, EXT, 128), F32),
            pltpu.VMEM((SLOTS, 2, 5, 3 * SIDE, 128), F32),
            pltpu.VMEM((2, 8, 128), F32),
            pltpu.VMEM((BATCHES, SLOTS, SIDE, SIDE), F32),
            pltpu.VMEM((8, SIDE, SIDE), BF16),
            pltpu.VMEM((2, SIDE, SIDE), BF16),
            pltpu.VMEM((2, 2, SIDE, 128), F32),
            pltpu.VMEM((MODES, 2, SIDE, SIDE), BF16),
            pltpu.VMEM((2, MODES * SIDE, SIDE), BF16),
            pltpu.VMEM((2, MODES * SIDE, SIDE), F32),
            pltpu.VMEM((MODES, EXT, 128), F32),
            pltpu.VMEM((MODES, EXT, 128), F32),
            pltpu.VMEM((3, MODES, 128, 128), F32),
            pltpu.VMEM((MODES, 128, 128), F32),
            pltpu.VMEM((3, MODES, 32, 128), F32),
            pltpu.VMEM((4, MODES, 32, 128), F32),
            pltpu.VMEM((2, 4, 2, 8, 128), F32),
            pltpu.VMEM((4, 2, 8, 128), F32),
            pltpu.VMEM((2, 8, 128), F32),
            pltpu.VMEM((2, EXT, 128), F32),
            pltpu.VMEM((2, SIDE, 128), F32),
            pltpu.VMEM((2, SIDE, 128), F32),
            pltpu.VMEM((2, 2, SIDE, 128), F32),
            pltpu.SemaphoreType.DMA((messages,)),
            pltpu.SemaphoreType.DMA((messages,)),
            pltpu.SemaphoreType.DMA((8,)),
            pltpu.SemaphoreType.REGULAR,
        ],
        cost_estimate=pl.CostEstimate(flops=80 << 30, bytes_accessed=12 << 20, transcendentals=0),
        compiler_params=pltpu.CompilerParams(
            collective_id=0, has_side_effects=True, vmem_limit_bytes=60 << 20
        ),
        name="whole_sweep",
    )(
        pos_rows, pos_cols, counts,
        object_field, probe, magnitudes, *tables,
    )
    return (out, probe_out, jnp.sum(errors, axis=(1, 2)))


def solution(mesh):
    finer = Mesh(mesh.devices.reshape(4, 2, 4, 2, 2), AXES)
    return jax.shard_map(
        on_device,
        mesh=finer,
        in_specs=(
            P(None, ROW, COL),
            P(),
            P(ROW, COL, None, None),
            P(ROW, COL, None, None),
            P(ROW, COL, None),
            P(ROW, COL, None, None, None, None),
        ),
        out_specs=(P(None, ROW, COL), P(), P()),
        check_vma=False,
    )
```

```python
import functools
import math

import jax
import jax.numpy as jnp
import numpy as np
from jax import lax
from jax.experimental import pallas as pl
from jax.experimental.pallas import tpu as pltpu
from jax.sharding import Mesh
from jax.sharding import PartitionSpec as P

BATCHES = 2
ITERS = 2
SLOTS = 3
MODES = 4
SIDE = 256
HALF = 128
EXT = 512
UPDATES = BATCHES * ITERS
AXES = ("row_0", "row_1", "col_0", "col_1", "col_2")
ROW = ("row_0", "row_1")
COL = ("col_0", "col_1", "col_2")
F32 = jnp.float32
BF16 = jnp.bfloat16

object_rate = 0.9
probe_rate = 0.5
floor_value = 0.5
tiny_value = 1e-06


def transform_tables():
    index = np.arange(SIDE)
    angles = (index[:, None] * index[None, :] % SIDE) * (2.0 * math.pi / SIDE)
    scale = 1.0 / math.sqrt(SIDE)
    c = np.cos(angles) * scale
    s = -np.sin(angles) * scale
    near = np.arange(HALF)
    tables = []
    for parity in range(2):
        pick = np.arange(parity, SIDE, 2)
        cr, sr = c[np.ix_(pick, near)], s[np.ix_(pick, near)]
        tables.append(np.block([[cr, -sr], [sr, cr]]))
    for parity in range(2):
        pick = np.arange(parity, SIDE, 2)
        cr, sr = c[np.ix_(near, pick)], s[np.ix_(near, pick)]
        tables.append(np.block([[cr, sr], [-sr, cr]]))
    tables = tables + [t.T for t in tables]
    order = np.concatenate([np.arange(0, SIDE, 2), np.arange(1, SIDE, 2)])
    sort = np.eye(SIDE)[order]
    return (np.stack(tables).astype(jnp.bfloat16), np.stack([sort, sort.T]).astype(jnp.bfloat16))


def where_am_i():
    y, lo, x, hi, core = (lax.axis_index(name) for name in AXES)
    row, col = y * 2 + lo, x * 4 + hi * 2 + core
    z = hi * 2 + lo

    def tile(r, c):
        return (r // 2, r % 2, c // 4, (c // 2) % 2, c % 2)

    def along(axis, value):
        if axis == "x":
            return (y, lo, value, hi, core)
        if axis == "y":
            return (value, lo, x, hi, core)
        return (y, value % 2, x, value // 2, core)

    partner = (y, lo, x, hi, 1 - core)
    coords = {"x": x, "y": y, "z": z}
    return row, col, core, coords, along, partner, tile


ORDERS = (("x", "y", "z"), ("y", "x", "z"))
CH = 16
STEPS = SIDE // CH
UNROLL = 16


def fold(x):
    total = x[0:8, :]
    for i in range(1, x.shape[0] // 8):
        total = total + x[8 * i:8 * i + 8, :]
    return total


def visit(
    batch, slot, rows_ref, cols_ref, counts_ref, obj, probe, mags, tables,
    terms, pgrad, stats, win, wave, half, field,
):
    lane = lax.broadcasted_iota(jnp.int32, (CH, 128), 1)
    row0 = rows_ref[0, 0, batch, slot]
    col0 = cols_ref[0, 0, batch, slot]
    live = jnp.where(slot < counts_ref[0, 0, batch], 1.0, 0.0).astype(F32)
    block = lax.shift_right_logical(col0, 7)
    shift = col0 & 127
    back = (128 - shift) & 127
    none = jnp.zeros((8, 128), F32)

    def make_exit(i, power):
        at = pl.multiple_of(i * CH, CH)
        keep = lane < 128 - shift
        w = []
        for h in range(2):
            for p in range(2):
                rolled = [
                    pltpu.roll(obj[p, block + j, pl.ds(row0 + h * HALF + at, CH), :], back, 1)
                    for j in range(3)
                ]
                w.append([jnp.where(keep, rolled[j], rolled[j + 1]) for j in range(2)])
        for j in range(2):
            for h in range(2):
                wr, wi = w[2 * h][j], w[2 * h + 1][j]
                win[0, j, pl.ds(h * HALF + at, CH), :] = wr
                win[1, j, pl.ds(h * HALF + at, CH), :] = wi
                power = power + fold(wr * wr + wi * wi)
            for k in range(MODES):
                re, im = [], []
                for h in range(2):
                    wr, wi = w[2 * h][j], w[2 * h + 1][j]
                    pr = probe[0, k, pl.ds(j * SIDE + h * HALF + at, CH), :]
                    pi = probe[1, k, pl.ds(j * SIDE + h * HALF + at, CH), :]
                    re.append(pr * wr - pi * wi)
                    im.append(pr * wi + pi * wr)
                cols = slice(j * 128, (j + 1) * 128)
                wave[k, 0, pl.ds(at, CH), cols] = (re[0] + re[1]).astype(BF16)
                wave[k, 0, pl.ds(HALF + at, CH), cols] = (im[0] + im[1]).astype(BF16)
                wave[k, 1, pl.ds(at, CH), cols] = (re[0] - re[1]).astype(BF16)
                wave[k, 1, pl.ds(HALF + at, CH), cols] = (im[0] - im[1]).astype(BF16)
        return power

    power = lax.fori_loop(0, STEPS // 2, make_exit, none, unroll=UNROLL // 2)
    stats[0] = stats[0] + live * power

    for k in range(MODES):
        for parity in range(2):
            res = jnp.dot(tables[parity], wave[k, parity], preferred_element_type=F32)
            spot = slice(k * SIDE + parity * HALF, k * SIDE + (parity + 1) * HALF)
            for o in range(2):
                near = res[o * HALF:(o + 1) * HALF, 0:HALF]
                far = res[o * HALF:(o + 1) * HALF, HALF:SIDE]
                half[0, spot, o * HALF:(o + 1) * HALF] = (near + far).astype(BF16)
                half[1, spot, o * HALF:(o + 1) * HALF] = (near - far).astype(BF16)
    for parity in range(2):
        field[parity] = jnp.dot(half[parity], tables[4 + parity], preferred_element_type=F32)

    def correct(i, misfit):
        at = pl.multiple_of(i * CH, CH)
        parity = i // (STEPS // 2)
        to = pl.multiple_of((i % (STEPS // 2)) * CH, CH)
        for q in range(2):
            parts = [
                (field[q, pl.ds(k * SIDE + at, CH), 0:HALF], field[q, pl.ds(k * SIDE + at, CH), HALF:SIDE])
                for k in range(MODES)
            ]
            total = sum(re * re + im * im for re, im in parts)
            modulus = jnp.sqrt(total)
            amplitude = mags[batch, slot, pl.ds(at, CH), q * HALF:(q + 1) * HALF]
            factor = live * (amplitude / jnp.maximum(modulus, floor_value) - 1.0)
            gap = modulus - amplitude
            misfit = misfit + fold(gap * gap)
            cols = slice(q * HALF, (q + 1) * HALF)
            for k in range(MODES):
                wave[k, parity, pl.ds(to, CH), cols] = (parts[k][0] * factor).astype(BF16)
                wave[k, parity, pl.ds(HALF + to, CH), cols] = (parts[k][1] * factor).astype(BF16)
        return misfit

    misfit = lax.fori_loop(0, STEPS, correct, none, unroll=UNROLL)
    stats[1] = stats[1] + live * misfit

    for k in range(MODES):
        even = jnp.dot(tables[2], wave[k, 0], preferred_element_type=F32)
        odd = jnp.dot(tables[3], wave[k, 1], preferred_element_type=F32)
        for h, value in enumerate(((even + odd).astype(BF16), (even - odd).astype(BF16))):
            spot = slice(k * SIDE + h * HALF, k * SIDE + (h + 1) * HALF)
            for o in range(2):
                for q in range(2):
                    half[q, spot, o * HALF:(o + 1) * HALF] = value[
                        o * HALF:(o + 1) * HALF, q * HALF:(q + 1) * HALF
                    ]
    for parity in range(2):
        field[parity] = jnp.dot(half[parity], tables[6 + parity], preferred_element_type=F32)

    def spread(i, c):
        at = pl.multiple_of(i * CH, CH)
        term = [[None, None], [None, None]]
        for j in range(2):
            wr = win[0, j, pl.ds(at, CH), :]
            wi = win[1, j, pl.ds(at, CH), :]
            tr = ti = None
            for k in range(MODES):
                source = pl.ds(k * SIDE + at, CH)
                if j == 0:
                    ur = field[0, source, 0:HALF] + field[1, source, 0:HALF]
                    ui = field[0, source, HALF:SIDE] + field[1, source, HALF:SIDE]
                else:
                    ur = field[0, source, 0:HALF] - field[1, source, 0:HALF]
                    ui = field[0, source, HALF:SIDE] - field[1, source, HALF:SIDE]
                spot = pl.ds(j * SIDE + at, CH)
                pr = probe[0, k, spot, :]
                pi = probe[1, k, spot, :]
                ar = pr * ur + pi * ui
                ai = pr * ui - pi * ur
                tr = ar if tr is None else tr + ar
                ti = ai if ti is None else ti + ai
                pgrad[0, k, spot, :] = pgrad[0, k, spot, :] + (wr * ur + wi * ui)
                pgrad[1, k, spot, :] = pgrad[1, k, spot, :] + (wr * ui - wi * ur)
            term[0][j], term[1][j] = tr, ti
        low = lane < shift
        zero = jnp.zeros((CH, 128), F32)
        spot = pl.ds(SIDE + at, CH)
        for p in range(2):
            a = pltpu.roll(term[p][0], shift, 1)
            b = pltpu.roll(term[p][1], shift, 1)
            terms[slot, p, 1, spot, :] = jnp.where(low, zero, a)
            terms[slot, p, 2, spot, :] = jnp.where(low, a, b)
            terms[slot, p, 3, spot, :] = jnp.where(low, b, zero)
        return c

    lax.fori_loop(0, STEPS, spread, 0, unroll=UNROLL)


def body(
    rows_ref, cols_ref, counts_ref, object_in, probe_in, mags_in, tables_in, sort_in,
    object_out, probe_out, errors,
    obj, probes, grad, pgrad, terms, stats, mags, tables, sort, win, wave, half, field,
    core_in, acc, one_in, one, two_in, z_in, tile_in, tile_z, tile_core,
    inner_in, side_in, corner_in, row_in, rdma_send, rdma_recv, local, ready,
):
    row, col, core, coords, along, partner, tile = where_am_i()
    up, down = tile((row + 7) % 8, col), tile((row + 1) % 8, col)
    beside = (col + 15 + 2 * core) % 16
    outer = tile(row, beside)
    outer_up, outer_down = tile((row + 7) % 8, beside), tile((row + 1) % 8, beside)
    has_up, has_down = row > 0, row < 7
    has_outer = jnp.where(core == 0, col > 0, col < 15)
    inner_halo, outer_halo = 3 * (1 - core), 3 * core
    inner_own, outer_own = 2 - core, 1 + core
    greeted = [partner, outer, up, down, outer_up, outer_down]
    for axis in ("x", "y", "z"):
        for d in (1, 2, 3):
            greeted.append(along(axis, (coords[axis] + d) % 4))

    def greet(sem):
        for peer in greeted:
            pl.semaphore_signal(sem, inc=1, device_id=peer, device_id_type=pl.DeviceIdType.MESH)

    for p in range(2):
        for b in (0, 3):
            obj[p, b] = jnp.zeros((EXT, 128), F32)
        for b in (1, 2):
            obj[p, b, 0:HALF, :] = jnp.zeros((HALF, 128), F32)
            obj[p, b, SIDE + HALF:EXT, :] = jnp.zeros((HALF, 128), F32)
    barrier = pltpu.get_barrier_semaphore()
    greet(barrier)

    loads = []

    def load(src, dst):
        copy = pltpu.make_async_copy(src, dst, local.at[len(loads)])
        copy.start()
        loads.append(copy)

    for j in range(2):
        load(object_in.at[:, :, j * 128:(j + 1) * 128], obj.at[:, 1 + j, HALF:HALF + SIDE, :])
    for j in range(2):
        load(
            probe_in.at[:, :, :, j * 128:(j + 1) * 128],
            probes.at[0, :, :, j * SIDE:(j + 1) * SIDE, :],
        )
    load(tables_in, tables)
    load(sort_in, sort)
    load(mags_in.at[0, 0], mags)

    count = [0]

    def message(src, dst, peer):
        n = count[0]
        count[0] += 1
        return pltpu.make_async_remote_copy(
            src_ref=src, dst_ref=dst, send_sem=rdma_send.at[n], recv_sem=rdma_recv.at[n],
            device_id=peer, device_id_type=pl.DeviceIdType.MESH,
        )

    def send(src, dst, peer):
        copy = message(src, dst, peer)
        copy.start()
        return copy

    def wait(copies):
        for copy in copies:
            copy.wait()

    class Halo:
        def __init__(self, p):
            both = jnp.logical_and
            own, top, low = slice(HALF, SIDE + HALF), slice(HALF, SIDE), slice(SIDE, SIDE + HALF)
            above, below = slice(0, HALF), slice(SIDE + HALF, EXT)
            there = 3 * (1 - core)
            self.parts = [
                (message(obj.at[p, 1:3, top, :], obj.at[p, 1:3, below, :], up), has_up, has_down),
                (message(obj.at[p, 1:3, low, :], obj.at[p, 1:3, above, :], down), has_down, has_up),
                (message(obj.at[p, outer_own, own, :], obj.at[p, there, own, :], outer), has_outer, has_outer),
                (
                    message(obj.at[p, outer_own, top, :], obj.at[p, there, below, :], outer_up),
                    both(has_up, has_outer), both(has_down, has_outer),
                ),
                (
                    message(obj.at[p, outer_own, low, :], obj.at[p, there, above, :], outer_down),
                    both(has_down, has_outer), both(has_up, has_outer),
                ),
            ]
            self.inner = message(obj.at[p, inner_own], obj.at[p, 3 * core], partner)

        def start(self):
            for copy, sends, _ in self.parts:
                @pl.when(sends)
                def _():
                    copy.start()

        def wait_some(self, parts):
            for copy, sends, takes in parts:
                @pl.when(sends)
                def _():
                    copy.wait_send()

                @pl.when(takes)
                def _():
                    copy.wait_recv()

        def turn(self):
            self.wait_some(self.parts[0:2])
            self.inner.start()

        def finish(self):
            self.wait_some(self.parts[2:])
            self.inner.wait()

    pl.semaphore_wait(barrier, len(greeted))
    wait(loads[0:2])
    halo = [Halo(p) for p in range(2)]
    for p in range(2):
        halo[p].start()

    def clear(i, c):
        at = pl.multiple_of(i * 64, 64)
        nothing = jnp.zeros((64, 128), F32)
        for s in range(SLOTS):
            for p in range(2):
                for b in range(5):
                    terms[s, p, b, pl.ds(at, 64), :] = nothing
        return c

    lax.fori_loop(0, 12, clear, 0)
    pgrad[...] = jnp.zeros_like(pgrad)
    wait(loads[2:7])

    def pieces(x):
        high = x.astype(BF16)
        rest = x - high.astype(F32)
        middle = rest.astype(BF16)
        return (high, middle, (rest - middle.astype(F32)).astype(BF16))

    def arrange(n, c):
        b, s = n // SLOTS, n % SLOTS
        x = sum(jnp.dot(sort[0], v, preferred_element_type=F32) for v in pieces(mags[b, s]))
        mags[b, s] = sum(jnp.dot(v, sort[1], preferred_element_type=F32) for v in pieces(x))
        return c

    lax.fori_loop(0, BATCHES * SLOTS, arrange, 0)

    for p in range(2):
        halo[p].turn()
    for p in range(2):
        halo[p].finish()
    greet(ready)

    base = count[0]

    def update(u, carry):
        count[0] = base
        batch = u % BATCHES
        now = u % 2
        probe, fresh = probes.at[now], probes.at[1 - now]
        stats[...] = jnp.zeros_like(stats)

        def one_slot(slot, c):
            visit(
                batch, slot, rows_ref, cols_ref, counts_ref, obj, probe, mags, tables,
                terms, pgrad, stats, win, wave, half, field,
            )
            return c

        lax.fori_loop(0, SLOTS, one_slot, 0)

        spots = []
        for s in range(SLOTS):
            row0 = rows_ref[0, 0, batch, s]
            col0 = cols_ref[0, 0, batch, s]
            spots.append((1 - lax.shift_right_logical(col0, 7), SIDE - row0))

        def add_terms(p, b):
            def chunk(i, c):
                at = pl.multiple_of(i * 32, 32)
                grad[p, b, pl.ds(at, 32), :] = sum(
                    terms[s, p, spots[s][0] + b, pl.ds(spots[s][1] + at, 32), :] for s in range(SLOTS)
                )
                return c

            lax.fori_loop(0, EXT // 32, chunk, 0, unroll=4)

        pl.semaphore_wait(ready, len(greeted))

        inner_sent, outer_sent = [], []
        core_sent = [
            send(stats, tile_core, partner),
            send(pgrad.at[1 - core, 0:2], core_in.at[0:2], partner),
            send(pgrad.at[1 - core, 2:4], core_in.at[2:4], partner),
        ]
        for p in range(2):
            add_terms(p, inner_halo)
            inner_sent.append(send(grad.at[p, inner_halo], inner_in.at[p], partner))
        for p in range(2):
            add_terms(p, outer_halo)
            outer_sent.append([
                send(grad.at[p, outer_halo, HALF:SIDE + HALF, :], side_in.at[p], outer),
                send(grad.at[p, outer_halo, 0:HALF, :], corner_in.at[p, HALF:SIDE, :], outer_up),
                send(grad.at[p, outer_halo, SIDE + HALF:EXT, :], corner_in.at[p, 0:HALF, :], outer_down),
            ])

        def scatter(phase, source, landing, length, tile_value, groups=(0, 1)):
            me = coords[ORDERS[0][phase]]
            slot = tile_in.at[phase, me]
            if tile_value is not None:
                tile_in[phase, me] = tile_value
            sent = []
            for d in (2, 1, 3):
                if tile_value is not None:
                    sent.append(send(slot, slot, along(ORDERS[0][phase], (me + d) % 4)))
                for g in groups:
                    axis = ORDERS[g][phase]
                    to = (coords[axis] + d) % 4
                    at = pl.multiple_of(to * length, length)
                    sent.append(
                        send(
                            source.at[2 * g:2 * g + 2, pl.ds(at, length), :],
                            landing.at[d - 1, 2 * g:2 * g + 2],
                            along(axis, to),
                        )
                    )
            return sent

        def gather_sum(phase, source, landing, length):
            out = []
            for g in range(2):
                at = pl.multiple_of(coords[ORDERS[g][phase]] * length, length)
                for k in (2 * g, 2 * g + 1):
                    out.append(
                        source[k, pl.ds(at, length), :] + landing[0, k] + landing[1, k] + landing[2, k]
                    )
            return out

        def tile_total(phase):
            return (tile_in[phase, 0] + tile_in[phase, 1]) + (tile_in[phase, 2] + tile_in[phase, 3])

        def send_rows(p):
            inner_sent[p].wait()
            grad[p, inner_own] = grad[p, inner_own] + inner_in[p]
            return [
                send(grad.at[p, 1:3, 0:HALF, :], row_in.at[p, :, HALF:SIDE, :], up),
                send(grad.at[p, 1:3, SIDE + HALF:EXT, :], row_in.at[p, :, 0:HALF, :], down),
            ]

        wait(core_sent[0:2])
        for k in (0, 1):
            acc[k] = pgrad[core, k] + core_in[k]
        sent = scatter(0, acc, one_in, 128, stats[...] + tile_core[...], (0,))
        wait(core_sent[2:3])
        for k in (2, 3):
            acc[k] = pgrad[core, k] + core_in[k]
        sent += scatter(0, acc, one_in, 128, None, (1,))

        def peak_step(i, best):
            at = pl.multiple_of(i * 16, 16)
            total = None
            for p in range(2):
                for k in range(MODES):
                    v = probe[p, k, pl.ds(at, 16), :]
                    total = v * v if total is None else total + v * v
            return jnp.maximum(best, jnp.maximum(total[0:8], total[8:16]))

        best = lax.fori_loop(0, EXT // 16, peak_step, jnp.zeros((8, 128), F32), unroll=4)
        rate = object_rate / (jnp.max(best) + tiny_value)

        def finish_object(p):
            wait(rows_sent[p] + outer_sent[p])
            for h, has in ((0, has_up), (1, has_down)):
                there = slice(h * HALF, (h + 1) * HALF)
                here = slice((h + 1) * HALF, (h + 2) * HALF)
                for b in (1, 2):
                    total = grad[p, b, here, :] + jnp.where(has, row_in[p, b - 1, there, :], 0.0)
                    side = side_in[p, there, :] + jnp.where(has, corner_in[p, there, :], 0.0)
                    total = total + jnp.where(jnp.logical_and(has_outer, outer_own == b), side, 0.0)
                    obj[p, b, here, :] = obj[p, b, here, :] + rate * total

            @pl.when(u < UPDATES - 1)
            def _():
                halo[p].start()

        for p in range(2):
            add_terms(p, 1)
            add_terms(p, 2)
        rows_sent = [send_rows(p) for p in range(2)]

        wait(sent)
        for k, v in enumerate(gather_sum(0, acc, one_in, 128)):
            one[k] = v
        sent = scatter(1, one, two_in, 32, tile_total(0))

        wait(sent)
        z = coords["z"]
        for k, v in enumerate(gather_sum(1, one, two_in, 32)):
            z_in[z, k] = v
        tile_z[z] = tile_total(1)
        sent = []
        for d in (2, 1, 3):
            peer = along("z", (z + d) % 4)
            sent.append(send(tile_z.at[z], tile_z.at[z], peer))
            sent.append(send(z_in.at[z], z_in.at[z], peer))
        pgrad[...] = jnp.zeros_like(pgrad)
        halo = [Halo(p) for p in range(2)]
        wait(sent)

        totals = (tile_z[0] + tile_z[1]) + (tile_z[2] + tile_z[3])
        errors[u] = totals[1]
        gain = probe_rate * SIDE * SIDE / jnp.sum(totals[0])
        starts = []
        for g in range(2):
            a, b = coords[ORDERS[g][0]], coords[ORDERS[g][1]]
            starts.append((a * 128, a * 128 + b * 32))
        for k in range(MODES):
            spot = pl.ds(pl.multiple_of(starts[k // 2][1], 32), 32)
            total = (z_in[0, k] + z_in[1, k]) + (z_in[2, k] + z_in[3, k])
            fresh[core, k, spot, :] = probe[core, k, spot, :] + gain * total

        def block_of(g, at, length):
            at = pl.multiple_of(at, length)
            return fresh.at[core, 2 * g:2 * g + 2, pl.ds(at, length), :]

        def spread(phase, length):
            out = {}
            for d in (2, 1, 3):
                for g in range(2):
                    axis = ORDERS[g][phase]
                    block = block_of(g, starts[g][phase], length)
                    out[d, g] = send(block, block, along(axis, (coords[axis] + d) % 4))
            return out

        out2 = spread(1, 32)
        finish_object(0)
        wait(out2.values())
        out1 = spread(0, 128)
        finish_object(1)
        to_core = []
        for g in range(2):
            block = block_of(g, starts[g][0], 128)
            to_core.append(send(block, block, partner))

        @pl.when(u < UPDATES - 1)
        def _():
            for p in range(2):
                halo[p].turn()

        for d in (1, 3, 2):
            for g in range(2):
                out1[d, g].wait()
                axis = ORDERS[g][0]
                block = block_of(g, (coords[axis] + 4 - d) % 4 * 128, 128)
                to_core.append(send(block, block, partner))

        wait(to_core)

        @pl.when(u < UPDATES - 1)
        def _():
            for p in range(2):
                halo[p].finish()
            greet(ready)

        return carry

    lax.fori_loop(0, UPDATES, update, 0)

    stores = []
    for j in range(2):
        stores.append(
            pltpu.make_async_copy(
                obj.at[:, 1 + j, HALF:HALF + SIDE, :], object_out.at[:, :, j * 128:(j + 1) * 128], local.at[j]
            )
        )
        stores.append(
            pltpu.make_async_copy(
                probes.at[UPDATES % 2, :, :, j * SIDE:(j + 1) * SIDE, :],
                probe_out.at[:, :, :, j * 128:(j + 1) * 128],
                local.at[2 + j],
            )
        )
    for copy in stores:
        copy.start()
    wait(stores)


def on_device(object_field, probe, pos_rows, pos_cols, counts, magnitudes):
    tables = tuple(jnp.asarray(t) for t in transform_tables())
    anywhere = pl.BlockSpec(memory_space=pl.ANY)
    whole = pl.BlockSpec(memory_space=pltpu.VMEM)
    smem = pl.BlockSpec(memory_space=pltpu.SMEM)
    messages = 96
    out, probe_out, errors = pl.pallas_call(
        body,
        out_shape=(
            jax.ShapeDtypeStruct((2, SIDE, SIDE), F32),
            jax.ShapeDtypeStruct((2, MODES, SIDE, SIDE), F32),
            jax.ShapeDtypeStruct((UPDATES, 8, 128), F32),
        ),
        in_specs=[smem, smem, smem] + [anywhere] * 5,
        out_specs=(anywhere, anywhere, whole),
        scratch_shapes=[
            pltpu.VMEM((2, 4, EXT, 128), F32),
            pltpu.VMEM((2, 2, MODES, EXT, 128), F32),
            pltpu.VMEM((2, 4, EXT, 128), F32),
            pltpu.VMEM((2, MODES, EXT, 128), F32),
            pltpu.VMEM((SLOTS, 2, 5, 3 * SIDE, 128), F32),
            pltpu.VMEM((2, 8, 128), F32),
            pltpu.VMEM((BATCHES, SLOTS, SIDE, SIDE), F32),
            pltpu.VMEM((8, SIDE, SIDE), BF16),
            pltpu.VMEM((2, SIDE, SIDE), BF16),
            pltpu.VMEM((2, 2, SIDE, 128), F32),
            pltpu.VMEM((MODES, 2, SIDE, SIDE), BF16),
            pltpu.VMEM((2, MODES * SIDE, SIDE), BF16),
            pltpu.VMEM((2, MODES * SIDE, SIDE), F32),
            pltpu.VMEM((MODES, EXT, 128), F32),
            pltpu.VMEM((MODES, EXT, 128), F32),
            pltpu.VMEM((3, MODES, 128, 128), F32),
            pltpu.VMEM((MODES, 128, 128), F32),
            pltpu.VMEM((3, MODES, 32, 128), F32),
            pltpu.VMEM((4, MODES, 32, 128), F32),
            pltpu.VMEM((2, 4, 2, 8, 128), F32),
            pltpu.VMEM((4, 2, 8, 128), F32),
            pltpu.VMEM((2, 8, 128), F32),
            pltpu.VMEM((2, EXT, 128), F32),
            pltpu.VMEM((2, SIDE, 128), F32),
            pltpu.VMEM((2, SIDE, 128), F32),
            pltpu.VMEM((2, 2, SIDE, 128), F32),
            pltpu.SemaphoreType.DMA((messages,)),
            pltpu.SemaphoreType.DMA((messages,)),
            pltpu.SemaphoreType.DMA((8,)),
            pltpu.SemaphoreType.REGULAR,
        ],
        cost_estimate=pl.CostEstimate(flops=80 << 30, bytes_accessed=12 << 20, transcendentals=0),
        compiler_params=pltpu.CompilerParams(
            collective_id=0, has_side_effects=True, vmem_limit_bytes=60 << 20
        ),
        name="whole_sweep",
    )(
        pos_rows, pos_cols, counts,
        object_field, probe, magnitudes, *tables,
    )
    return (out, probe_out, jnp.sum(errors, axis=(1, 2)))


def solution(mesh):
    finer = Mesh(mesh.devices.reshape(4, 2, 4, 2, 2), AXES)
    return jax.shard_map(
        on_device,
        mesh=finer,
        in_specs=(
            P(None, ROW, COL),
            P(),
            P(ROW, COL, None, None),
            P(ROW, COL, None, None),
            P(ROW, COL, None),
            P(ROW, COL, None, None, None, None),
        ),
        out_specs=(P(None, ROW, COL), P(), P()),
        check_vma=False,
    )
```
